8 devices in a mesh: col: 2 (over z, y), row: 4 (over x, core).
Axes of the slice: x: 2, y: 2, z: 1, core: 2. Of those that a mesh axis runs over, the one named last changes fastest.
Arguments:
- t_amps: float32 [256, 6400], P('row', 'col')
- denoms: float32 [256, 6400], P('row', 'col')
- v_oovv: bfloat16 [256, 6400], P('row', 'col')
- v_vvvv: bfloat16 [6400, 6400], P('row', 'col')
- v_oooo: bfloat16 [256, 256], replicated
- w_direct: bfloat16 [1280, 1280], P(None, 'col')
- w_exch: bfloat16 [1280, 1280], P(None, 'col')
Outputs:
- output: float32 [256, 6400], P('row', 'col')
All inputs are finite; a program needn't handle non-finite values.
Results may differ from the reference program's by a relative error of at most 0.001.
Values are sent between devices in bfloat16 or wider.
A program may use at most 1 GiB of HBM per device.

```python
import jax
import jax.numpy as jnp

OCC = 16
VIRT = 80
PAIRS_OCC = OCC * OCC
PAIRS_VIRT = VIRT * VIRT
PH_DIM = OCC * VIRT


def setup_inputs(seed: int = 0) -> dict:
    keys = jax.random.split(jax.random.key(seed), 7)
    amp_scale = 1.5 * (OCC * VIRT) ** -0.5
    t_amps = amp_scale * jax.random.normal(keys[0], (PAIRS_OCC, PAIRS_VIRT), jnp.float32)
    denoms = -jax.random.uniform(keys[1], (PAIRS_OCC, PAIRS_VIRT), jnp.float32, 1.0, 3.0)
    v_oovv = jax.random.normal(keys[2], (PAIRS_OCC, PAIRS_VIRT), jnp.float32).astype(jnp.bfloat16)
    vvvv_scale = (OCC / VIRT) ** 0.5 / 1.5
    v_vvvv = (vvvv_scale * jax.random.normal(keys[3], (PAIRS_VIRT, PAIRS_VIRT), jnp.float32)).astype(jnp.bfloat16)
    oooo_scale = (VIRT / OCC) ** 0.5 / 1.5
    v_oooo = (oooo_scale * jax.random.normal(keys[4], (PAIRS_OCC, PAIRS_OCC), jnp.float32)).astype(jnp.bfloat16)
    w_direct = (0.6 * jax.random.normal(keys[5], (PH_DIM, PH_DIM), jnp.float32)).astype(jnp.bfloat16)
    w_exch = (0.6 * jax.random.normal(keys[6], (PH_DIM, PH_DIM), jnp.float32)).astype(jnp.bfloat16)
    return {"t_amps": t_amps, "denoms": denoms, "v_oovv": v_oovv, "v_vvvv": v_vvvv, "v_oooo": v_oooo, "w_direct": w_direct, "w_exch": w_exch}


def reference(t_amps, denoms, v_oovv, v_vvvv, v_oooo, w_direct, w_exch):
    t_half = t_amps.astype(jnp.bfloat16)
    ladder = jnp.dot(t_half, v_vvvv, preferred_element_type=jnp.float32)
    inter_x = jnp.dot(v_oovv, t_half.T, preferred_element_type=jnp.float32)
    hole_mat = (v_oooo.astype(jnp.float32) + 0.5 * inter_x).astype(jnp.bfloat16)
    hole_term = jnp.dot(hole_mat.T, t_half, preferred_element_type=jnp.float32)
    t_wide = t_half.astype(jnp.float32).reshape(OCC, OCC, VIRT, VIRT)
    wd_wide = w_direct.astype(jnp.float32).reshape(OCC, VIRT, OCC, VIRT)
    wx_wide = w_exch.astype(jnp.float32).reshape(OCC, VIRT, OCC, VIRT)
    direct_term = jnp.einsum("ikac,kcjb->ijab", t_wide, wd_wide)
    exch_term = jnp.einsum("ikcb,kcja->ijab", t_wide, wx_wide)
    ph_net = direct_term - exch_term
    ph_sym = (ph_net + ph_net.transpose(1, 0, 3, 2)).reshape(PAIRS_OCC, PAIRS_VIRT)
    residual = v_oovv.astype(jnp.float32) + ladder + hole_term + ph_sym
    return residual / denoms
```

```python
import functools

import jax
import jax.numpy as jnp
from jax import lax
from jax.experimental import pallas as pl
from jax.experimental.pallas import tpu as pltpu
from jax.sharding import PartitionSpec as P

MESH = pl.DeviceIdType.MESH
F32 = jnp.float32
BF16 = jnp.bfloat16

OCC = 16
VIRT = 80
ROWS = 64
COLS = 3200
KPAD = 1664
WIDE = 640
NCH = COLS // WIDE
ZT = 72
ZS = 40

T_X, T_Y, T_P, T_FWD, R_P, R_2, R_3, G_P = 0, 2, 4, 5, 7, 8, 10, 12
E_D, L_D, E_X, L_X, O_D, F_Y, G_Y, X_Y, M_1, M_2, M_3 = 16, 21, 26, 31, 36, 41, 46, 51, 52, 53, 54
N_SEM = 55


def split_segments(parts, lane):
    out = []
    for q in range(8):
        m, s = divmod(80 * q, 128)
        seg = parts[m]
        if s:
            seg = pltpu.roll(seg, 128 - s, axis=1)
            if s + 80 > 128:
                seg = jnp.where(lane < 128 - s, seg, pltpu.roll(parts[m + 1], 128 - s, axis=1))
        out.append(jnp.where(lane < 80, seg, 0.0))
    return out


def join_segments(segs, lane):
    r = [segs[0]] + [pltpu.roll(segs[q], (80 * q) % 128, axis=1) for q in range(1, 8)]
    return [
        jnp.where(lane < 80, r[0], r[1]),
        jnp.where(lane < 32, r[1], jnp.where(lane < 112, r[2], r[3])),
        jnp.where(lane < 64, r[3], r[4]),
        jnp.where(lane < 16, r[4], jnp.where(lane < 96, r[5], r[6])),
        jnp.where(lane < 48, r[6], r[7]),
    ]


def kernel(
    t_hbm, d_hbm, o_hbm, v_hbm, oooo_hbm, wd_hbm, wx_hbm, out_hbm,
    tf, dbuf, ov, vbuf, ob, wdp, wxb, obuf,
    tcol, ty, tr1, zt, tb, l3, r3o, r5o, zf, zg, fbuf, gbuf, gpart, frecv, grecv,
    xp, prx, pown, xrecv, xpart, xyrecv, msend, mfull,
    lsem, osem, ss, rs,
):
    r = lax.axis_index("row")
    c = lax.axis_index("col")
    k = lax.rem(r, 2)
    x = r // 2
    p1 = r + 1 - 2 * k
    p2 = lax.rem(r + 2, 4)
    p3 = lax.rem(p1 + 2, 4)
    diag = x == c
    off = x != c
    d_p, d_x, d_d, d_y = (c, p1), (c, p2), (c, p3), (1 - c, r)
    other = 2 * (1 - x)
    own = 2 * x

    def rc(src, dst, slot, dev):
        return pltpu.make_async_remote_copy(
            src_ref=src, dst_ref=dst, send_sem=ss.at[slot], recv_sem=rs.at[slot],
            device_id=dev, device_id_type=MESH,
        )

    def wide(n, base=0):
        return pl.ds(pl.multiple_of(base + n * WIDE, 128), WIDE)

    ld_t = pltpu.make_async_copy(t_hbm, tf, lsem.at[0])
    ld_v = pltpu.make_async_copy(v_hbm, vbuf.at[pl.ds(pl.multiple_of(64 * k, 64), 1600)], lsem.at[1])
    ld_wd = pltpu.make_async_copy(wd_hbm, wdp.at[:, pl.ds(0, VIRT)], lsem.at[2])
    ld_wx = pltpu.make_async_copy(wx_hbm, wxb, lsem.at[3])
    ld_o = pltpu.make_async_copy(o_hbm, ov, lsem.at[4])
    ld_d = pltpu.make_async_copy(d_hbm, dbuf, lsem.at[5])
    ld_oooo = pltpu.make_async_copy(oooo_hbm.at[pl.ds(pl.multiple_of(ROWS * r, ROWS), ROWS)], ob, lsem.at[6])
    ld_t.start()

    barrier = pltpu.get_barrier_semaphore()
    for dev in (d_p, d_x, d_d, d_y):
        pl.semaphore_signal(barrier, inc=1, device_id=dev, device_id_type=MESH)
    for ld in (ld_wd, ld_wx, ld_v, ld_o, ld_oooo, ld_d):
        ld.start()
    ld_t.wait()

    @pl.loop(0, 4)
    def _(s):
        rows = pl.ds(pl.multiple_of(16 * s, 16), 16)
        tcol[r, rows] = tf[rows].astype(BF16)

    pl.semaphore_wait(barrier, 4)

    def half(h):
        return pl.ds(32 * h, 32)

    def t_x(h, blk):
        return rc(tcol.at[blk, half(h)], tcol.at[blk, half(h)], T_X + h, d_x)

    def t_y(h):
        return rc(tcol.at[r, half(h)], ty.at[half(h)], T_Y + h, d_y)

    def t_fwd(h, blk):
        return rc(tcol.at[blk, half(h)], tcol.at[blk, half(h)], T_FWD + h, d_p)

    def t_p(blk):
        return rc(tcol.at[blk], tcol.at[blk], T_P, d_p)

    def my_k(core):
        return pl.ds(pl.multiple_of(1536 * core, 128), KPAD)

    def r_p(blk):
        return rc(ty.at[:, my_k(1 - k)], tr1.at[blk], R_P, d_p)

    def r_2(h):
        return rc(tcol.at[p2, half(h), my_k(k)], tr1.at[p2, half(h)], R_2 + h, d_y)

    def r_3(h):
        return rc(tcol.at[p3, half(h), my_k(k)], tr1.at[p3, half(h)], R_3 + h, d_y)

    for h in range(2):
        t_x(h, r).start()
        t_y(h).start()
    t_p(r).start()

    lane64 = lax.broadcasted_iota(jnp.int32, (ROWS, 128), 1)
    vbuf[pl.ds(pl.multiple_of(1600 * (1 - k), 64), 64)] = jnp.zeros((64, COLS), BF16)
    wdp[:, pl.ds(VIRT, 48)] = jnp.zeros((OCC, 48, WIDE), BF16)

    def slabs(ref, col_half):
        @pl.loop(0, NCH)
        def _(g):
            parts = [
                ref[:, pl.ds(pl.multiple_of(g * WIDE + 128 * m, 128), 128)].astype(F32)
                for m in range(5)
            ]
            for q, seg in enumerate(split_segments(parts, lane64)):
                zt[pl.ds(pl.multiple_of((col_half * 40 + g * 8 + q) * ZT, 8), ROWS)] = seg

    slabs(tf, c)

    for h in range(2):
        t_x(h, p2).wait_recv()
        t_fwd(h, p2).start()

        @pl.when(diag)
        def _():
            r_2(h).start()

    for h in range(2):
        t_fwd(h, p3).wait_recv()

        @pl.when(diag)
        def _():
            r_3(h).start()

    for h in range(2):
        t_y(h).wait_recv()

    @pl.when(off)
    def _():
        r_p(r).start()

    slabs(ty, 1 - c)

    for i in range(4):
        @pl.loop(0, OCC)
        def _(kk):
            blk = zt[pl.ds(i * OCC + kk, VIRT, stride=ZT)].astype(BF16)
            tb[i * OCC + kk] = blk
            l3[pl.ds(i * VIRT, VIRT), pl.ds(pl.multiple_of(kk * 128, 128), 128)] = blk

    ld_wd.wait()
    r3o[...] = jnp.dot(l3[...], wdp[...].reshape(OCC * 128, WIDE), preferred_element_type=F32)
    ld_wx.wait()
    rhs = jnp.concatenate([tb[pl.ds(i * OCC, OCC)].reshape(OCC * VIRT, 128) for i in range(4)], axis=1)
    r5o[...] = lax.dot_general(wxb[...], rhs, (((0,), (0,)), ((), ())), preferred_element_type=F32)

    lane80 = lax.broadcasted_iota(jnp.int32, (VIRT, 128), 1)

    @pl.loop(0, 4)
    def _(i):
        rows = pl.ds(pl.multiple_of(i * VIRT, 8), VIRT)
        parts = [r3o[rows, pl.ds(128 * m, 128)] for m in range(5)]
        for j, seg in enumerate(split_segments(parts, lane80)):
            s_ij = seg - r5o[pl.ds(j * VIRT, VIRT), pl.ds(pl.multiple_of(i * 128, 128), 128)]
            zf[pl.ds((j // 4) * 16 + i * 4 + j % 4, VIRT, stride=ZS)] = s_ij
            s_ji = jnp.transpose(jnp.concatenate([s_ij, jnp.zeros((48, 128), F32)], axis=0))
            zg[pl.ds(j * 4 + i, VIRT, stride=ZS)] = s_ji[:VIRT]

    lane32 = lax.broadcasted_iota(jnp.int32, (32, 128), 1)
    for z, flat in ((zg, gbuf), (zf, fbuf)):
        @pl.loop(0, 2 * NCH)
        def _(g):
            segs = [z[pl.ds(pl.multiple_of((g * 8 + q) * ZS, 8), 32)] for q in range(8)]
            for m, tile in enumerate(join_segments(segs, lane32)):
                flat[:, pl.ds(pl.multiple_of(g * WIDE + 128 * m, 128), 128)] = tile

    def g_y(n):
        return rc(gbuf.at[:, wide(n, COLS * (1 - c))], grecv.at[:, wide(n)], G_Y + n, d_y)

    def f_y(n):
        return rc(fbuf.at[:, wide(n, COLS * (1 - c))], frecv.at[:, wide(n)], F_Y + n, d_y)

    def g_p():
        return rc(gbuf.at[pl.ds(pl.multiple_of(16 * (1 - k), 16), 16)], gpart, G_P, d_p)

    @pl.when(off)
    def _():
        for n in range(NCH):
            g_y(n).start()

    @pl.when(off)
    def _():
        @pl.loop(0, NCH)
        def _(n):
            grecv[:, wide(n)] = gbuf[:, wide(n, COLS * c)]

    @pl.when(diag)
    def _():
        g_p().start()
        g_p().wait_recv()
        mine = pl.ds(pl.multiple_of(16 * k, 16), 16)
        theirs = pl.ds(pl.multiple_of(16 * (1 - k), 16), 16)

        @pl.loop(0, 2 * NCH)
        def _(n):
            fbuf[mine, wide(n)] += gbuf[mine, wide(n)]
            fbuf[theirs, wide(n)] += gpart[:, wide(n)]

    for n in range(NCH):
        f_y(n).start()

    @pl.when(diag)
    def _():
        t_p(p1).wait_recv()

        @pl.loop(0, 4)
        def _(b):
            tr1[b] = tcol[b, :, my_k(k)]

    @pl.when(off)
    def _():
        t_p(p1).wait_recv()
        tr1[r] = ty[:, my_k(k)]
        r_p(p1).wait_recv()
        for h in range(2):
            r_2(h).wait_recv()
            r_3(h).wait_recv()

    ld_v.wait()

    def ladder(first, n):
        lhs = tr1[pl.ds(first, 2)].reshape(128, KPAD)
        prod = jnp.dot(lhs, vbuf[:, wide(n)], preferred_element_type=F32)
        xp[pl.ds(first, 2), :, :, :, wide(n)] = prod.reshape(2, 4, 2, 8, WIDE)

    def pair(n, hf, slot):
        return rc(xp.at[p3, :, hf, :, wide(n)], prx.at[:, hf, :, wide(n)], slot + n, d_p)

    def cross(n, hf, slot):
        return rc(xp.at[p2, :, hf, :, wide(n)], xrecv.at[:, hf, :, wide(n)], slot + n, d_x)

    def combine(n, hf, slot_d, slot_x):
        pair(n, hf, slot_d).wait_recv()
        xp[p2, :, hf, :, wide(n)] += prx[:, hf, :, wide(n)]
        cross(n, hf, slot_x).start()

    early, late = 1 - x, x

    @pl.loop(0, NCH)
    def _(n):
        ladder(other, n)
        pair(n, early, E_D).start()

        @pl.when(n > 0)
        def _():
            combine(n - 1, early, E_D, E_X)

    combine(NCH - 1, early, E_D, E_X)

    ld_o.wait()
    xpart[...] = lax.dot_general(
        ov[...], tcol[...].reshape(4 * ROWS, COLS), (((1,), (1,)), ((), ())), preferred_element_type=F32
    )
    x_y = rc(xpart, xyrecv, X_Y, d_y)
    x_y.start()

    def out_pair(n):
        return rc(xp.at[p1, :, :, :, wide(n)], pown.at[:, :, :, wide(n)], O_D + n, d_p)

    @pl.loop(0, NCH)
    def _(n):
        ladder(own, n)
        out_pair(n).start()

    x_y.wait_recv()
    ld_oooo.wait()
    m_rows = (ob[...].astype(F32) + 0.5 * (xpart[...] + xyrecv[...])).astype(BF16)
    for q in range(4):
        msend[q] = m_rows[:, q * ROWS:(q + 1) * ROWS]
    mfull[r] = msend[r]
    m_copies = [
        rc(msend.at[p1], mfull.at[r], M_1, d_p),
        rc(msend.at[p2], mfull.at[r], M_2, d_x),
        rc(msend.at[p3], mfull.at[r], M_3, d_d),
    ]
    for cp in m_copies:
        cp.start()

    row8 = lax.broadcasted_iota(jnp.int32, (8, WIDE), 0)
    here = (row8 // 4) == k

    @pl.loop(0, NCH)
    def _(n):
        @pl.when(diag)
        def _():
            g_y(n).wait_recv()

        for b in range(2):
            for t in range(4):
                g4 = grecv[pl.ds(16 * b + 4 * t, 4), wide(n)]
                g8 = jnp.where(here, jnp.concatenate([g4, g4], axis=0), 0.0)
                xp[other + b, t, late, :, wide(n)] += g8
        pair(n, late, L_D).start()

        @pl.when(n > 0)
        def _():
            combine(n - 1, late, L_D, L_X)

    combine(NCH - 1, late, L_D, L_X)

    for cp in (
        rc(msend.at[p1], mfull.at[p1], M_1, d_p),
        rc(msend.at[p2], mfull.at[p2], M_2, d_x),
        rc(msend.at[p3], mfull.at[p3], M_3, d_d),
    ):
        cp.wait_recv()
    ld_d.wait()

    def put(n):
        return pltpu.make_async_copy(obuf.at[:, wide(n)], out_hbm.at[:, wide(n)], osem.at[n])

    @pl.loop(0, NCH)
    def _(n):
        r2 = lax.dot_general(
            mfull[...].reshape(4 * ROWS, ROWS), tcol[:, :, wide(n)].reshape(4 * ROWS, WIDE),
            (((0,), (0,)), ((), ())), preferred_element_type=F32,
        )
        acc = ov[:, wide(n)].astype(F32) + r2
        out_pair(n).wait_recv()
        f_y(n).wait_recv()
        cross(n, 1 - x, L_X).wait_recv()
        cross(n, x, E_X).wait_recv()
        part = xp[r, :, :, :, wide(n)] + pown[:, :, :, wide(n)] + xrecv[:, :, :, wide(n)]
        acc = acc + part.reshape(ROWS, WIDE)
        obuf[:, wide(n)] = acc
        for i in range(4):
            for ref, hf, base in ((fbuf, c, COLS * c), (frecv, 1 - c, 0)):
                f8 = jnp.concatenate(
                    [ref[pl.ds(4 * i, 4), wide(n, base)], ref[pl.ds(16 + 4 * i, 4), wide(n, base)]], axis=0
                )
                rows = pl.ds(pl.multiple_of(16 * i + 8 * hf, 8), 8)
                obuf[rows, wide(n)] += f8
        obuf[:, wide(n)] = obuf[:, wide(n)] / dbuf[:, wide(n)]
        put(n).start()

    for n in range(NCH):
        put(n).wait()
        f_y(n).wait_send()
        out_pair(n).wait_send()
        pair(n, early, E_D).wait_send()
        pair(n, late, L_D).wait_send()
        cross(n, early, E_X).wait_send()
        cross(n, late, L_X).wait_send()
    for cp in m_copies:
        cp.wait_send()
    x_y.wait_send()
    t_p(r).wait_send()
    for h in range(2):
        t_x(h, r).wait_send()
        t_y(h).wait_send()
        t_fwd(h, p2).wait_send()

    @pl.when(diag)
    def _():
        g_p().wait_send()
        for h in range(2):
            r_2(h).wait_send()
            r_3(h).wait_send()

    @pl.when(off)
    def _():
        r_p(r).wait_send()
        for n in range(NCH):
            g_y(n).wait_send()


def solution(mesh):
    def sweep(t_blk, d_blk, o_blk, v_blk, oooo, wd_blk, wx_blk):
        any_spec = pl.BlockSpec(memory_space=pl.ANY)
        vm = pltpu.VMEM
        return pl.pallas_call(
            kernel,
            out_shape=jax.ShapeDtypeStruct((ROWS, COLS), F32),
            in_specs=[any_spec] * 7,
            out_specs=any_spec,
            scratch_shapes=[
                vm((ROWS, COLS), F32),
                vm((ROWS, COLS), F32),
                vm((ROWS, COLS), BF16),
                vm((KPAD, COLS), BF16),
                vm((ROWS, 256), BF16),
                vm((OCC, 128, WIDE), BF16),
                vm((OCC * VIRT, WIDE), BF16),
                vm((ROWS, COLS), F32),
                vm((4, ROWS, COLS), BF16),
                vm((ROWS, COLS), BF16),
                vm((4, ROWS, KPAD), BF16),
                vm((VIRT * ZT, 128), F32),
                vm((ROWS, VIRT, 128), BF16),
                vm((4 * VIRT, OCC * 128), BF16),
                vm((4 * VIRT, WIDE), F32),
                vm((WIDE, 512), F32),
                vm((VIRT * ZS, 128), F32),
                vm((VIRT * ZS, 128), F32),
                vm((32, 2 * COLS), F32),
                vm((32, 2 * COLS), F32),
                vm((16, 2 * COLS), F32),
                vm((32, COLS), F32),
                vm((32, COLS), F32),
                vm((4, 4, 2, 8, COLS), F32),
                vm((4, 2, 8, COLS), F32),
                vm((4, 2, 8, COLS), F32),
                vm((4, 2, 8, COLS), F32),
                vm((ROWS, 256), F32),
                vm((ROWS, 256), F32),
                vm((4, ROWS, ROWS), BF16),
                vm((4, ROWS, ROWS), BF16),
                pltpu.SemaphoreType.DMA((7,)),
                pltpu.SemaphoreType.DMA((NCH,)),
                pltpu.SemaphoreType.DMA((N_SEM,)),
                pltpu.SemaphoreType.DMA((N_SEM,)),
            ],
            compiler_params=pltpu.CompilerParams(
                collective_id=0, has_side_effects=True, vmem_limit_bytes=60 * 1024 * 1024
            ),
            name="ccd_sweep",
        )(t_blk, d_blk, o_blk, v_blk, oooo, wd_blk.reshape(OCC, VIRT, WIDE), wx_blk)

    amp = P("row", "col")
    wide_spec = P(None, "col")
    return jax.shard_map(
        sweep, mesh=mesh, in_specs=(amp, amp, amp, amp, P(), wide_spec, wide_spec), out_specs=amp, check_vma=False
    )
```

```python
import functools

import jax
import jax.numpy as jnp
from jax import lax
from jax.experimental import pallas as pl
from jax.experimental.pallas import tpu as pltpu
from jax.sharding import PartitionSpec as P

MESH = pl.DeviceIdType.MESH
F32 = jnp.float32
BF16 = jnp.bfloat16

OCC = 16
VIRT = 80
ROWS = 64
COLS = 3200
KPAD = 1664
WIDE = 640
NCH = COLS // WIDE
ZT = 72
ZS = 40

T_X, T_Y, T_P, T_FWD, R_P, R_2, R_3, G_P = 0, 2, 4, 5, 7, 8, 10, 12
E_D, L_D, E_X, L_X, O_D, F_Y, G_Y, X_Y, M_1, M_2, M_3 = 16, 21, 26, 31, 36, 41, 46, 51, 52, 53, 54
N_SEM = 55


def split_segments(parts, lane):
    out = []
    for q in range(8):
        m, s = divmod(80 * q, 128)
        seg = parts[m]
        if s:
            seg = pltpu.roll(seg, 128 - s, axis=1)
            if s + 80 > 128:
                seg = jnp.where(lane < 128 - s, seg, pltpu.roll(parts[m + 1], 128 - s, axis=1))
        out.append(jnp.where(lane < 80, seg, 0.0))
    return out


def join_segments(segs, lane):
    r = [segs[0]] + [pltpu.roll(segs[q], (80 * q) % 128, axis=1) for q in range(1, 8)]
    return [
        jnp.where(lane < 80, r[0], r[1]),
        jnp.where(lane < 32, r[1], jnp.where(lane < 112, r[2], r[3])),
        jnp.where(lane < 64, r[3], r[4]),
        jnp.where(lane < 16, r[4], jnp.where(lane < 96, r[5], r[6])),
        jnp.where(lane < 48, r[6], r[7]),
    ]


def kernel(
    t_hbm, d_hbm, o_hbm, v_hbm, oooo_hbm, wd_hbm, wx_hbm, out_hbm,
    tf, dbuf, ov, vbuf, ob, wdp, wxb, obuf,
    tcol, ty, tr1, zt, tb, l3, r3o, r5o, zf, zg, fbuf, gbuf, gpart, frecv, grecv,
    xp, prx, pown, xrecv, xpart, xyrecv, msend, mfull,
    lsem, osem, ss, rs,
):
    r = lax.axis_index("row")
    c = lax.axis_index("col")
    k = lax.rem(r, 2)
    x = r // 2
    p1 = r + 1 - 2 * k
    p2 = lax.rem(r + 2, 4)
    p3 = lax.rem(p1 + 2, 4)
    diag = x == c
    off = x != c
    d_p, d_x, d_d, d_y = (c, p1), (c, p2), (c, p3), (1 - c, r)
    other = 2 * (1 - x)
    own = 2 * x

    def rc(src, dst, slot, dev):
        return pltpu.make_async_remote_copy(
            src_ref=src, dst_ref=dst, send_sem=ss.at[slot], recv_sem=rs.at[slot],
            device_id=dev, device_id_type=MESH,
        )

    def wide(n, base=0):
        return pl.ds(pl.multiple_of(base + n * WIDE, 128), WIDE)

    ld_t = pltpu.make_async_copy(t_hbm, tf, lsem.at[0])
    ld_v = pltpu.make_async_copy(v_hbm, vbuf.at[pl.ds(pl.multiple_of(64 * k, 64), 1600)], lsem.at[1])
    ld_wd = pltpu.make_async_copy(wd_hbm, wdp.at[:, pl.ds(0, VIRT)], lsem.at[2])
    ld_wx = pltpu.make_async_copy(wx_hbm, wxb, lsem.at[3])
    ld_o = pltpu.make_async_copy(o_hbm, ov, lsem.at[4])
    ld_d = pltpu.make_async_copy(d_hbm, dbuf, lsem.at[5])
    ld_oooo = pltpu.make_async_copy(oooo_hbm.at[pl.ds(pl.multiple_of(ROWS * r, ROWS), ROWS)], ob, lsem.at[6])
    ld_t.start()

    barrier = pltpu.get_barrier_semaphore()
    for dev in (d_p, d_x, d_d, d_y):
        pl.semaphore_signal(barrier, inc=1, device_id=dev, device_id_type=MESH)
    for ld in (ld_wd, ld_wx, ld_v, ld_o, ld_oooo, ld_d):
        ld.start()
    ld_t.wait()

    @pl.loop(0, 4)
    def _(s):
        rows = pl.ds(pl.multiple_of(16 * s, 16), 16)
        tcol[r, rows] = tf[rows].astype(BF16)

    pl.semaphore_wait(barrier, 4)

    def half(h):
        return pl.ds(32 * h, 32)

    def t_x(h, blk):
        return rc(tcol.at[blk, half(h)], tcol.at[blk, half(h)], T_X + h, d_x)

    def t_y(h):
        return rc(tcol.at[r, half(h)], ty.at[half(h)], T_Y + h, d_y)

    def t_fwd(h, blk):
        return rc(tcol.at[blk, half(h)], tcol.at[blk, half(h)], T_FWD + h, d_p)

    def t_p(blk):
        return rc(tcol.at[blk], tcol.at[blk], T_P, d_p)

    def my_k(core):
        return pl.ds(pl.multiple_of(1536 * core, 128), KPAD)

    def r_p(blk):
        return rc(ty.at[:, my_k(1 - k)], tr1.at[blk], R_P, d_p)

    def r_2(h):
        return rc(tcol.at[p2, half(h), my_k(k)], tr1.at[p2, half(h)], R_2 + h, d_y)

    def r_3(h):
        return rc(tcol.at[p3, half(h), my_k(k)], tr1.at[p3, half(h)], R_3 + h, d_y)

    for h in range(2):
        t_x(h, r).start()
        t_y(h).start()
    t_p(r).start()

    lane64 = lax.broadcasted_iota(jnp.int32, (ROWS, 128), 1)
    vbuf[pl.ds(pl.multiple_of(1600 * (1 - k), 64), 64)] = jnp.zeros((64, COLS), BF16)
    wdp[:, pl.ds(VIRT, 48)] = jnp.zeros((OCC, 48, WIDE), BF16)

    def slabs(ref, col_half):
        @pl.loop(0, NCH)
        def _(g):
            parts = [
                ref[:, pl.ds(pl.multiple_of(g * WIDE + 128 * m, 128), 128)].astype(F32)
                for m in range(5)
            ]
            for q, seg in enumerate(split_segments(parts, lane64)):
                zt[pl.ds(pl.multiple_of((col_half * 40 + g * 8 + q) * ZT, 8), ROWS)] = seg

    slabs(tf, c)

    for h in range(2):
        t_x(h, p2).wait_recv()
        t_fwd(h, p2).start()

        @pl.when(diag)
        def _():
            r_2(h).start()

    for h in range(2):
        t_fwd(h, p3).wait_recv()

        @pl.when(diag)
        def _():
            r_3(h).start()

    def ladder(first, n):
        lhs = tr1[pl.ds(first, 2)].reshape(128, KPAD)
        prod = jnp.dot(lhs, vbuf[:, wide(n)], preferred_element_type=F32)
        xp[pl.ds(first, 2), :, :, :, wide(n)] = prod.reshape(2, 4, 2, 8, WIDE)

    def pair(n, hf, slot):
        return rc(xp.at[p3, :, hf, :, wide(n)], prx.at[:, hf, :, wide(n)], slot + n, d_p)

    def cross(n, hf, slot):
        return rc(xp.at[p2, :, hf, :, wide(n)], xrecv.at[:, hf, :, wide(n)], slot + n, d_x)

    def combine(n, hf, slot_d, slot_x):
        pair(n, hf, slot_d).wait_recv()
        xp[p2, :, hf, :, wide(n)] += prx[:, hf, :, wide(n)]
        cross(n, hf, slot_x).start()

    early, late = 1 - x, x

    def early_pass():
        ld_v.wait()

        @pl.loop(0, NCH)
        def _(n):
            ladder(other, n)
            pair(n, early, E_D).start()

            @pl.when(n > 0)
            def _():
                combine(n - 1, early, E_D, E_X)

        combine(NCH - 1, early, E_D, E_X)

    @pl.when(diag)
    def _():
        t_p(p1).wait_recv()

        @pl.loop(0, 4)
        def _(b):
            tr1[b] = tcol[b, :, my_k(k)]

        early_pass()

    for h in range(2):
        t_y(h).wait_recv()

    @pl.when(off)
    def _():
        r_p(r).start()

    @pl.when(off)
    def _():
        t_p(p1).wait_recv()

    ld_o.wait()
    xpart[...] = lax.dot_general(
        ov[...], tcol[...].reshape(4 * ROWS, COLS), (((1,), (1,)), ((), ())), preferred_element_type=F32
    )
    x_y = rc(xpart, xyrecv, X_Y, d_y)
    x_y.start()

    slabs(ty, 1 - c)

    for i in range(4):
        @pl.loop(0, OCC)
        def _(kk):
            blk = zt[pl.ds(i * OCC + kk, VIRT, stride=ZT)].astype(BF16)
            tb[i * OCC + kk] = blk
            l3[pl.ds(i * VIRT, VIRT), pl.ds(pl.multiple_of(kk * 128, 128), 128)] = blk

    ld_wd.wait()
    r3o[...] = jnp.dot(l3[...], wdp[...].reshape(OCC * 128, WIDE), preferred_element_type=F32)
    ld_wx.wait()
    rhs = jnp.concatenate([tb[pl.ds(i * OCC, OCC)].reshape(OCC * VIRT, 128) for i in range(4)], axis=1)
    r5o[...] = lax.dot_general(wxb[...], rhs, (((0,), (0,)), ((), ())), preferred_element_type=F32)

    lane80 = lax.broadcasted_iota(jnp.int32, (VIRT, 128), 1)

    @pl.loop(0, 4)
    def _(i):
        rows = pl.ds(pl.multiple_of(i * VIRT, 8), VIRT)
        parts = [r3o[rows, pl.ds(128 * m, 128)] for m in range(5)]
        for j, seg in enumerate(split_segments(parts, lane80)):
            s_ij = seg - r5o[pl.ds(j * VIRT, VIRT), pl.ds(pl.multiple_of(i * 128, 128), 128)]
            zf[pl.ds((j // 4) * 16 + i * 4 + j % 4, VIRT, stride=ZS)] = s_ij
            s_ji = jnp.transpose(jnp.concatenate([s_ij, jnp.zeros((48, 128), F32)], axis=0))
            zg[pl.ds(j * 4 + i, VIRT, stride=ZS)] = s_ji[:VIRT]

    lane32 = lax.broadcasted_iota(jnp.int32, (32, 128), 1)

    def g_y(n):
        return rc(gbuf.at[:, wide(n, COLS * (1 - c))], grecv.at[:, wide(n)], G_Y + n, d_y)

    def f_y(n):
        return rc(fbuf.at[:, wide(n, COLS * (1 - c))], frecv.at[:, wide(n)], F_Y + n, d_y)

    def g_p():
        return rc(gbuf.at[pl.ds(pl.multiple_of(16 * (1 - k), 16), 16)], gpart, G_P, d_p)

    def flatten(z, g):
        segs = [z[pl.ds(pl.multiple_of((g * 8 + q) * ZS, 8), 32)] for q in range(8)]
        return join_segments(segs, lane32)

    @pl.loop(0, NCH)
    def _(n):
        for m, tile in enumerate(flatten(zg, n + NCH * (1 - c))):
            gbuf[:, pl.ds(pl.multiple_of(COLS * (1 - c) + n * WIDE + 128 * m, 128), 128)] = tile

        @pl.when(off)
        def _():
            g_y(n).start()

    @pl.loop(0, NCH)
    def _(n):
        tiles = flatten(zg, n + NCH * c)

        @pl.when(diag)
        def _():
            for m, tile in enumerate(tiles):
                gbuf[:, pl.ds(pl.multiple_of(COLS * c + n * WIDE + 128 * m, 128), 128)] = tile

        @pl.when(off)
        def _():
            for m, tile in enumerate(tiles):
                grecv[:, pl.ds(pl.multiple_of(n * WIDE + 128 * m, 128), 128)] = tile

    mine = pl.ds(pl.multiple_of(16 * k, 16), 16)
    theirs = pl.ds(pl.multiple_of(16 * (1 - k), 16), 16)

    @pl.when(diag)
    def _():
        g_p().start()
        g_p().wait_recv()

    def f_flat(hf, send):
        @pl.loop(0, NCH)
        def _(n):
            for m, tile in enumerate(flatten(zf, n + NCH * hf)):
                fbuf[:, pl.ds(pl.multiple_of(COLS * hf + n * WIDE + 128 * m, 128), 128)] = tile

            @pl.when(diag)
            def _():
                cols = wide(n, COLS * hf)
                fbuf[mine, cols] += gbuf[mine, cols]
                fbuf[theirs, cols] += gpart[:, cols]

            if send:
                f_y(n).start()

    f_flat(1 - c, True)
    f_flat(c, False)

    @pl.when(off)
    def _():
        tr1[r] = ty[:, my_k(k)]
        r_p(p1).wait_recv()
        for h in range(2):
            r_2(h).wait_recv()
            r_3(h).wait_recv()
        early_pass()

    def out_pair(n):
        return rc(xp.at[p1, :, :, :, wide(n)], pown.at[:, :, :, wide(n)], O_D + n, d_p)

    @pl.loop(0, NCH)
    def _(n):
        ladder(own, n)
        out_pair(n).start()

    x_y.wait_recv()
    ld_oooo.wait()
    m_rows = (ob[...].astype(F32) + 0.5 * (xpart[...] + xyrecv[...])).astype(BF16)
    for q in range(4):
        msend[q] = m_rows[:, q * ROWS:(q + 1) * ROWS]
    mfull[r] = msend[r]
    m_copies = [
        rc(msend.at[p1], mfull.at[r], M_1, d_p),
        rc(msend.at[p2], mfull.at[r], M_2, d_x),
        rc(msend.at[p3], mfull.at[r], M_3, d_d),
    ]
    for cp in m_copies:
        cp.start()

    row8 = lax.broadcasted_iota(jnp.int32, (8, WIDE), 0)
    here = (row8 // 4) == k

    @pl.loop(0, NCH)
    def _(n):
        @pl.when(diag)
        def _():
            g_y(n).wait_recv()

        for b in range(2):
            for t in range(4):
                g4 = grecv[pl.ds(16 * b + 4 * t, 4), wide(n)]
                g8 = jnp.where(here, jnp.concatenate([g4, g4], axis=0), 0.0)
                xp[other + b, t, late, :, wide(n)] += g8
        pair(n, late, L_D).start()

        @pl.when(n > 0)
        def _():
            combine(n - 1, late, L_D, L_X)

    combine(NCH - 1, late, L_D, L_X)

    for cp in (
        rc(msend.at[p1], mfull.at[p1], M_1, d_p),
        rc(msend.at[p2], mfull.at[p2], M_2, d_x),
        rc(msend.at[p3], mfull.at[p3], M_3, d_d),
    ):
        cp.wait_recv()
    ld_d.wait()

    def put(n):
        return pltpu.make_async_copy(obuf.at[:, wide(n)], out_hbm.at[:, wide(n)], osem.at[n])

    @pl.loop(0, NCH)
    def _(n):
        r2 = lax.dot_general(
            mfull[...].reshape(4 * ROWS, ROWS), tcol[:, :, wide(n)].reshape(4 * ROWS, WIDE),
            (((0,), (0,)), ((), ())), preferred_element_type=F32,
        )
        acc = ov[:, wide(n)].astype(F32) + r2
        out_pair(n).wait_recv()
        f_y(n).wait_recv()
        cross(n, 1 - x, L_X).wait_recv()
        cross(n, x, E_X).wait_recv()
        part = xp[r, :, :, :, wide(n)] + pown[:, :, :, wide(n)] + xrecv[:, :, :, wide(n)]
        acc = acc + part.reshape(ROWS, WIDE)
        obuf[:, wide(n)] = acc
        for i in range(4):
            for ref, hf, base in ((fbuf, c, COLS * c), (frecv, 1 - c, 0)):
                f8 = jnp.concatenate(
                    [ref[pl.ds(4 * i, 4), wide(n, base)], ref[pl.ds(16 + 4 * i, 4), wide(n, base)]], axis=0
                )
                rows = pl.ds(pl.multiple_of(16 * i + 8 * hf, 8), 8)
                obuf[rows, wide(n)] += f8
        obuf[:, wide(n)] = obuf[:, wide(n)] / dbuf[:, wide(n)]
        put(n).start()

    for n in range(NCH):
        put(n).wait()
        f_y(n).wait_send()
        out_pair(n).wait_send()
        pair(n, early, E_D).wait_send()
        pair(n, late, L_D).wait_send()
        cross(n, early, E_X).wait_send()
        cross(n, late, L_X).wait_send()
    for cp in m_copies:
        cp.wait_send()
    x_y.wait_send()
    t_p(r).wait_send()
    for h in range(2):
        t_x(h, r).wait_send()
        t_y(h).wait_send()
        t_fwd(h, p2).wait_send()

    @pl.when(diag)
    def _():
        g_p().wait_send()
        for h in range(2):
            r_2(h).wait_send()
            r_3(h).wait_send()

    @pl.when(off)
    def _():
        r_p(r).wait_send()
        for n in range(NCH):
            g_y(n).wait_send()


def solution(mesh):
    def sweep(t_blk, d_blk, o_blk, v_blk, oooo, wd_blk, wx_blk):
        any_spec = pl.BlockSpec(memory_space=pl.ANY)
        vm = pltpu.VMEM
        return pl.pallas_call(
            kernel,
            out_shape=jax.ShapeDtypeStruct((ROWS, COLS), F32),
            in_specs=[any_spec] * 7,
            out_specs=any_spec,
            scratch_shapes=[
                vm((ROWS, COLS), F32),
                vm((ROWS, COLS), F32),
                vm((ROWS, COLS), BF16),
                vm((KPAD, COLS), BF16),
                vm((ROWS, 256), BF16),
                vm((OCC, 128, WIDE), BF16),
                vm((OCC * VIRT, WIDE), BF16),
                vm((ROWS, COLS), F32),
                vm((4, ROWS, COLS), BF16),
                vm((ROWS, COLS), BF16),
                vm((4, ROWS, KPAD), BF16),
                vm((VIRT * ZT, 128), F32),
                vm((ROWS, VIRT, 128), BF16),
                vm((4 * VIRT, OCC * 128), BF16),
                vm((4 * VIRT, WIDE), F32),
                vm((WIDE, 512), F32),
                vm((VIRT * ZS, 128), F32),
                vm((VIRT * ZS, 128), F32),
                vm((32, 2 * COLS), F32),
                vm((32, 2 * COLS), F32),
                vm((16, 2 * COLS), F32),
                vm((32, COLS), F32),
                vm((32, COLS), F32),
                vm((4, 4, 2, 8, COLS), F32),
                vm((4, 2, 8, COLS), F32),
                vm((4, 2, 8, COLS), F32),
                vm((4, 2, 8, COLS), F32),
                vm((ROWS, 256), F32),
                vm((ROWS, 256), F32),
                vm((4, ROWS, ROWS), BF16),
                vm((4, ROWS, ROWS), BF16),
                pltpu.SemaphoreType.DMA((7,)),
                pltpu.SemaphoreType.DMA((NCH,)),
                pltpu.SemaphoreType.DMA((N_SEM,)),
                pltpu.SemaphoreType.DMA((N_SEM,)),
            ],
            compiler_params=pltpu.CompilerParams(
                collective_id=0, has_side_effects=True, vmem_limit_bytes=60 * 1024 * 1024
            ),
            name="ccd_sweep",
        )(t_blk, d_blk, o_blk, v_blk, oooo, wd_blk.reshape(OCC, VIRT, WIDE), wx_blk)

    amp = P("row", "col")
    wide_spec = P(None, "col")
    return jax.shard_map(
        sweep, mesh=mesh, in_specs=(amp, amp, amp, amp, P(), wide_spec, wide_spec), out_specs=amp, check_vma=False
    )
```

```python
import functools

import jax
import jax.numpy as jnp
from jax import lax
from jax.experimental import pallas as pl
from jax.experimental.pallas import tpu as pltpu
from jax.sharding import PartitionSpec as P

MESH = pl.DeviceIdType.MESH
F32 = jnp.float32
BF16 = jnp.bfloat16

OCC = 16
VIRT = 80
ROWS = 64
COLS = 3200
KPAD = 1664
WIDE = 640
NCH = COLS // WIDE
ZS = 40

T_X, T_Y, T_P, T_FWD, R_P, R_X, R_Y, G_P = 0, 2, 4, 5, 7, 8, 10, 12
E_D, E_X, L_D, L_X, O_D, F_Y, G_Y = 13, 23, 33, 38, 43, 48, 58
X_Y, M_1, M_2, M_3 = 68, 69, 70, 71
N_SEM = 72


def split_segments(parts, lane):
    out = []
    for q in range(8):
        m, s = divmod(80 * q, 128)
        seg = parts[m]
        if s:
            seg = pltpu.roll(seg, 128 - s, axis=1)
            if s + 80 > 128:
                seg = jnp.where(lane < 128 - s, seg, pltpu.roll(parts[m + 1], 128 - s, axis=1))
        out.append(jnp.where(lane < 80, seg, 0.0))
    return out


def join_segments(segs, lane):
    r = [segs[0]] + [pltpu.roll(segs[q], (80 * q) % 128, axis=1) for q in range(1, 8)]
    return [
        jnp.where(lane < 80, r[0], r[1]),
        jnp.where(lane < 32, r[1], jnp.where(lane < 112, r[2], r[3])),
        jnp.where(lane < 64, r[3], r[4]),
        jnp.where(lane < 16, r[4], jnp.where(lane < 96, r[5], r[6])),
        jnp.where(lane < 48, r[6], r[7]),
    ]


def kernel(
    t_hbm, d_hbm, o_hbm, v_hbm, oooo_hbm, wd_hbm, wx_hbm, out_hbm,
    tf, dbuf, ov, vbuf, ob, wdp, wxb, obuf,
    tcol, ty, tr1, zt, tb, l3, r3o, r5o, zf, zg, fbuf, gbuf, gpart, frecv, grecv,
    xp, prx, pown, xrecv, xpart, xyrecv, msend, mfull,
    lsem, osem, ss, rs,
):
    r = lax.axis_index("row")
    c = lax.axis_index("col")
    k = lax.rem(r, 2)
    x = r // 2
    p1 = r + 1 - 2 * k
    p2 = lax.rem(r + 2, 4)
    p3 = lax.rem(p1 + 2, 4)
    diag = x == c
    off = x != c
    d_p, d_x, d_d, d_y, d_z = (c, p1), (c, p2), (c, p3), (1 - c, r), (1 - c, p1)
    other = 2 * (1 - x)
    own = 2 * x

    def rc(src, dst, slot, dev):
        return pltpu.make_async_remote_copy(
            src_ref=src, dst_ref=dst, send_sem=ss.at[slot], recv_sem=rs.at[slot],
            device_id=dev, device_id_type=MESH,
        )

    def wide(n, base=0):
        return pl.ds(pl.multiple_of(base + n * WIDE, 128), WIDE)

    ld_t = pltpu.make_async_copy(t_hbm, tf, lsem.at[0])
    ld_v = pltpu.make_async_copy(v_hbm, vbuf.at[pl.ds(pl.multiple_of(64 * k, 64), 1600)], lsem.at[1])
    ld_wd = pltpu.make_async_copy(wd_hbm, wdp.at[:, pl.ds(0, VIRT)], lsem.at[2])
    ld_wx = pltpu.make_async_copy(wx_hbm, wxb, lsem.at[3])
    ld_o = pltpu.make_async_copy(o_hbm, ov, lsem.at[4])
    ld_d = pltpu.make_async_copy(d_hbm, dbuf, lsem.at[5])
    ld_oooo = pltpu.make_async_copy(oooo_hbm.at[pl.ds(pl.multiple_of(ROWS * r, ROWS), ROWS)], ob, lsem.at[6])
    ld_t.start()

    barrier = pltpu.get_barrier_semaphore()
    for dev in (d_p, d_x, d_d, d_y, d_z):
        pl.semaphore_signal(barrier, inc=1, device_id=dev, device_id_type=MESH)
    for ld in (ld_wd, ld_wx, ld_v, ld_o, ld_oooo, ld_d):
        ld.start()
    ld_t.wait()

    @pl.loop(0, 4)
    def _(s):
        rows = pl.ds(pl.multiple_of(16 * s, 16), 16)
        tcol[r, rows] = tf[rows].astype(BF16)

    pl.semaphore_wait(barrier, 5)

    def half(h):
        return pl.ds(32 * h, 32)

    def t_x(h, blk):
        return rc(tcol.at[blk, half(h)], tcol.at[blk, half(h)], T_X + h, d_x)

    def t_y(h):
        return rc(tcol.at[r, half(h)], ty.at[half(h)], T_Y + h, d_y)

    def t_fwd(h, blk):
        return rc(tcol.at[blk, half(h)], tcol.at[blk, half(h)], T_FWD + h, d_p)

    def t_p(blk):
        return rc(tcol.at[blk], tcol.at[blk], T_P, d_p)

    def my_k(core):
        return pl.ds(pl.multiple_of(1536 * core, 128), KPAD)

    def r_p(blk):
        return rc(ty.at[:, my_k(1 - k)], tr1.at[blk], R_P, d_p)

    def r_x(cross_core):
        core, dev = (1 - k, d_d) if cross_core else (k, d_x)
        return rc(ty.at[half(0), my_k(core)], tr1.at[r, half(0)], R_X + cross_core, dev)

    def r_y(cross_core):
        core, dev = (1 - k, d_z) if cross_core else (k, d_y)
        return rc(tcol.at[p2, half(1), my_k(core)], tr1.at[p2, half(1)], R_Y + cross_core, dev)

    t_x(0, r).start()
    for h in range(2):
        t_y(h).start()

    @pl.when(off)
    def _():
        t_x(1, r).start()

    t_p(r).start()

    lane32 = lax.broadcasted_iota(jnp.int32, (32, 128), 1)
    lane80 = lax.broadcasted_iota(jnp.int32, (VIRT, 128), 1)
    vbuf[pl.ds(pl.multiple_of(1600 * (1 - k), 64), 64)] = jnp.zeros((64, COLS), BF16)
    wdp[:, pl.ds(VIRT, 48)] = jnp.zeros((OCC, 48, WIDE), BF16)

    def slabs(ref, h, col_half):
        @pl.loop(0, NCH)
        def _(g):
            parts = [
                ref[half(h), pl.ds(pl.multiple_of(g * WIDE + 128 * m, 128), 128)].astype(F32)
                for m in range(5)
            ]
            for q, seg in enumerate(split_segments(parts, lane32)):
                zt[h, pl.ds(pl.multiple_of((col_half * 40 + g * 8 + q) * ZS, 8), 32)] = seg

    def s_blocks(h):
        slabs(ty, h, 1 - c)
        for i in range(2):
            @pl.loop(0, OCC)
            def _(kk):
                blk = zt[h, pl.ds(i * OCC + kk, VIRT, stride=ZS)].astype(BF16)
                tb[i * OCC + kk] = blk
                l3[pl.ds(i * VIRT, VIRT), pl.ds(pl.multiple_of(kk * 128, 128), 128)] = blk

        if h == 0:
            ld_wd.wait()
        r3o[...] = jnp.dot(l3[...], wdp[...].reshape(OCC * 128, WIDE), preferred_element_type=F32)
        if h == 0:
            ld_wx.wait()
        rhs = jnp.concatenate([tb[pl.ds(i * OCC, OCC)].reshape(OCC * VIRT, 128) for i in range(2)], axis=1)
        r5o[...] = lax.dot_general(wxb[...], rhs, (((0,), (0,)), ((), ())), preferred_element_type=F32)

        @pl.loop(0, 2)
        def _(i):
            rows = pl.ds(pl.multiple_of(i * VIRT, 8), VIRT)
            parts = [r3o[rows, pl.ds(128 * m, 128)] for m in range(5)]
            for j, seg in enumerate(split_segments(parts, lane80)):
                s_ij = seg - r5o[pl.ds(j * VIRT, VIRT), pl.ds(pl.multiple_of(i * 128, 128), 128)]
                zf[pl.ds((j // 4) * 16 + (2 * h + i) * 4 + j % 4, VIRT, stride=ZS)] = s_ij
                s_ji = jnp.transpose(jnp.concatenate([s_ij, jnp.zeros((48, 128), F32)], axis=0))
                row = jnp.where(diag, j * 4 + 2 * h + i, h * 16 + j * 2 + i)
                zg[pl.ds(row, VIRT, stride=ZS)] = s_ji[:VIRT]

    def tile_at(base, n, m):
        return pl.ds(pl.multiple_of(base + n * WIDE + 128 * m, 128), 128)

    def slab(z, g, q, row, size):
        return z[pl.ds(pl.multiple_of((g * 8 + q) * ZS + row, 8), size)]

    def g_y(n, h):
        rows = pl.ds(16 * h, 16)
        return rc(gbuf.at[rows, wide(n, COLS * (1 - c))], grecv.at[rows, wide(n)], G_Y + NCH * h + n, d_y)

    def f_y(n, h):
        rows = pl.ds(8 * h, 8)
        return rc(fbuf.at[:, rows, wide(n, COLS * (1 - c))], frecv.at[:, rows, wide(n)], F_Y + NCH * h + n, d_y)

    def g_off(h):
        lane16 = lax.broadcasted_iota(jnp.int32, (16, 128), 1)
        rows = pl.ds(16 * h, 16)

        @pl.loop(0, NCH)
        def _(n):
            segs = [slab(zg, n + NCH * (1 - c), q, 16 * h, 16) for q in range(8)]
            for m, tile in enumerate(join_segments(segs, lane16)):
                gbuf[rows, tile_at(COLS * (1 - c), n, m)] = tile
            g_y(n, h).start()

        @pl.loop(0, NCH)
        def _(n):
            segs = [slab(zg, n + NCH * c, q, 16 * h, 16) for q in range(8)]
            for m, tile in enumerate(join_segments(segs, lane16)):
                grecv[rows, tile_at(0, n, m)] = tile

    def f_off(h, send):
        lane8 = lax.broadcasted_iota(jnp.int32, (8, 128), 1)
        rows = pl.ds(8 * h, 8)
        hf = 1 - c if send else c

        @pl.loop(0, NCH)
        def _(n):
            for b in range(2):
                segs = [slab(zf, n + NCH * hf, q, 16 * b + 8 * h, 8) for q in range(8)]
                for m, tile in enumerate(join_segments(segs, lane8)):
                    fbuf[b, rows, tile_at(COLS * hf, n, m)] = tile
            if send:
                f_y(n, h).start()

    def g_p():
        return rc(gbuf.at[pl.ds(pl.multiple_of(16 * (1 - k), 16), 16)], gpart, G_P, d_p)

    def q_diag():
        @pl.loop(0, 2 * NCH)
        def _(n):
            segs = [slab(zg, n, q, 0, 32) for q in range(8)]
            for m, tile in enumerate(join_segments(segs, lane32)):
                gbuf[:, tile_at(0, n, m)] = tile

        g_p().start()
        g_p().wait_recv()
        mine = pl.ds(pl.multiple_of(16 * k, 16), 16)

        for hf in (1 - c, c):
            @pl.loop(0, NCH)
            def _(n):
                segs = [slab(zf, n + NCH * hf, q, 0, 32) for q in range(8)]
                cols = wide(n, COLS * hf)
                for m, tile in enumerate(join_segments(segs, lane32)):
                    at = tile_at(COLS * hf, n, m)
                    fbuf[0, :, at] = tile[:16]
                    fbuf[1, :, at] = tile[16:]
                fbuf[k, :, cols] += gbuf[mine, cols]
                fbuf[1 - k, :, cols] += gpart[:, cols]
                if hf is not c:
                    for h in range(2):
                        f_y(n, h).start()

    for h in range(2):
        slabs(tf, h, c)

    def ladder_own(n):
        lhs = tr1[pl.ds(own, 2)].reshape(128, KPAD)
        prod = jnp.dot(lhs, vbuf[:, wide(n)], preferred_element_type=F32)
        xp[pl.ds(own, 2), :, :, :, wide(n)] = prod.reshape(2, 4, 2, 8, WIDE)

    early, late = 1 - x, x

    def pair_e(n, h):
        ts = pl.ds(2 * h, 2)
        return rc(xp.at[p3, ts, early, :, wide(n)], prx.at[ts, early, :, wide(n)], E_D + NCH * h + n, d_p)

    def cross_e(n, h, hf):
        ts = pl.ds(2 * h, 2)
        return rc(xp.at[p2, ts, hf, :, wide(n)], xrecv.at[ts, hf, :, wide(n)], E_X + NCH * h + n, d_x)

    def pair_l(n):
        return rc(xp.at[p3, :, late, :, wide(n)], prx.at[:, late, :, wide(n)], L_D + n, d_p)

    def cross_l(n, hf):
        return rc(xp.at[p2, :, hf, :, wide(n)], xrecv.at[:, hf, :, wide(n)], L_X + n, d_x)

    def ladder_other(h):
        @pl.loop(0, NCH)
        def _(n):
            lhs = tr1[pl.ds(other, 2), half(h)].reshape(64, KPAD)
            prod = jnp.dot(lhs, vbuf[:, wide(n)], preferred_element_type=F32)
            xp[pl.ds(other, 2), pl.ds(2 * h, 2), :, :, wide(n)] = prod.reshape(2, 2, 2, 8, WIDE)
            pair_e(n, h).start()

    def combine_e(h):
        @pl.loop(0, NCH)
        def _(n):
            ts = pl.ds(2 * h, 2)
            pair_e(n, h).wait_recv()
            xp[p2, ts, early, :, wide(n)] += prx[ts, early, :, wide(n)]
            cross_e(n, h, early).start()

    def combine_l(n):
        pair_l(n).wait_recv()
        xp[p2, :, late, :, wide(n)] += prx[:, late, :, wide(n)]
        cross_l(n, late).start()

    def x_y():
        return rc(xpart, xyrecv, X_Y, d_y)

    def x_part():
        xpart[...] = lax.dot_general(
            ov[...], tcol[...].reshape(4 * ROWS, COLS), (((1,), (1,)), ((), ())), preferred_element_type=F32
        )
        x_y().start()

    def take(h):
        tr1[pl.ds(other, 2), half(h)] = tcol[pl.ds(other, 2), half(h), my_k(k)]

    def send_m():
        x_y().wait_recv()
        m_rows = (ob[...].astype(F32) + 0.5 * (xpart[...] + xyrecv[...])).astype(BF16)
        for q in range(4):
            msend[q] = m_rows[:, q * ROWS:(q + 1) * ROWS]
        mfull[r] = msend[r]
        for cp in m_out():
            cp.start()

    def m_out():
        return (
            rc(msend.at[p1], mfull.at[r], M_1, d_p),
            rc(msend.at[p2], mfull.at[r], M_2, d_x),
            rc(msend.at[p3], mfull.at[r], M_3, d_d),
        )

    def m_in():
        return (
            rc(msend.at[p1], mfull.at[p1], M_1, d_p),
            rc(msend.at[p2], mfull.at[p2], M_2, d_x),
            rc(msend.at[p3], mfull.at[p3], M_3, d_d),
        )

    @pl.when(diag)
    def _():
        t_y(0).wait_recv()
        for q in range(2):
            r_x(q).start()
        t_x(1, r).start()
        t_x(0, p2).wait_recv()
        t_fwd(0, p2).start()
        t_fwd(0, p3).wait_recv()
        take(0)
        ld_v.wait()
        ladder_other(0)
        combine_e(0)
        t_x(1, p2).wait_recv()
        for q in range(2):
            r_y(q).start()
        t_fwd(1, p2).start()
        s_blocks(0)
        t_fwd(1, p3).wait_recv()
        take(1)
        ladder_other(1)
        combine_e(1)
        t_p(p1).wait_recv()
        tr1[r] = tcol[r, :, my_k(k)]
        tr1[p1] = tcol[p1, :, my_k(k)]
        ld_o.wait()
        x_part()
        t_y(1).wait_recv()
        s_blocks(1)
        q_diag()
        ld_oooo.wait()

    @pl.when(off)
    def _():
        t_y(0).wait_recv()
        s_blocks(0)
        g_off(0)
        t_x(0, p2).wait_recv()
        t_fwd(0, p2).start()
        f_off(0, True)
        ld_v.wait()
        for q in range(2):
            r_x(q).wait_recv()
        ladder_other(0)
        combine_e(0)
        t_y(1).wait_recv()
        r_p(r).start()
        tr1[r] = ty[:, my_k(k)]
        s_blocks(1)
        g_off(1)
        t_x(1, p2).wait_recv()
        t_fwd(1, p2).start()
        for q in range(2):
            r_y(q).wait_recv()
        ladder_other(1)
        combine_e(1)
        t_p(p1).wait_recv()
        for h in range(2):
            t_fwd(h, p3).wait_recv()
        ld_o.wait()
        x_part()
        f_off(1, True)
        ld_oooo.wait()
        send_m()
        for h in range(2):
            f_off(h, False)
        r_p(p1).wait_recv()

    def out_pair(n):
        return rc(xp.at[p1, :, :, :, wide(n)], pown.at[:, :, :, wide(n)], O_D + n, d_p)

    row8 = lax.broadcasted_iota(jnp.int32, (8, WIDE), 0)
    here = (row8 // 4) == k

    @pl.loop(0, NCH)
    def _(n):
        ladder_own(n)
        out_pair(n).start()

        @pl.when(diag)
        def _():
            for h in range(2):
                g_y(n, h).wait_recv()

        for b in range(2):
            for t in range(4):
                g2 = [grecv[pl.ds(16 * h + 8 * b + 2 * t, 2), wide(n)] for h in range(2)]
                g8 = jnp.where(here, jnp.concatenate(g2 + g2, axis=0), 0.0)
                xp[other + b, t, late, :, wide(n)] += g8
        pair_l(n).start()

        @pl.when(n > 0)
        def _():
            combine_l(n - 1)

    combine_l(NCH - 1)

    @pl.when(diag)
    def _():
        send_m()

    for cp in m_in():
        cp.wait_recv()
    ld_d.wait()

    def put(n):
        return pltpu.make_async_copy(obuf.at[:, wide(n)], out_hbm.at[:, wide(n)], osem.at[n])

    @pl.loop(0, NCH)
    def _(n):
        r2 = lax.dot_general(
            mfull[...].reshape(4 * ROWS, ROWS), tcol[:, :, wide(n)].reshape(4 * ROWS, WIDE),
            (((0,), (0,)), ((), ())), preferred_element_type=F32,
        )
        acc = ov[:, wide(n)].astype(F32) + r2
        out_pair(n).wait_recv()
        for h in range(2):
            f_y(n, h).wait_recv()
        for h in range(2):
            cross_e(n, h, x).wait_recv()
        cross_l(n, 1 - x).wait_recv()
        part = xp[r, :, :, :, wide(n)] + pown[:, :, :, wide(n)] + xrecv[:, :, :, wide(n)]
        acc = acc + part.reshape(ROWS, WIDE)
        obuf[:, wide(n)] = acc
        for i in range(4):
            for ref, hf, base in ((fbuf, c, COLS * c), (frecv, 1 - c, 0)):
                f8 = jnp.concatenate([ref[b, pl.ds(4 * i, 4), wide(n, base)] for b in range(2)], axis=0)
                rows = pl.ds(pl.multiple_of(16 * i + 8 * hf, 8), 8)
                obuf[rows, wide(n)] += f8
        obuf[:, wide(n)] = obuf[:, wide(n)] / dbuf[:, wide(n)]
        put(n).start()

    for n in range(NCH):
        put(n).wait()
        for h in range(2):
            f_y(n, h).wait_send()
        out_pair(n).wait_send()
        pair_l(n).wait_send()
        cross_l(n, late).wait_send()
        for h in range(2):
            pair_e(n, h).wait_send()
            cross_e(n, h, early).wait_send()
    for cp in m_out():
        cp.wait_send()
    x_y().wait_send()
    t_p(r).wait_send()
    for h in range(2):
        t_x(h, r).wait_send()
        t_y(h).wait_send()
        t_fwd(h, p2).wait_send()

    @pl.when(diag)
    def _():
        g_p().wait_send()
        for q in range(2):
            r_x(q).wait_send()
            r_y(q).wait_send()

    @pl.when(off)
    def _():
        r_p(r).wait_send()
        for n in range(NCH):
            for h in range(2):
                g_y(n, h).wait_send()


def solution(mesh):
    def sweep(t_blk, d_blk, o_blk, v_blk, oooo, wd_blk, wx_blk):
        any_spec = pl.BlockSpec(memory_space=pl.ANY)
        vm = pltpu.VMEM
        return pl.pallas_call(
            kernel,
            out_shape=jax.ShapeDtypeStruct((ROWS, COLS), F32),
            in_specs=[any_spec] * 7,
            out_specs=any_spec,
            scratch_shapes=[
                vm((ROWS, COLS), F32),
                vm((ROWS, COLS), F32),
                vm((ROWS, COLS), BF16),
                vm((KPAD, COLS), BF16),
                vm((ROWS, 256), BF16),
                vm((OCC, 128, WIDE), BF16),
                vm((OCC * VIRT, WIDE), BF16),
                vm((ROWS, COLS), F32),
                vm((4, ROWS, COLS), BF16),
                vm((ROWS, COLS), BF16),
                vm((4, ROWS, KPAD), BF16),
                vm((2, VIRT * ZS, 128), F32),
                vm((32, VIRT, 128), BF16),
                vm((2 * VIRT, OCC * 128), BF16),
                vm((2 * VIRT, WIDE), F32),
                vm((WIDE, 256), F32),
                vm((VIRT * ZS, 128), F32),
                vm((VIRT * ZS, 128), F32),
                vm((2, 16, 2 * COLS), F32),
                vm((32, 2 * COLS), F32),
                vm((16, 2 * COLS), F32),
                vm((2, 16, COLS), F32),
                vm((32, COLS), F32),
                vm((4, 4, 2, 8, COLS), F32),
                vm((4, 2, 8, COLS), F32),
                vm((4, 2, 8, COLS), F32),
                vm((4, 2, 8, COLS), F32),
                vm((ROWS, 256), F32),
                vm((ROWS, 256), F32),
                vm((4, ROWS, ROWS), BF16),
                vm((4, ROWS, ROWS), BF16),
                pltpu.SemaphoreType.DMA((7,)),
                pltpu.SemaphoreType.DMA((NCH,)),
                pltpu.SemaphoreType.DMA((N_SEM,)),
                pltpu.SemaphoreType.DMA((N_SEM,)),
            ],
            compiler_params=pltpu.CompilerParams(
                collective_id=0, has_side_effects=True, vmem_limit_bytes=60 * 1024 * 1024
            ),
            name="ccd_sweep",
        )(t_blk, d_blk, o_blk, v_blk, oooo, wd_blk.reshape(OCC, VIRT, WIDE), wx_blk)

    amp = P("row", "col")
    wide_spec = P(None, "col")
    return jax.shard_map(
        sweep, mesh=mesh, in_specs=(amp, amp, amp, amp, P(), wide_spec, wide_spec), out_specs=amp, check_vma=False
    )
```

```python
import functools

import jax
import jax.numpy as jnp
from jax import lax
from jax.experimental import pallas as pl
from jax.experimental.pallas import tpu as pltpu
from jax.sharding import PartitionSpec as P

MESH = pl.DeviceIdType.MESH
F32 = jnp.float32
BF16 = jnp.bfloat16

OCC = 16
VIRT = 80
ROWS = 64
COLS = 3200
KPAD = 1664
WIDE = 640
NCH = COLS // WIDE
ZS = 40

T_X, T_Y, T_P, T_FWD, R_P, R_X, R_Y, G_P = 0, 4, 8, 9, 13, 14, 18, 22
E_D, E_X, L_D, L_X, O_D, F_Y, G_Y = 23, 33, 43, 53, 63, 68, 78
X_Y, M_1, M_2, M_3 = 88, 89, 90, 91
N_SEM = 92


def split_segments(parts, lane):
    out = []
    for q in range(8):
        m, s = divmod(80 * q, 128)
        seg = parts[m]
        if s:
            seg = pltpu.roll(seg, 128 - s, axis=1)
            if s + 80 > 128:
                seg = jnp.where(lane < 128 - s, seg, pltpu.roll(parts[m + 1], 128 - s, axis=1))
        out.append(jnp.where(lane < 80, seg, 0.0))
    return out


def join_segments(segs, lane):
    r = [segs[0]] + [pltpu.roll(segs[q], (80 * q) % 128, axis=1) for q in range(1, 8)]
    return [
        jnp.where(lane < 80, r[0], r[1]),
        jnp.where(lane < 32, r[1], jnp.where(lane < 112, r[2], r[3])),
        jnp.where(lane < 64, r[3], r[4]),
        jnp.where(lane < 16, r[4], jnp.where(lane < 96, r[5], r[6])),
        jnp.where(lane < 48, r[6], r[7]),
    ]


def kernel(
    t_hbm, d_hbm, o_hbm, v_hbm, oooo_hbm, wd_hbm, wx_hbm, obuf,
    tf, dbuf, ov, vbuf, ob, wdp, wxb,
    tcol, ty, tr1, zt, tb, l3, r3o, r5o, zf, zg, fbuf, gbuf, gpart, frecv, grecv,
    xp, prx, pown, xrecv, xpart, xyrecv, msend, mfull,
    lsem, ss, rs,
):
    r = lax.axis_index("row")
    c = lax.axis_index("col")
    k = lax.rem(r, 2)
    x = r // 2
    p1 = r + 1 - 2 * k
    p2 = lax.rem(r + 2, 4)
    p3 = lax.rem(p1 + 2, 4)
    diag = x == c
    off = x != c
    d_p, d_x, d_d, d_y, d_z = (c, p1), (c, p2), (c, p3), (1 - c, r), (1 - c, p1)
    other = 2 * (1 - x)
    own = 2 * x

    def rc(src, dst, slot, dev):
        return pltpu.make_async_remote_copy(
            src_ref=src, dst_ref=dst, send_sem=ss.at[slot], recv_sem=rs.at[slot],
            device_id=dev, device_id_type=MESH,
        )

    def wide(n, base=0):
        return pl.ds(pl.multiple_of(base + n * WIDE, 128), WIDE)

    ld_t = pltpu.make_async_copy(t_hbm, tf, lsem.at[0])
    ld_v = pltpu.make_async_copy(v_hbm, vbuf.at[pl.ds(pl.multiple_of(64 * k, 64), 1600)], lsem.at[1])
    ld_wd = pltpu.make_async_copy(wd_hbm, wdp.at[:, pl.ds(0, VIRT)], lsem.at[2])
    ld_wx = pltpu.make_async_copy(wx_hbm, wxb, lsem.at[3])
    ld_o = pltpu.make_async_copy(o_hbm, ov, lsem.at[4])
    ld_d = pltpu.make_async_copy(d_hbm, dbuf, lsem.at[5])
    ld_oooo = pltpu.make_async_copy(oooo_hbm.at[pl.ds(pl.multiple_of(ROWS * r, ROWS), ROWS)], ob, lsem.at[6])
    ld_t.start()

    barrier = pltpu.get_barrier_semaphore()
    for dev in (d_p, d_x, d_d, d_y, d_z):
        pl.semaphore_signal(barrier, inc=1, device_id=dev, device_id_type=MESH)
    for ld in (ld_wd, ld_wx, ld_v, ld_o, ld_oooo, ld_d):
        ld.start()
    ld_t.wait()

    @pl.loop(0, 4)
    def _(s):
        rows = pl.ds(pl.multiple_of(16 * s, 16), 16)
        tcol[r, rows] = tf[rows].astype(BF16)

    pl.semaphore_wait(barrier, 5)

    def half(h):
        return pl.ds(32 * h, 32)

    def quarter(q):
        return pl.ds(16 * q, 16)

    def t_x(q, blk):
        return rc(tcol.at[blk, quarter(q)], tcol.at[blk, quarter(q)], T_X + q, d_x)

    def t_y(q):
        return rc(tcol.at[r, quarter(q)], ty.at[quarter(q)], T_Y + q, d_y)

    def t_fwd(q, blk):
        return rc(tcol.at[blk, quarter(q)], tcol.at[blk, quarter(q)], T_FWD + q, d_p)

    def t_p(blk):
        return rc(tcol.at[blk], tcol.at[blk], T_P, d_p)

    def my_k(core):
        return pl.ds(pl.multiple_of(1536 * core, 128), KPAD)

    def r_p(blk):
        return rc(ty.at[:, my_k(1 - k)], tr1.at[blk], R_P, d_p)

    def r_x(q, cross_core):
        core, dev = (1 - k, d_d) if cross_core else (k, d_x)
        return rc(ty.at[quarter(q), my_k(core)], tr1.at[r, quarter(q)], R_X + 2 * q + cross_core, dev)

    def r_y(q, cross_core):
        core, dev = (1 - k, d_z) if cross_core else (k, d_y)
        return rc(tcol.at[p2, quarter(q), my_k(core)], tr1.at[p2, quarter(q)], R_Y + 2 * (q - 2) + cross_core, dev)

    for q in range(2):
        t_x(q, r).start()
        t_y(q).start()
    for q in range(2, 4):
        t_y(q).start()

    @pl.when(off)
    def _():
        for q in range(2, 4):
            t_x(q, r).start()

    t_p(r).start()

    lane32 = lax.broadcasted_iota(jnp.int32, (32, 128), 1)
    lane80 = lax.broadcasted_iota(jnp.int32, (VIRT, 128), 1)
    vbuf[pl.ds(pl.multiple_of(1600 * (1 - k), 64), 64)] = jnp.zeros((64, COLS), BF16)
    wdp[:, pl.ds(VIRT, 48)] = jnp.zeros((OCC, 48, WIDE), BF16)

    def slabs(ref, h, col_half):
        @pl.loop(0, NCH)
        def _(g):
            parts = [
                ref[half(h), pl.ds(pl.multiple_of(g * WIDE + 128 * m, 128), 128)].astype(F32)
                for m in range(5)
            ]
            for q, seg in enumerate(split_segments(parts, lane32)):
                zt[h, pl.ds(pl.multiple_of((col_half * 40 + g * 8 + q) * ZS, 8), 32)] = seg

    def s_blocks(h):
        slabs(ty, h, 1 - c)
        for i in range(2):
            @pl.loop(0, OCC)
            def _(kk):
                blk = zt[h, pl.ds(i * OCC + kk, VIRT, stride=ZS)].astype(BF16)
                tb[i * OCC + kk] = blk
                l3[pl.ds(i * VIRT, VIRT), pl.ds(pl.multiple_of(kk * 128, 128), 128)] = blk

        if h == 0:
            ld_wd.wait()
        r3o[...] = jnp.dot(l3[...], wdp[...].reshape(OCC * 128, WIDE), preferred_element_type=F32)
        if h == 0:
            ld_wx.wait()
        rhs = jnp.concatenate([tb[pl.ds(i * OCC, OCC)].reshape(OCC * VIRT, 128) for i in range(2)], axis=1)
        r5o[...] = lax.dot_general(wxb[...], rhs, (((0,), (0,)), ((), ())), preferred_element_type=F32)

        @pl.loop(0, 2)
        def _(i):
            rows = pl.ds(pl.multiple_of(i * VIRT, 8), VIRT)
            parts = [r3o[rows, pl.ds(128 * m, 128)] for m in range(5)]
            for j, seg in enumerate(split_segments(parts, lane80)):
                s_ij = seg - r5o[pl.ds(j * VIRT, VIRT), pl.ds(pl.multiple_of(i * 128, 128), 128)]
                zf[pl.ds((j // 4) * 16 + (2 * h + i) * 4 + j % 4, VIRT, stride=ZS)] = s_ij
                s_ji = jnp.transpose(jnp.concatenate([s_ij, jnp.zeros((48, 128), F32)], axis=0))
                row = jnp.where(diag, j * 4 + 2 * h + i, h * 16 + j * 2 + i)
                zg[pl.ds(row, VIRT, stride=ZS)] = s_ji[:VIRT]

    def tile_at(base, n, m):
        return pl.ds(pl.multiple_of(base + n * WIDE + 128 * m, 128), 128)

    def slab(z, g, q, row, size):
        return z[pl.ds(pl.multiple_of((g * 8 + q) * ZS + row, 8), size)]

    def g_y(n, h):
        rows = pl.ds(16 * h, 16)
        return rc(gbuf.at[rows, wide(n, COLS * (1 - c))], grecv.at[rows, wide(n)], G_Y + NCH * h + n, d_y)

    def f_y(n, h):
        rows = pl.ds(8 * h, 8)
        return rc(fbuf.at[:, rows, wide(n, COLS * (1 - c))], frecv.at[:, rows, wide(n)], F_Y + NCH * h + n, d_y)

    def g_off(h):
        lane16 = lax.broadcasted_iota(jnp.int32, (16, 128), 1)
        rows = pl.ds(16 * h, 16)

        @pl.loop(0, NCH)
        def _(n):
            segs = [slab(zg, n + NCH * (1 - c), q, 16 * h, 16) for q in range(8)]
            for m, tile in enumerate(join_segments(segs, lane16)):
                gbuf[rows, tile_at(COLS * (1 - c), n, m)] = tile
            g_y(n, h).start()

        @pl.loop(0, NCH)
        def _(n):
            segs = [slab(zg, n + NCH * c, q, 16 * h, 16) for q in range(8)]
            for m, tile in enumerate(join_segments(segs, lane16)):
                grecv[rows, tile_at(0, n, m)] = tile

    def f_off(h, send):
        lane8 = lax.broadcasted_iota(jnp.int32, (8, 128), 1)
        rows = pl.ds(8 * h, 8)
        hf = 1 - c if send else c

        @pl.loop(0, NCH)
        def _(n):
            for b in range(2):
                segs = [slab(zf, n + NCH * hf, q, 16 * b + 8 * h, 8) for q in range(8)]
                for m, tile in enumerate(join_segments(segs, lane8)):
                    fbuf[b, rows, tile_at(COLS * hf, n, m)] = tile
            if send:
                f_y(n, h).start()

    def g_p():
        return rc(gbuf.at[pl.ds(pl.multiple_of(16 * (1 - k), 16), 16)], gpart, G_P, d_p)

    def q_diag():
        @pl.loop(0, 2 * NCH)
        def _(n):
            segs = [slab(zg, n, q, 0, 32) for q in range(8)]
            for m, tile in enumerate(join_segments(segs, lane32)):
                gbuf[:, tile_at(0, n, m)] = tile

        g_p().start()

        def flat(hf):
            @pl.loop(0, NCH)
            def _(n):
                segs = [slab(zf, n + NCH * hf, q, 0, 32) for q in range(8)]
                for m, tile in enumerate(join_segments(segs, lane32)):
                    at = tile_at(COLS * hf, n, m)
                    fbuf[0, :, at] = tile[:16]
                    fbuf[1, :, at] = tile[16:]

        def add(hf, send):
            mine = pl.ds(pl.multiple_of(16 * k, 16), 16)

            @pl.loop(0, NCH)
            def _(n):
                cols = wide(n, COLS * hf)
                fbuf[k, :, cols] += gbuf[mine, cols]
                fbuf[1 - k, :, cols] += gpart[:, cols]
                if send:
                    for h in range(2):
                        f_y(n, h).start()

        flat(1 - c)
        flat(c)
        g_p().wait_recv()
        add(1 - c, True)
        add(c, False)

    for h in range(2):
        slabs(tf, h, c)

    early, late = 1 - x, x

    def pair_e(n, h):
        ts = pl.ds(2 * h, 2)
        return rc(xp.at[p3, ts, early, :, wide(n)], prx.at[ts, early, :, wide(n)], E_D + NCH * h + n, d_p)

    def cross_e(n, h, hf):
        ts = pl.ds(2 * h, 2)
        return rc(xp.at[p2, ts, hf, :, wide(n)], xrecv.at[ts, hf, :, wide(n)], E_X + NCH * h + n, d_x)

    def pair_l(n, h):
        ts = pl.ds(2 * h, 2)
        return rc(xp.at[p3, ts, late, :, wide(n)], prx.at[ts, late, :, wide(n)], L_D + NCH * h + n, d_p)

    def cross_l(n, h, hf):
        ts = pl.ds(2 * h, 2)
        return rc(xp.at[p2, ts, hf, :, wide(n)], xrecv.at[ts, hf, :, wide(n)], L_X + NCH * h + n, d_x)

    def over_columns(step):
        @pl.loop(0, 2)
        def _(g):
            step(pl.ds(pl.multiple_of(g * 2 * WIDE, 128), 2 * WIDE), (2 * g, 2 * g + 1))

        step(pl.ds(4 * WIDE, WIDE), (4,))

    def ladder_0():
        def step(cols, ns):
            lhs = tr1[pl.ds(other, 2), half(0)].reshape(64, KPAD)
            prod = jnp.dot(lhs, vbuf[:, cols], preferred_element_type=F32)
            xp[pl.ds(other, 2), pl.ds(0, 2), :, :, cols] = prod.reshape(2, 2, 2, 8, -1)
            for n in ns:
                pair_e(n, 0).start()

        over_columns(step)

    def ladder_1():
        def step(cols, ns):
            lhs = jnp.concatenate(
                [tr1[pl.ds(other, 2), half(1)].reshape(64, KPAD), tr1[pl.ds(own, 2)].reshape(128, KPAD)], axis=0
            )
            prod = jnp.dot(lhs, vbuf[:, cols], preferred_element_type=F32)
            xp[pl.ds(other, 2), pl.ds(2, 2), :, :, cols] = prod[:64].reshape(2, 2, 2, 8, -1)
            xp[pl.ds(own, 2), :, :, :, cols] = prod[64:].reshape(2, 4, 2, 8, -1)
            for n in ns:
                pair_e(n, 1).start()
                out_pair(n).start()

        over_columns(step)

    def combine_e(h):
        @pl.loop(0, NCH)
        def _(n):
            ts = pl.ds(2 * h, 2)
            pair_e(n, h).wait_recv()
            xp[p2, ts, early, :, wide(n)] += prx[ts, early, :, wide(n)]
            cross_e(n, h, early).start()

    def combine_l(n, h):
        ts = pl.ds(2 * h, 2)
        pair_l(n, h).wait_recv()
        xp[p2, ts, late, :, wide(n)] += prx[ts, late, :, wide(n)]
        cross_l(n, h, late).start()

    def out_pair(n):
        return rc(xp.at[p1, :, :, :, wide(n)], pown.at[:, :, :, wide(n)], O_D + n, d_p)

    row8 = lax.broadcasted_iota(jnp.int32, (8, WIDE), 0)
    here = (row8 // 4) == k

    def late_pass(hs, wait_g):
        @pl.loop(0, NCH)
        def _(n):
            if wait_g:
                for hh in range(2):
                    g_y(n, hh).wait_recv()
            for h in hs:
                for b in range(2):
                    for t in (2 * h, 2 * h + 1):
                        g2 = [grecv[pl.ds(16 * hh + 8 * b + 2 * t, 2), wide(n)] for hh in range(2)]
                        g8 = jnp.where(here, jnp.concatenate(g2 + g2, axis=0), 0.0)
                        xp[other + b, t, late, :, wide(n)] += g8
                pair_l(n, h).start()

            @pl.when(n > 0)
            def _():
                for h in hs:
                    combine_l(n - 1, h)

        for h in hs:
            combine_l(NCH - 1, h)

    def x_y():
        return rc(xpart, xyrecv, X_Y, d_y)

    def x_part():
        xpart[...] = lax.dot_general(
            ov[...], tcol[...].reshape(4 * ROWS, COLS), (((1,), (1,)), ((), ())), preferred_element_type=F32
        )
        x_y().start()

    def take(h):
        tr1[pl.ds(other, 2), half(h)] = tcol[pl.ds(other, 2), half(h), my_k(k)]

    def send_m():
        x_y().wait_recv()
        m_rows = (ob[...].astype(F32) + 0.5 * (xpart[...] + xyrecv[...])).astype(BF16)
        for q in range(4):
            msend[q] = m_rows[:, q * ROWS:(q + 1) * ROWS]
        mfull[r] = msend[r]
        for cp in m_out():
            cp.start()

    def m_out():
        return (
            rc(msend.at[p1], mfull.at[r], M_1, d_p),
            rc(msend.at[p2], mfull.at[r], M_2, d_x),
            rc(msend.at[p3], mfull.at[r], M_3, d_d),
        )

    def m_in():
        return (
            rc(msend.at[p1], mfull.at[p1], M_1, d_p),
            rc(msend.at[p2], mfull.at[p2], M_2, d_x),
            rc(msend.at[p3], mfull.at[p3], M_3, d_d),
        )

    @pl.when(diag)
    def _():
        for q in range(2):
            t_y(q).wait_recv()
            for cc in range(2):
                r_x(q, cc).start()
            t_x(q, p2).wait_recv()
            t_fwd(q, p2).start()
        for q in range(2, 4):
            t_x(q, r).start()
        for q in range(2):
            t_fwd(q, p3).wait_recv()
        take(0)
        ld_v.wait()
        ladder_0()
        combine_e(0)
        t_x(2, p2).wait_recv()
        t_fwd(2, p2).start()
        for cc in range(2):
            r_y(2, cc).start()
        s_blocks(0)
        t_x(3, p2).wait_recv()
        t_fwd(3, p2).start()
        for cc in range(2):
            r_y(3, cc).start()
        t_p(p1).wait_recv()
        tr1[r] = tcol[r, :, my_k(k)]
        tr1[p1] = tcol[p1, :, my_k(k)]
        for q in range(2, 4):
            t_fwd(q, p3).wait_recv()
        take(1)
        ladder_1()
        combine_e(1)
        ld_o.wait()
        x_part()
        for q in range(2, 4):
            t_y(q).wait_recv()
        s_blocks(1)
        q_diag()
        ld_oooo.wait()
        send_m()
        late_pass((0, 1), True)

    @pl.when(off)
    def _():
        for q in range(2):
            t_y(q).wait_recv()
        s_blocks(0)
        g_off(0)
        for q in range(2):
            t_x(q, p2).wait_recv()
            t_fwd(q, p2).start()
        for q in range(2, 4):
            t_y(q).wait_recv()
        r_p(r).start()
        tr1[r] = ty[:, my_k(k)]
        s_blocks(1)
        g_off(1)
        ld_v.wait()
        for q in range(2):
            for cc in range(2):
                r_x(q, cc).wait_recv()
        ladder_0()
        combine_e(0)
        late_pass((0,), False)
        for q in range(2, 4):
            t_x(q, p2).wait_recv()
            t_fwd(q, p2).start()
        t_p(p1).wait_recv()
        for q in range(4):
            t_fwd(q, p3).wait_recv()
        ld_o.wait()
        x_part()
        f_off(0, True)
        for q in range(2, 4):
            for cc in range(2):
                r_y(q, cc).wait_recv()
        r_p(p1).wait_recv()
        ladder_1()
        ld_oooo.wait()
        send_m()
        combine_e(1)
        f_off(1, True)
        late_pass((1,), False)
        for h in range(2):
            f_off(h, False)

    for cp in m_in():
        cp.wait_recv()
    ld_d.wait()

    @pl.loop(0, NCH)
    def _(n):
        r2 = lax.dot_general(
            mfull[...].reshape(4 * ROWS, ROWS), tcol[:, :, wide(n)].reshape(4 * ROWS, WIDE),
            (((0,), (0,)), ((), ())), preferred_element_type=F32,
        )
        acc = ov[:, wide(n)].astype(F32) + r2
        out_pair(n).wait_recv()
        for h in range(2):
            f_y(n, h).wait_recv()
        for h in range(2):
            cross_e(n, h, x).wait_recv()
            cross_l(n, h, 1 - x).wait_recv()
        part = xp[r, :, :, :, wide(n)] + pown[:, :, :, wide(n)] + xrecv[:, :, :, wide(n)]
        acc = acc + part.reshape(ROWS, WIDE)
        obuf[:, wide(n)] = acc
        for i in range(4):
            for ref, hf, base in ((fbuf, c, COLS * c), (frecv, 1 - c, 0)):
                f8 = jnp.concatenate([ref[b, pl.ds(4 * i, 4), wide(n, base)] for b in range(2)], axis=0)
                rows = pl.ds(pl.multiple_of(16 * i + 8 * hf, 8), 8)
                obuf[rows, wide(n)] += f8
        obuf[:, wide(n)] = obuf[:, wide(n)] / dbuf[:, wide(n)]

    for n in range(NCH):
        out_pair(n).wait_send()
        for h in range(2):
            f_y(n, h).wait_send()
            pair_l(n, h).wait_send()
            cross_l(n, h, late).wait_send()
            pair_e(n, h).wait_send()
            cross_e(n, h, early).wait_send()
    for cp in m_out():
        cp.wait_send()
    x_y().wait_send()
    t_p(r).wait_send()
    for q in range(4):
        t_x(q, r).wait_send()
        t_y(q).wait_send()
        t_fwd(q, p2).wait_send()

    @pl.when(diag)
    def _():
        g_p().wait_send()
        for q in range(2):
            for cc in range(2):
                r_x(q, cc).wait_send()
                r_y(q + 2, cc).wait_send()

    @pl.when(off)
    def _():
        r_p(r).wait_send()
        for n in range(NCH):
            for h in range(2):
                g_y(n, h).wait_send()


def solution(mesh):
    def sweep(t_blk, d_blk, o_blk, v_blk, oooo, wd_blk, wx_blk):
        any_spec = pl.BlockSpec(memory_space=pl.ANY)
        vm = pltpu.VMEM
        return pl.pallas_call(
            kernel,
            out_shape=pltpu.VMEM((ROWS, COLS), F32),
            in_specs=[any_spec] * 7,
            out_specs=pl.BlockSpec(memory_space=pltpu.VMEM),
            scratch_shapes=[
                vm((ROWS, COLS), F32),
                vm((ROWS, COLS), F32),
                vm((ROWS, COLS), BF16),
                vm((KPAD, COLS), BF16),
                vm((ROWS, 256), BF16),
                vm((OCC, 128, WIDE), BF16),
                vm((OCC * VIRT, WIDE), BF16),
                vm((4, ROWS, COLS), BF16),
                vm((ROWS, COLS), BF16),
                vm((4, ROWS, KPAD), BF16),
                vm((2, VIRT * ZS, 128), F32),
                vm((32, VIRT, 128), BF16),
                vm((2 * VIRT, OCC * 128), BF16),
                vm((2 * VIRT, WIDE), F32),
                vm((WIDE, 256), F32),
                vm((VIRT * ZS, 128), F32),
                vm((VIRT * ZS, 128), F32),
                vm((2, 16, 2 * COLS), F32),
                vm((32, 2 * COLS), F32),
                vm((16, 2 * COLS), F32),
                vm((2, 16, COLS), F32),
                vm((32, COLS), F32),
                vm((4, 4, 2, 8, COLS), F32),
                vm((4, 2, 8, COLS), F32),
                vm((4, 2, 8, COLS), F32),
                vm((4, 2, 8, COLS), F32),
                vm((ROWS, 256), F32),
                vm((ROWS, 256), F32),
                vm((4, ROWS, ROWS), BF16),
                vm((4, ROWS, ROWS), BF16),
                pltpu.SemaphoreType.DMA((7,)),
                pltpu.SemaphoreType.DMA((N_SEM,)),
                pltpu.SemaphoreType.DMA((N_SEM,)),
            ],
            compiler_params=pltpu.CompilerParams(
                collective_id=0, has_side_effects=True, vmem_limit_bytes=54 * 1024 * 1024
            ),
            name="ccd_sweep",
        )(t_blk, d_blk, o_blk, v_blk, oooo, wd_blk.reshape(OCC, VIRT, WIDE), wx_blk)

    amp = P("row", "col")
    wide_spec = P(None, "col")
    return jax.shard_map(
        sweep, mesh=mesh, in_specs=(amp, amp, amp, amp, P(), wide_spec, wide_spec), out_specs=amp, check_vma=False
    )
```

```python
import functools

import jax
import jax.numpy as jnp
from jax import lax
from jax.experimental import pallas as pl
from jax.experimental.pallas import tpu as pltpu
from jax.sharding import PartitionSpec as P

MESH = pl.DeviceIdType.MESH
F32 = jnp.float32
BF16 = jnp.bfloat16

OCC = 16
VIRT = 80
ROWS = 64
COLS = 3200
KPAD = 1664
WIDE = 640
NCH = COLS // WIDE
ZS = 40

T_X, T_Y, T_P, T_FWD, R_P, G_P, R_X, R_Y, G_Y = 0, 4, 7, 8, 10, 10, 11, 13, 11
E_D, L_D, O_D, E_X, L_X, F_Y, X_Y, M_1, M_2, M_3 = 17, 19, 21, 22, 23, 27, 29, 30, 31, 32
N_RECV = 33
S_TX, S_TY, S_TP, S_FWD, S_R, S_PAIR, S_OUT, S_X, S_F, S_G, S_XY, S_M = range(12)
N_SEND = 12


def split_segments(parts, lane):
    out = []
    for q in range(8):
        m, s = divmod(80 * q, 128)
        seg = parts[m]
        if s:
            seg = pltpu.roll(seg, 128 - s, axis=1)
            if s + 80 > 128:
                seg = jnp.where(lane < 128 - s, seg, pltpu.roll(parts[m + 1], 128 - s, axis=1))
        out.append(jnp.where(lane < 80, seg, 0.0))
    return out


def join_segments(segs, lane):
    r = [segs[0]] + [pltpu.roll(segs[q], (80 * q) % 128, axis=1) for q in range(1, 8)]
    return [
        jnp.where(lane < 80, r[0], r[1]),
        jnp.where(lane < 32, r[1], jnp.where(lane < 112, r[2], r[3])),
        jnp.where(lane < 64, r[3], r[4]),
        jnp.where(lane < 16, r[4], jnp.where(lane < 96, r[5], r[6])),
        jnp.where(lane < 48, r[6], r[7]),
    ]


def kernel(
    t_hbm, d_hbm, o_hbm, v_hbm, oooo_hbm, wd_hbm, wx_hbm, obuf,
    tf, dbuf, ov, vbuf, ob, wdp, wxb,
    tcol, ty, tr1, zt, wxs, tb, l3, r3a, r3b, r5a, r5b, zf, zg, gps, gpz, fbuf, gbuf, frecv, grecv,
    xp, prx, pown, xrecv, xpart, xyrecv, msend, mfull,
    lsem, ss, rs,
):
    r = lax.axis_index("row")
    c = lax.axis_index("col")
    k = lax.rem(r, 2)
    x = r // 2
    p1 = r + 1 - 2 * k
    p2 = lax.rem(r + 2, 4)
    p3 = lax.rem(p1 + 2, 4)
    diag = x == c
    off = x != c
    d_p, d_x, d_d, d_y, d_z = (c, p1), (c, p2), (c, p3), (1 - c, r), (1 - c, p1)
    other = 2 * (1 - x)
    own = 2 * x

    def rc(src, dst, leave, arrive, dev):
        return pltpu.make_async_remote_copy(
            src_ref=src, dst_ref=dst, send_sem=ss.at[leave], recv_sem=rs.at[arrive],
            device_id=dev, device_id_type=MESH,
        )

    def wide(n, base=0):
        return pl.ds(pl.multiple_of(base + n * WIDE, 128), WIDE)

    def half(h):
        return pl.ds(32 * h, 32)

    def quarter(q):
        return pl.ds(16 * q, 16)

    def ld_t(q):
        return pltpu.make_async_copy(t_hbm.at[quarter(q)], tf.at[quarter(q)], lsem.at[q])

    ld_v = pltpu.make_async_copy(v_hbm, vbuf.at[pl.ds(pl.multiple_of(64 * k, 64), 1600)], lsem.at[4])
    ld_wd = pltpu.make_async_copy(wd_hbm, wdp.at[:, pl.ds(0, VIRT)], lsem.at[5])
    ld_wx = pltpu.make_async_copy(wx_hbm, wxb, lsem.at[6])
    ld_o = pltpu.make_async_copy(o_hbm, ov, lsem.at[7])
    ld_d = pltpu.make_async_copy(d_hbm, dbuf, lsem.at[8])
    ld_oooo = pltpu.make_async_copy(oooo_hbm.at[pl.ds(pl.multiple_of(ROWS * r, ROWS), ROWS)], ob, lsem.at[9])
    for q in range(4):
        ld_t(q).start()

    barrier = pltpu.get_barrier_semaphore()
    for dev in (d_p, d_x, d_d, d_y, d_z):
        pl.semaphore_signal(barrier, inc=1, device_id=dev, device_id_type=MESH)
    for ld in (ld_wx, ld_wd, ld_v, ld_o, ld_oooo, ld_d):
        ld.start()

    def t_x(q, blk):
        return rc(tcol.at[blk, quarter(q)], tcol.at[blk, quarter(q)], S_TX, T_X + q, d_x)

    def t_y(q):
        return rc(tcol.at[r, quarter(q)], ty.at[quarter(q)], S_TY, T_Y + min(q, 2), d_y)

    def t_y_in():
        return rc(tcol.at[r, half(1)], ty.at[half(1)], S_TY, T_Y + 2, d_y)

    def t_fwd(q):
        return rc(tcol.at[p2, quarter(q)], tcol.at[p2, quarter(q)], S_FWD, T_FWD + q // 2, d_p)

    def t_fwd_in(h):
        return rc(tcol.at[p3, half(h)], tcol.at[p3, half(h)], S_FWD, T_FWD + h, d_p)

    def t_p(blk):
        return rc(tcol.at[blk], tcol.at[blk], S_TP, T_P, d_p)

    def my_k(core):
        return pl.ds(pl.multiple_of(1536 * core, 128), KPAD)

    def r_p(blk):
        return rc(ty.at[:, my_k(1 - k)], tr1.at[blk], S_R, R_P, d_p)

    def r_x(core):
        slot = R_X + lax.rem(k + core, 2)
        return rc(ty.at[quarter(0), my_k(core)], tr1.at[r, quarter(0)], S_R, slot, (c, other + core))

    def r_y(q, core):
        slot = R_Y + 2 * (q > 1) + lax.rem(k + core, 2)
        return rc(tcol.at[p2, quarter(q), my_k(core)], tr1.at[p2, quarter(q)], S_R, slot, (1 - c, own + core))

    def r_y_in(core):
        slot = R_Y + 2 + lax.rem(k + core, 2)
        return rc(tr1.at[p2, half(1)], tr1.at[p2, half(1)], S_R, slot, (1 - c, own + core))

    for q in range(4):
        ld_t(q).wait()
        tcol[r, quarter(q)] = tf[quarter(q)].astype(BF16)
        if q == 0:
            pl.semaphore_wait(barrier, 5)
        if q < 2:
            t_x(q, r).start()
        else:
            pl.when(off)(t_x(q, r).start)
        if q < 3:
            t_y(q).start()
        else:
            pl.when(off)(t_y(q).start)
    t_p(r).start()

    lane32 = lax.broadcasted_iota(jnp.int32, (32, 128), 1)
    lane40 = lax.broadcasted_iota(jnp.int32, (40, 128), 1)
    lane16 = lax.broadcasted_iota(jnp.int32, (16, 128), 1)
    vbuf[pl.ds(pl.multiple_of(1600 * (1 - k), 64), 64)] = jnp.zeros((64, COLS), BF16)
    wdp[:, pl.ds(VIRT, 48)] = jnp.zeros((OCC, 48, WIDE), BF16)

    def slabs(ref, h, col_half):
        @pl.loop(0, NCH)
        def _(g):
            parts = [
                ref[half(h), pl.ds(pl.multiple_of(g * WIDE + 128 * m, 128), 128)].astype(F32)
                for m in range(5)
            ]
            for q, seg in enumerate(split_segments(parts, lane32)):
                zt[h, pl.ds(pl.multiple_of((col_half * 40 + g * 8 + q) * ZS, 8), 32)] = seg

    def regroup(h, vh, l3_rows, tb_at):
        def rows(ik):
            return zt[h, pl.ds(40 * ZS * vh + ik, 40, stride=ZS)]

        @pl.loop(0, OCC)
        def _(kk):
            blk = jnp.concatenate([rows(kk), rows(OCC + kk)], axis=0).astype(BF16)
            l3[l3_rows, pl.ds(pl.multiple_of(kk * 128, 128), 128)] = blk

        for i in range(2):
            @pl.loop(0, OCC // 2)
            def _(k2):
                blk = jnp.concatenate([rows(i * OCC + 2 * k2), rows(i * OCC + 2 * k2 + 1)], axis=0).astype(BF16)
                tb[tb_at + i, pl.ds(pl.multiple_of(k2 * VIRT, 16), VIRT)] = blk

    def r3(rows):
        return jnp.dot(l3[rows], wdp[...].reshape(OCC * 128, WIDE), preferred_element_type=F32)

    def r5(vh, first, count):
        rhs = jnp.concatenate([tb[first + i] for i in range(count)], axis=1)
        return lax.dot_general(wxs[vh], rhs, (((0,), (0,)), ((), ())), preferred_element_type=F32)

    def s_before():
        for h in range(2):
            slabs(tf, h, c)
        ld_wx.wait()

        @pl.loop(0, OCC // 2)
        def _(k2):
            w = [wxb[2 * k2 + e].astype(F32) for e in range(2)]
            at = pl.ds(pl.multiple_of(k2 * VIRT, 16), VIRT)
            for vh in range(2):
                part = [w[e][40 * vh:40 * vh + 40] for e in range(2)]
                wxs[vh, at] = jnp.concatenate(part, axis=0).astype(BF16)

        for h in range(2):
            regroup(h, c, pl.ds(VIRT * h, VIRT), 2 * h)
        ld_wd.wait()
        r3a[...] = r3(pl.ds(0, 2 * VIRT))
        r5a[...] = r5(c, 0, 4)

    def s_prep(h):
        slabs(ty, h, 1 - c)
        regroup(h, 1 - c, pl.ds(0, VIRT), 0)

    def s_blocks(h):
        r3b[...] = r3(pl.ds(0, VIRT))
        r5b[...] = r5a[:, 256 * h:256 * h + 256] + r5(1 - c, 0, 2)

        @pl.loop(0, 2)
        def _(i):
            rows_a = pl.ds(pl.multiple_of(VIRT * h + 40 * i, 8), 40)
            rows_b = pl.ds(pl.multiple_of(40 * i, 8), 40)
            seg_a = split_segments([r3a[rows_a, pl.ds(128 * m, 128)] for m in range(5)], lane40)
            seg_b = split_segments([r3b[rows_b, pl.ds(128 * m, 128)] for m in range(5)], lane40)
            lanes = pl.ds(pl.multiple_of(i * 128, 128), 128)
            for j in range(8):
                s_a = seg_a[j] - r5b[pl.ds(pl.multiple_of(j * VIRT + 40 * c, 8), 40), lanes]
                s_b = seg_b[j] - r5b[pl.ds(pl.multiple_of(j * VIRT + 40 * (1 - c), 8), 40), lanes]
                row = (j // 4) * 16 + (2 * h + i) * 4 + j % 4
                zf[pl.ds(40 * ZS * c + row, 40, stride=ZS)] = s_a
                zf[pl.ds(40 * ZS * (1 - c) + row, 40, stride=ZS)] = s_b
                both = [jnp.where(c == 0, s_a, s_b), jnp.where(c == 0, s_b, s_a), jnp.zeros((48, 128), F32)]
                row = jnp.where(diag, j * 4 + 2 * h + i, h * 16 + j * 2 + i)
                zg[pl.ds(row, VIRT, stride=ZS)] = jnp.transpose(jnp.concatenate(both, axis=0))[:VIRT]

    def tile_at(base, n, m):
        return pl.ds(pl.multiple_of(base + n * WIDE + 128 * m, 128), 128)

    def slab(z, g, q, row, size):
        return z[pl.ds(pl.multiple_of((g * 8 + q) * ZS + row, 8), size)]

    def g_y(n, h):
        rows = pl.ds(16 * h, 16)
        return rc(gbuf.at[rows, wide(n)], grecv.at[rows, wide(n)], S_G, G_Y + h, d_y)

    def g_y_in(h):
        return rc(gbuf.at[pl.ds(16 * h, 16)], grecv.at[pl.ds(16 * h, 16)], S_G, G_Y + h, d_y)

    def f_y_in(h):
        rows = pl.ds(8 * h, 8)
        return rc(frecv.at[:, rows], frecv.at[:, rows], S_F, F_Y + h, d_y)

    def f_y(n, h):
        rows = pl.ds(8 * h, 8)
        return rc(fbuf.at[:, rows, wide(n, COLS * (1 - c))], frecv.at[:, rows, wide(n)], S_F, F_Y + h, d_y)

    def g_off(h):
        rows = pl.ds(16 * h, 16)

        @pl.loop(0, NCH)
        def _(n):
            segs = [slab(zg, n + NCH * (1 - c), q, 16 * h, 16) for q in range(8)]
            for m, tile in enumerate(join_segments(segs, lane16)):
                gbuf[rows, tile_at(0, n, m)] = tile
            g_y(n, h).start()

        @pl.loop(0, NCH)
        def _(n):
            segs = [slab(zg, n + NCH * c, q, 16 * h, 16) for q in range(8)]
            for m, tile in enumerate(join_segments(segs, lane16)):
                grecv[rows, tile_at(0, n, m)] = tile

    def f_off(h, send):
        lane8 = lax.broadcasted_iota(jnp.int32, (8, 128), 1)
        rows = pl.ds(8 * h, 8)
        hf = 1 - c if send else c

        @pl.loop(0, NCH)
        def _(n):
            for b in range(2):
                segs = [slab(zf, n + NCH * hf, q, 16 * b + 8 * h, 8) for q in range(8)]
                for m, tile in enumerate(join_segments(segs, lane8)):
                    fbuf[b, rows, tile_at(COLS * hf, n, m)] = tile
            if send:
                f_y(n, h).start()

    def g_p():
        return rc(gps, gpz, S_G, G_P, d_p)

    def give_g():
        @pl.loop(0, VIRT, unroll=8)
        def _(v):
            gps[v] = zg[pl.ds(pl.multiple_of(v * ZS + 16 * (1 - k), 8), 16)]

        g_p().start()

    def q_diag():
        g_p().wait_recv()

        def flat(hf, send):
            @pl.loop(0, NCH)
            def _(n):
                for b, mine in ((k, True), (1 - k, False)):
                    row = pl.multiple_of(16 * b, 16)
                    segs = []
                    for q in range(8):
                        g = n + NCH * hf
                        extra = slab(zg, g, q, row, 16) if mine else gpz[g * 8 + q]
                        segs.append(slab(zf, g, q, row, 16) + extra)
                    for m, tile in enumerate(join_segments(segs, lane16)):
                        fbuf[b, :, tile_at(COLS * hf, n, m)] = tile
                if send:
                    for h in range(2):
                        f_y(n, h).start()

        flat(1 - c, True)
        flat(c, False)

    s_before()

    early, late = 1 - x, x

    def pair(hf, h, cols, slot):
        ts = pl.ds(2 * h, 2)
        return rc(xp.at[p3, ts, hf, :, cols], prx.at[ts, hf, :, cols], S_PAIR, slot, d_p)

    def pair_e(n, h):
        return pair(early, h, wide(n), E_D + h)

    def pair_l(n, h):
        return pair(late, h, wide(n), L_D + h)

    def cross(hf, h, cols, slot):
        ts = pl.ds(2 * h, 2)
        return rc(xp.at[p2, ts, hf, :, cols], xrecv.at[ts, hf, :, cols], S_X, slot, d_x)

    def combine(hf, h, first, last, slot):
        @pl.loop(first, last)
        def _(n):
            ts = pl.ds(2 * h, 2)
            xp[p2, ts, hf, :, wide(n)] += prx[ts, hf, :, wide(n)]
            cross(hf, h, wide(n), slot(n)).start()

    def over_columns(step):
        @pl.loop(0, 2)
        def _(g):
            step(pl.ds(pl.multiple_of(g * 2 * WIDE, 128), 2 * WIDE), (2 * g, 2 * g + 1))

        step(pl.ds(4 * WIDE, WIDE), (4,))

    def ladder_0():
        def step(cols, ns):
            lhs = tr1[pl.ds(other, 2), half(0)].reshape(64, KPAD)
            prod = jnp.dot(lhs, vbuf[:, cols], preferred_element_type=F32)
            xp[pl.ds(other, 2), pl.ds(0, 2), :, :, cols] = prod.reshape(2, 2, 2, 8, -1)
            for n in ns:
                pair_e(n, 0).start()

        over_columns(step)

    def ladder_1():
        def step(cols, ns):
            lhs = jnp.concatenate(
                [tr1[pl.ds(other, 2), half(1)].reshape(64, KPAD), tr1[pl.ds(own, 2)].reshape(128, KPAD)], axis=0
            )
            prod = jnp.dot(lhs, vbuf[:, cols], preferred_element_type=F32)
            xp[pl.ds(other, 2), pl.ds(2, 2), :, :, cols] = prod[:64].reshape(2, 2, 2, 8, -1)
            xp[pl.ds(own, 2), :, :, :, cols] = prod[64:].reshape(2, 4, 2, 8, -1)
            for n in ns:
                pair_e(n, 1).start()
                out_pair(n).start()

        over_columns(step)

    def combine_e(h):
        pair(early, h, pl.ds(0, COLS), E_D + h).wait_recv()
        combine(early, h, 0, NCH, lambda n: E_X)

    def combine_l(h, first=0, last=NCH):
        if first == 0:
            pair(late, h, pl.ds(0, COLS), L_D + h).wait_recv()
        combine(late, h, first, last, lambda n: L_X + 1 + n // 2 if h else L_X)

    def out_pair(n):
        return rc(xp.at[p1, :, :, :, wide(n)], pown.at[:, :, :, wide(n)], S_OUT, O_D, d_p)

    row8 = lax.broadcasted_iota(jnp.int32, (8, WIDE), 0)
    here = (row8 // 4) == k

    def late_add(hs, wait_g):
        if wait_g:
            for hh in range(2):
                g_y_in(hh).wait_recv()

        @pl.loop(0, NCH)
        def _(n):
            for h in hs:
                for b in range(2):
                    for t in (2 * h, 2 * h + 1):
                        g2 = [grecv[pl.ds(16 * hh + 8 * b + 2 * t, 2), wide(n)] for hh in range(2)]
                        g8 = jnp.where(here, jnp.concatenate(g2 + g2, axis=0), 0.0)
                        xp[other + b, t, late, :, wide(n)] += g8
                pair_l(n, h).start()

    def x_y():
        return rc(xpart, xyrecv, S_XY, X_Y, d_y)

    def x_part():
        xpart[...] = lax.dot_general(
            ov[...], tcol[...].reshape(4 * ROWS, COLS), (((1,), (1,)), ((), ())), preferred_element_type=F32
        )
        x_y().start()

    def take(h):
        tr1[pl.ds(other, 2), half(h)] = tcol[pl.ds(other, 2), half(h), my_k(k)]

    def send_m():
        x_y().wait_recv()
        m_rows = (ob[...].astype(F32) + 0.5 * (xpart[...] + xyrecv[...])).astype(BF16)
        for q in range(4):
            msend[q] = m_rows[:, q * ROWS:(q + 1) * ROWS]
        mfull[r] = msend[r]
        for cp in m_out():
            cp.start()

    def m_out():
        return (
            rc(msend.at[p1], mfull.at[r], S_M, M_1, d_p),
            rc(msend.at[p2], mfull.at[r], S_M, M_2, d_x),
            rc(msend.at[p3], mfull.at[r], S_M, M_3, d_d),
        )

    def m_in():
        return (
            rc(msend.at[p1], mfull.at[p1], S_M, M_1, d_p),
            rc(msend.at[p2], mfull.at[p2], S_M, M_2, d_x),
            rc(msend.at[p3], mfull.at[p3], S_M, M_3, d_d),
        )

    @pl.when(diag)
    def _():
        t_y(0).wait_recv()
        for cc in (1, 0):
            r_x(cc).start()
        for q in range(2, 4):
            t_x(q, r).start()
        t_x(0, p2).wait_recv()
        t_fwd(0).start()
        t_x(1, p2).wait_recv()
        t_fwd(1).start()
        for cc in (1, 0):
            r_y(1, cc).start()
        t_y(3).start()
        t_fwd_in(0).wait_recv()
        take(0)
        ld_v.wait()
        ladder_0()
        t_y(1).wait_recv()
        s_prep(0)
        for q in range(2, 4):
            t_x(q, p2).wait_recv()
            t_fwd(q).start()
            for cc in (1, 0):
                r_y(q, cc).start()
        combine_e(0)
        s_blocks(0)
        t_p(p1).wait_recv()
        tr1[r] = tcol[r, :, my_k(k)]
        tr1[p1] = tcol[p1, :, my_k(k)]
        t_fwd_in(1).wait_recv()
        take(1)
        ladder_1()
        ld_o.wait()
        x_part()
        combine_e(1)
        t_y_in().wait_recv()
        s_prep(1)
        s_blocks(1)
        give_g()
        q_diag()
        late_add((0, 1), True)
        combine_l(0)
        combine_l(1, 0, 3)
        ld_oooo.wait()
        send_m()
        combine_l(1, 3)

    @pl.when(off)
    def _():
        for q in range(2):
            t_y(q).wait_recv()
        s_prep(0)
        s_blocks(0)
        g_off(0)
        for q in range(2):
            t_x(q, p2).wait_recv()
            t_fwd(q).start()
        ld_v.wait()
        for cc in (1, 0):
            r_x(cc).wait_recv()
            r_y(1, cc).wait_recv()
        ladder_0()
        t_y_in().wait_recv()
        r_p(r).start()
        tr1[r] = ty[:, my_k(k)]
        s_prep(1)
        for q in range(2, 4):
            t_x(q, p2).wait_recv()
            t_fwd(q).start()
        combine_e(0)
        s_blocks(1)
        g_off(1)
        late_add((0,), False)
        t_p(p1).wait_recv()
        for h in range(2):
            t_fwd_in(h).wait_recv()
        ld_o.wait()
        x_part()
        combine_l(0)
        f_off(0, True)
        for cc in (1, 0):
            r_y_in(cc).wait_recv()
        r_p(p1).wait_recv()
        ladder_1()
        late_add((1,), False)
        ld_oooo.wait()
        send_m()
        combine_e(1)
        f_off(1, True)
        combine_l(1)
        for h in range(2):
            f_off(h, False)

    for cp in m_in():
        cp.wait_recv()
    ld_d.wait()
    rc(xp.at[p1], pown, S_OUT, O_D, d_p).wait_recv()
    for h in range(2):
        f_y_in(h).wait_recv()
    rc(xp.at[p2, :, x], xrecv.at[:, x], S_X, E_X, d_x).wait_recv()
    cross(1 - x, 0, pl.ds(0, COLS), L_X).wait_recv()

    def finish(cols, ns):
        cross(1 - x, 1, cols, L_X + 1 + ns[0] // 2).wait_recv()
        width = len(ns) * WIDE
        r2 = lax.dot_general(
            mfull[...].reshape(4 * ROWS, ROWS), tcol[:, :, cols].reshape(4 * ROWS, width),
            (((0,), (0,)), ((), ())), preferred_element_type=F32,
        )
        part = xp[r, :, :, :, cols] + pown[:, :, :, cols] + xrecv[:, :, :, cols]
        obuf[:, cols] = ov[:, cols].astype(F32) + r2 + part.reshape(ROWS, width)
        mine = pl.ds(pl.multiple_of(COLS * c + ns[0] * WIDE, 128), width)
        for i in range(4):
            for ref, hf, at in ((fbuf, c, mine), (frecv, 1 - c, cols)):
                f8 = jnp.concatenate([ref[b, pl.ds(4 * i, 4), at] for b in range(2)], axis=0)
                rows = pl.ds(pl.multiple_of(16 * i + 8 * hf, 8), 8)
                obuf[rows, cols] += f8
        obuf[:, cols] = obuf[:, cols] / dbuf[:, cols]

    over_columns(finish)

    rc(tcol.at[r], tcol.at[r], S_TX, T_X, d_x).wait_send()
    rc(tcol.at[r], ty, S_TY, T_Y, d_y).wait_send()
    rc(tcol.at[p2], tcol.at[p2], S_FWD, T_FWD, d_p).wait_send()
    t_p(r).wait_send()
    rc(xp.at[p3], prx, S_PAIR, E_D, d_p).wait_send()
    rc(xp.at[p1], pown, S_OUT, O_D, d_p).wait_send()
    rc(xp.at[p2], xrecv, S_X, E_X, d_x).wait_send()
    rc(frecv, frecv, S_F, F_Y, d_y).wait_send()
    x_y().wait_send()
    rc(msend.at[pl.ds(0, 3)], mfull.at[pl.ds(0, 3)], S_M, M_1, d_p).wait_send()

    @pl.when(diag)
    def _():
        g_p().wait_send()
        rc(tr1.at[pl.ds(0, 2)], tr1.at[pl.ds(0, 2)], S_R, R_Y, d_y).wait_send()

    @pl.when(off)
    def _():
        r_p(r).wait_send()
        rc(gbuf, grecv, S_G, G_Y, d_y).wait_send()


def solution(mesh):
    def sweep(t_blk, d_blk, o_blk, v_blk, oooo, wd_blk, wx_blk):
        any_spec = pl.BlockSpec(memory_space=pl.ANY)
        vm = pltpu.VMEM
        return pl.pallas_call(
            kernel,
            out_shape=pltpu.VMEM((ROWS, COLS), F32),
            in_specs=[any_spec] * 7,
            out_specs=pl.BlockSpec(memory_space=pltpu.VMEM),
            scratch_shapes=[
                vm((ROWS, COLS), F32),
                vm((ROWS, COLS), F32),
                vm((ROWS, COLS), BF16),
                vm((KPAD, COLS), BF16),
                vm((ROWS, 256), BF16),
                vm((OCC, 128, WIDE), BF16),
                vm((OCC, VIRT, WIDE), BF16),
                vm((4, ROWS, COLS), BF16),
                vm((ROWS, COLS), BF16),
                vm((4, ROWS, KPAD), BF16),
                vm((2, VIRT * ZS, 128), F32),
                vm((2, WIDE, WIDE), BF16),
                vm((4, WIDE, 128), BF16),
                vm((2 * VIRT, OCC * 128), BF16),
                vm((2 * VIRT, WIDE), F32),
                vm((VIRT, WIDE), F32),
                vm((WIDE, 512), F32),
                vm((WIDE, 256), F32),
                vm((VIRT * ZS, 128), F32),
                vm((VIRT * ZS, 128), F32),
                vm((VIRT, 16, 128), F32),
                vm((VIRT, 16, 128), F32),
                vm((2, 16, 2 * COLS), F32),
                vm((32, COLS), F32),
                vm((2, 16, COLS), F32),
                vm((32, COLS), F32),
                vm((4, 4, 2, 8, COLS), F32),
                vm((4, 2, 8, COLS), F32),
                vm((4, 2, 8, COLS), F32),
                vm((4, 2, 8, COLS), F32),
                vm((ROWS, 256), F32),
                vm((ROWS, 256), F32),
                vm((4, ROWS, ROWS), BF16),
                vm((4, ROWS, ROWS), BF16),
                pltpu.SemaphoreType.DMA((10,)),
                pltpu.SemaphoreType.DMA((N_SEND,)),
                pltpu.SemaphoreType.DMA((N_RECV,)),
            ],
            compiler_params=pltpu.CompilerParams(
                collective_id=0, has_side_effects=True, vmem_limit_bytes=54 * 1024 * 1024
            ),
            name="ccd_sweep",
        )(t_blk, d_blk, o_blk, v_blk, oooo, wd_blk.reshape(OCC, VIRT, WIDE), wx_blk.reshape(OCC, VIRT, WIDE))

    amp = P("row", "col")
    wide_spec = P(None, "col")
    return jax.shard_map(
        sweep, mesh=mesh, in_specs=(amp, amp, amp, amp, P(), wide_spec, wide_spec), out_specs=amp, check_vma=False
    )
```

```python
import functools

import jax
import jax.numpy as jnp
from jax import lax
from jax.experimental import pallas as pl
from jax.experimental.pallas import tpu as pltpu
from jax.sharding import PartitionSpec as P

MESH = pl.DeviceIdType.MESH
F32 = jnp.float32
BF16 = jnp.bfloat16

OCC = 16
VIRT = 80
ROWS = 64
COLS = 3200
KPAD = 1664
LANE = 128
HALF_V = VIRT // 2
BOTH = range(2)
WIDE = 640
NCH = COLS // WIDE
ZS = 40

T_X, T_Y, T_P, T_FWD, R_P, G_P, R_X, R_Y, G_Y = 0, 4, 7, 8, 10, 10, 11, 13, 11
E_D, L_D, O_D, E_X, L_X, F_Y, X_Y, M_1, M_2, M_3 = 17, 23, 25, 26, 27, 31, 33, 34, 35, 36
N_RECV = 37
S_TX, S_TY, S_TP, S_FWD, S_R, S_PAIR, S_OUT, S_X, S_F, S_G, S_XY, S_M = range(12)
N_SEND = 12


def split_segments(parts, lane):
    out = []
    for q in range(8):
        m, s = divmod(80 * q, LANE)
        seg = parts[m]
        if s:
            seg = pltpu.roll(seg, LANE - s, axis=1)
            if s + 80 > LANE:
                seg = jnp.where(lane < LANE - s, seg, pltpu.roll(parts[m + 1], LANE - s, axis=1))
        out.append(jnp.where(lane < 80, seg, 0.0))
    return out


def join_segments(segs, lane):
    r = [segs[0]] + [pltpu.roll(segs[q], (80 * q) % LANE, axis=1) for q in range(1, 8)]
    return [
        jnp.where(lane < 80, r[0], r[1]),
        jnp.where(lane < 32, r[1], jnp.where(lane < 112, r[2], r[3])),
        jnp.where(lane < 64, r[3], r[4]),
        jnp.where(lane < 16, r[4], jnp.where(lane < 96, r[5], r[6])),
        jnp.where(lane < 48, r[6], r[7]),
    ]


def kernel(
    t_hbm, d_hbm, o_hbm, v_hbm, oooo_hbm, wd_hbm, wx_hbm, obuf,
    tf, dbuf, ov, vbuf, ob, wdp, wxb,
    tcol, ty, tr1, zt, wxs, tb, l3, r3a, r3b, r5a, r5b, zf, zg, gps, gpz, fbuf, gbuf, frecv, grecv,
    xp, prx, pown, xrecv, xpart, xyrecv, msend, mfull,
    lsem, ss, rs,
):
    r = lax.axis_index("row")
    c = lax.axis_index("col")
    k = lax.rem(r, 2)
    x = r // 2
    p1 = r + 1 - 2 * k
    p2 = lax.rem(r + 2, 4)
    p3 = lax.rem(p1 + 2, 4)
    diag = x == c
    off = x != c
    d_p, d_x, d_d, d_y, d_z = (c, p1), (c, p2), (c, p3), (1 - c, r), (1 - c, p1)
    other = 2 * (1 - x)
    own = 2 * x

    def rc(src, dst, leave, arrive, dev):
        return pltpu.make_async_remote_copy(
            src_ref=src, dst_ref=dst, send_sem=ss.at[leave], recv_sem=rs.at[arrive],
            device_id=dev, device_id_type=MESH,
        )

    def wide(n, base=0):
        return pl.ds(pl.multiple_of(base + n * WIDE, LANE), WIDE)

    def half(h):
        return pl.ds(32 * h, 32)

    def quarter(q):
        return pl.ds(16 * q, 16)

    def ld_t(q):
        return pltpu.make_async_copy(t_hbm.at[quarter(q)], tf.at[quarter(q)], lsem.at[q])

    ld_v = pltpu.make_async_copy(v_hbm, vbuf.at[pl.ds(pl.multiple_of(64 * k, 64), 1600)], lsem.at[4])
    ld_wd = pltpu.make_async_copy(wd_hbm, wdp.at[:, pl.ds(0, VIRT)], lsem.at[5])
    ld_wx = pltpu.make_async_copy(wx_hbm, wxb, lsem.at[6])
    ld_o = pltpu.make_async_copy(o_hbm, ov, lsem.at[7])
    ld_d = pltpu.make_async_copy(d_hbm, dbuf, lsem.at[8])
    ld_oooo = pltpu.make_async_copy(oooo_hbm.at[pl.ds(pl.multiple_of(ROWS * r, ROWS), ROWS)], ob, lsem.at[9])
    for q in range(4):
        ld_t(q).start()

    barrier = pltpu.get_barrier_semaphore()
    for dev in (d_p, d_x, d_d, d_y, d_z):
        pl.semaphore_signal(barrier, inc=1, device_id=dev, device_id_type=MESH)
    for ld in (ld_wx, ld_wd, ld_v, ld_o, ld_oooo, ld_d):
        ld.start()

    def t_x(q, blk):
        return rc(tcol.at[blk, quarter(q)], tcol.at[blk, quarter(q)], S_TX, T_X + q, d_x)

    def t_y(q):
        return rc(tcol.at[r, quarter(q)], ty.at[quarter(q)], S_TY, T_Y + min(q, 2), d_y)

    def t_y_in():
        return rc(tcol.at[r, half(1)], ty.at[half(1)], S_TY, T_Y + 2, d_y)

    def t_fwd(q):
        return rc(tcol.at[p2, quarter(q)], tcol.at[p2, quarter(q)], S_FWD, T_FWD + q // 2, d_p)

    def t_fwd_in(h):
        return rc(tcol.at[p3, half(h)], tcol.at[p3, half(h)], S_FWD, T_FWD + h, d_p)

    def t_p(blk):
        return rc(tcol.at[blk], tcol.at[blk], S_TP, T_P, d_p)

    def my_k(core):
        return pl.ds(pl.multiple_of(1536 * core, LANE), KPAD)

    def r_p(blk):
        return rc(ty.at[:, my_k(1 - k)], tr1.at[blk], S_R, R_P, d_p)

    def r_x(q, core):
        slot = R_Y if q else R_X + lax.rem(k + core, 2)
        return rc(ty.at[quarter(q), my_k(core)], tr1.at[r, quarter(q)], S_R, slot, (c, other + core))

    def r_y(q, core):
        slot = R_Y + 1 if q == 1 else R_Y + 2 + lax.rem(k + core, 2)
        return rc(tcol.at[p2, quarter(q), my_k(core)], tr1.at[p2, quarter(q)], S_R, slot, (1 - c, own + core))

    def r_y_in(core):
        slot = R_Y + 2 + lax.rem(k + core, 2)
        return rc(tr1.at[p2, half(1)], tr1.at[p2, half(1)], S_R, slot, (1 - c, own + core))

    for q in range(4):
        ld_t(q).wait()
        tcol[r, quarter(q)] = tf[quarter(q)].astype(BF16)
        if q == 0:
            pl.semaphore_wait(barrier, 5)
        if q < 2:
            t_x(q, r).start()
        else:
            pl.when(off)(t_x(q, r).start)
        if q < 3:
            t_y(q).start()
        else:
            pl.when(off)(t_y(q).start)
    t_p(r).start()

    lane32 = lax.broadcasted_iota(jnp.int32, (32, LANE), 1)
    lane40 = lax.broadcasted_iota(jnp.int32, (HALF_V, LANE), 1)
    lane16 = lax.broadcasted_iota(jnp.int32, (16, LANE), 1)
    vbuf[pl.ds(pl.multiple_of(1600 * (1 - k), 64), 64)] = jnp.zeros((64, COLS), BF16)
    wdp[:, pl.ds(VIRT, 48)] = jnp.zeros((OCC, 48, WIDE), BF16)

    def slabs(ref, h, col_half):
        @pl.loop(0, NCH)
        def _(g):
            parts = [
                ref[half(h), pl.ds(pl.multiple_of(g * WIDE + LANE * m, LANE), LANE)].astype(F32)
                for m in range(5)
            ]
            for q, seg in enumerate(split_segments(parts, lane32)):
                zt[h, pl.ds(pl.multiple_of((col_half * 40 + g * 8 + q) * ZS, 8), 32)] = seg

    def regroup(h, vh, l3_rows, tb_at):
        def rows(ik):
            return zt[h, pl.ds(HALF_V * ZS * vh + ik, HALF_V, stride=ZS)]

        @pl.loop(0, OCC)
        def _(kk):
            blk = jnp.concatenate([rows(kk), rows(OCC + kk)], axis=0).astype(BF16)
            l3[l3_rows, pl.ds(pl.multiple_of(kk * LANE, LANE), LANE)] = blk

        for i in BOTH:
            @pl.loop(0, OCC // 2)
            def _(k2):
                blk = jnp.concatenate([rows(i * OCC + 2 * k2), rows(i * OCC + 2 * k2 + 1)], axis=0).astype(BF16)
                tb[tb_at + i, pl.ds(pl.multiple_of(k2 * VIRT, 16), VIRT)] = blk

    def r3(rows):
        return jnp.dot(l3[rows], wdp[...].reshape(OCC * LANE, WIDE), preferred_element_type=F32)

    def r5(vh, first, count):
        rhs = jnp.concatenate([tb[first + i] for i in range(count)], axis=1)
        return lax.dot_general(wxs[vh], rhs, (((0,), (0,)), ((), ())), preferred_element_type=F32)

    def s_before():
        for h in BOTH:
            slabs(tf, h, c)
        ld_wx.wait()

        @pl.loop(0, OCC // 2)
        def _(k2):
            w = [wxb[2 * k2 + e].astype(F32) for e in BOTH]
            at = pl.ds(pl.multiple_of(k2 * VIRT, 16), VIRT)
            for vh in BOTH:
                part = [w[e][HALF_V * vh:HALF_V * vh + 40] for e in BOTH]
                wxs[vh, at] = jnp.concatenate(part, axis=0).astype(BF16)

        for h in BOTH:
            regroup(h, c, pl.ds(VIRT * h, VIRT), 2 * h)
        ld_wd.wait()
        r3a[...] = r3(pl.ds(0, 2 * VIRT))
        r5a[...] = r5(c, 0, 4)

    def s_prep(h):
        slabs(ty, h, 1 - c)
        regroup(h, 1 - c, pl.ds(0, VIRT), 0)

    def s_blocks(h):
        r3b[...] = r3(pl.ds(0, VIRT))
        r5b[...] = r5a[:, 256 * h:256 * h + 256] + r5(1 - c, 0, 2)

        @pl.loop(0, 2)
        def _(i):
            rows_a = pl.ds(pl.multiple_of(VIRT * h + HALF_V * i, 8), HALF_V)
            rows_b = pl.ds(pl.multiple_of(HALF_V * i, 8), HALF_V)
            seg_a = split_segments([r3a[rows_a, pl.ds(LANE * m, LANE)] for m in range(5)], lane40)
            seg_b = split_segments([r3b[rows_b, pl.ds(LANE * m, LANE)] for m in range(5)], lane40)
            lanes = pl.ds(pl.multiple_of(i * LANE, LANE), LANE)
            for j in range(8):
                s_a = seg_a[j] - r5b[pl.ds(pl.multiple_of(j * VIRT + HALF_V * c, 8), HALF_V), lanes]
                s_b = seg_b[j] - r5b[pl.ds(pl.multiple_of(j * VIRT + HALF_V * (1 - c), 8), HALF_V), lanes]
                row = (j // 4) * 16 + (2 * h + i) * 4 + j % 4
                zf[pl.ds(HALF_V * ZS * c + row, HALF_V, stride=ZS)] = s_a
                zf[pl.ds(HALF_V * ZS * (1 - c) + row, HALF_V, stride=ZS)] = s_b
                both = [jnp.where(c == 0, s_a, s_b), jnp.where(c == 0, s_b, s_a), jnp.zeros((48, LANE), F32)]
                row = jnp.where(diag, j * 4 + 2 * h + i, h * 16 + j * 2 + i)
                zg[pl.ds(row, VIRT, stride=ZS)] = jnp.transpose(jnp.concatenate(both, axis=0))[:VIRT]

    def tile_at(base, n, m):
        return pl.ds(pl.multiple_of(base + n * WIDE + LANE * m, LANE), LANE)

    def slab(z, g, q, row, size):
        return z[pl.ds(pl.multiple_of((g * 8 + q) * ZS + row, 8), size)]

    def g_y(n, h):
        rows = pl.ds(16 * h, 16)
        return rc(gbuf.at[rows, wide(n)], grecv.at[rows, wide(n)], S_G, G_Y + h, d_y)

    def g_y_in(h):
        return rc(gbuf.at[pl.ds(16 * h, 16)], grecv.at[pl.ds(16 * h, 16)], S_G, G_Y + h, d_y)

    def f_y_in(h):
        rows = pl.ds(8 * h, 8)
        return rc(frecv.at[:, rows], frecv.at[:, rows], S_F, F_Y + h, d_y)

    def f_y(n, h):
        rows = pl.ds(8 * h, 8)
        return rc(fbuf.at[:, rows, wide(n, COLS * (1 - c))], frecv.at[:, rows, wide(n)], S_F, F_Y + h, d_y)

    def g_off(h):
        rows = pl.ds(16 * h, 16)

        @pl.loop(0, NCH)
        def _(n):
            segs = [slab(zg, n + NCH * (1 - c), q, 16 * h, 16) for q in range(8)]
            for m, tile in enumerate(join_segments(segs, lane16)):
                gbuf[rows, tile_at(0, n, m)] = tile
            g_y(n, h).start()

        @pl.loop(0, NCH)
        def _(n):
            segs = [slab(zg, n + NCH * c, q, 16 * h, 16) for q in range(8)]
            for m, tile in enumerate(join_segments(segs, lane16)):
                grecv[rows, tile_at(0, n, m)] = tile

    def f_off(h, hf, first=0, last=NCH):
        lane8 = lax.broadcasted_iota(jnp.int32, (8, LANE), 1)
        rows = pl.ds(8 * h, 8)

        @pl.loop(first, last)
        def _(n):
            for b in BOTH:
                segs = [slab(zf, n + NCH * hf, q, 16 * b + 8 * h, 8) for q in range(8)]
                for m, tile in enumerate(join_segments(segs, lane8)):
                    fbuf[b, rows, tile_at(COLS * hf, n, m)] = tile
            if hf is not c:
                f_y(n, h).start()

    def g_p():
        return rc(gps, gpz, S_G, G_P, d_p)

    def give_g():
        @pl.loop(0, VIRT, unroll=8)
        def _(v):
            gps[v] = zg[pl.ds(pl.multiple_of(v * ZS + 16 * (1 - k), 8), 16)]

        g_p().start()

    def q_diag():
        g_p().wait_recv()

        def flat(hf, send):
            @pl.loop(0, NCH)
            def _(n):
                for b, mine in ((k, True), (1 - k, False)):
                    row = pl.multiple_of(16 * b, 16)
                    segs = []
                    for q in range(8):
                        g = n + NCH * hf
                        extra = slab(zg, g, q, row, 16) if mine else gpz[g * 8 + q]
                        segs.append(slab(zf, g, q, row, 16) + extra)
                    for m, tile in enumerate(join_segments(segs, lane16)):
                        fbuf[b, :, tile_at(COLS * hf, n, m)] = tile
                if send:
                    for h in BOTH:
                        f_y(n, h).start()

        flat(1 - c, True)
        flat(c, False)

    s_before()

    early, late = 1 - x, x

    def pair(hf, h, cols, slot):
        ts = pl.ds(2 * h, 2)
        return rc(xp.at[p3, ts, hf, :, cols], prx.at[ts, hf, :, cols], S_PAIR, slot, d_p)

    def pair_e(n, h):
        return pair(early, h, wide(n), E_D + 3 * h + n // 2)

    def pair_l(n, h):
        return pair(late, h, wide(n), L_D + h)

    def cross(hf, h, cols, slot):
        ts = pl.ds(2 * h, 2)
        return rc(xp.at[p2, ts, hf, :, cols], xrecv.at[ts, hf, :, cols], S_X, slot, d_x)

    def over_columns(step):
        @pl.loop(0, 2)
        def _(g):
            step(pl.ds(pl.multiple_of(g * 2 * WIDE, LANE), 2 * WIDE), (2 * g, 2 * g + 1))

        step(pl.ds(4 * WIDE, WIDE), (4,))

    def ladder_0():
        def step(cols, ns):
            lhs = tr1[pl.ds(other, 2), half(0)].reshape(64, KPAD)
            prod = jnp.dot(lhs, vbuf[:, cols], preferred_element_type=F32)
            xp[pl.ds(other, 2), pl.ds(0, 2), :, :, cols] = prod.reshape(2, 2, 2, 8, -1)
            for n in ns:
                pair_e(n, 0).start()

        over_columns(step)

    def ladder_1():
        def step(cols, ns):
            lhs = jnp.concatenate(
                [tr1[pl.ds(other, 2), half(1)].reshape(64, KPAD), tr1[pl.ds(own, 2)].reshape(LANE, KPAD)], axis=0
            )
            prod = jnp.dot(lhs, vbuf[:, cols], preferred_element_type=F32)
            xp[pl.ds(other, 2), pl.ds(2, 2), :, :, cols] = prod[:64].reshape(2, 2, 2, 8, -1)
            xp[pl.ds(own, 2), :, :, :, cols] = prod[64:].reshape(2, 4, 2, 8, -1)
            for n in ns:
                pair_e(n, 1).start()
                out_pair(n).start()

        over_columns(step)

    def combine_e(h):
        def step(cols, ns):
            pair(early, h, cols, E_D + 3 * h + ns[0] // 2).wait_recv()
            ts = pl.ds(2 * h, 2)
            xp[p2, ts, early, :, cols] += prx[ts, early, :, cols]
            cross(early, h, cols, E_X).start()

        over_columns(step)

    def combine_l(h):
        pair(late, h, pl.ds(0, COLS), L_D + h).wait_recv()

        def step(cols, ns):
            ts = pl.ds(2 * h, 2)
            xp[p2, ts, late, :, cols] += prx[ts, late, :, cols]
            cross(late, h, cols, L_X + 1 + ns[0] // 2 if h else L_X).start()

        over_columns(step)

    def out_pair(n):
        return rc(xp.at[p1, :, :, :, wide(n)], pown.at[:, :, :, wide(n)], S_OUT, O_D, d_p)

    row8 = lax.broadcasted_iota(jnp.int32, (8, WIDE), 0)
    here = (row8 // 4) == k

    def late_add(hs, wait_g):
        if wait_g:
            for hh in BOTH:
                g_y_in(hh).wait_recv()

        @pl.loop(0, NCH)
        def _(n):
            for h in hs:
                for b in BOTH:
                    for t in (2 * h, 2 * h + 1):
                        g2 = [grecv[pl.ds(16 * hh + 8 * b + 2 * t, 2), wide(n)] for hh in BOTH]
                        g8 = jnp.where(here, jnp.concatenate(g2 + g2, axis=0), 0.0)
                        xp[other + b, t, late, :, wide(n)] += g8
                pair_l(n, h).start()

    def x_y():
        return rc(xpart, xyrecv, S_XY, X_Y, d_y)

    def x_part():
        xpart[...] = lax.dot_general(
            ov[...], tcol[...].reshape(4 * ROWS, COLS), (((1,), (1,)), ((), ())), preferred_element_type=F32
        )
        x_y().start()

    def take(h):
        tr1[pl.ds(other, 2), half(h)] = tcol[pl.ds(other, 2), half(h), my_k(k)]

    def send_m():
        x_y().wait_recv()
        m_rows = (ob[...].astype(F32) + 0.5 * (xpart[...] + xyrecv[...])).astype(BF16)
        for q in range(4):
            msend[q] = m_rows[:, q * ROWS:(q + 1) * ROWS]
        mfull[r] = msend[r]
        for cp in m_out():
            cp.start()

    def m_out():
        return (
            rc(msend.at[p1], mfull.at[r], S_M, M_1, d_p),
            rc(msend.at[p2], mfull.at[r], S_M, M_2, d_x),
            rc(msend.at[p3], mfull.at[r], S_M, M_3, d_d),
        )

    def m_in():
        return (
            rc(msend.at[p1], mfull.at[p1], S_M, M_1, d_p),
            rc(msend.at[p2], mfull.at[p2], S_M, M_2, d_x),
            rc(msend.at[p3], mfull.at[p3], S_M, M_3, d_d),
        )

    @pl.when(diag)
    def _():
        t_y(0).wait_recv()
        for cc in (1, 0):
            r_x(0, cc).start()
        t_x(0, p2).wait_recv()
        t_fwd(0).start()
        t_y(1).wait_recv()
        r_x(1, k).start()
        t_x(1, p2).wait_recv()
        t_fwd(1).start()
        r_y(1, 1 - k).start()
        t_y(3).start()
        for q in range(2, 4):
            t_x(q, r).start()
        t_fwd_in(0).wait_recv()
        take(0)
        ld_v.wait()
        ladder_0()
        s_prep(0)
        for q in range(2, 4):
            t_x(q, p2).wait_recv()
            t_fwd(q).start()
            for cc in (1, 0):
                r_y(q, cc).start()
        combine_e(0)
        s_blocks(0)
        t_p(p1).wait_recv()
        tr1[r] = tcol[r, :, my_k(k)]
        tr1[p1] = tcol[p1, :, my_k(k)]
        t_fwd_in(1).wait_recv()
        take(1)
        ladder_1()
        ld_o.wait()
        x_part()
        combine_e(1)
        t_y_in().wait_recv()
        s_prep(1)
        s_blocks(1)
        give_g()
        q_diag()
        late_add((0, 1), True)
        combine_l(0)
        ld_oooo.wait()
        send_m()
        combine_l(1)

    @pl.when(off)
    def _():
        for q in BOTH:
            t_y(q).wait_recv()
        s_prep(0)
        s_blocks(0)
        g_off(0)
        for q in BOTH:
            t_x(q, p2).wait_recv()
            t_fwd(q).start()
        f_off(0, 1 - c, 0, 3)
        ld_v.wait()
        for cc in (1, 0):
            r_x(0, cc).wait_recv()
        r_x(1, k).wait_recv()
        r_y(1, 1 - k).wait_recv()
        ladder_0()
        t_y_in().wait_recv()
        r_p(r).start()
        tr1[r] = ty[:, my_k(k)]
        s_prep(1)
        combine_e(0)
        s_blocks(1)
        for q in range(2, 4):
            t_x(q, p2).wait_recv()
            t_fwd(q).start()
        g_off(1)
        late_add((0,), False)
        t_p(p1).wait_recv()
        for h in BOTH:
            t_fwd_in(h).wait_recv()
        ld_o.wait()
        x_part()
        f_off(0, 1 - c, 3)
        combine_l(0)
        for cc in (1, 0):
            r_y_in(cc).wait_recv()
        r_p(p1).wait_recv()
        ladder_1()
        late_add((1,), False)
        ld_oooo.wait()
        send_m()
        combine_e(1)
        f_off(1, 1 - c)
        combine_l(1)
        for h in BOTH:
            f_off(h, c)

    for cp in m_in():
        cp.wait_recv()
    ld_d.wait()
    rc(xp.at[p1], pown, S_OUT, O_D, d_p).wait_recv()
    for h in BOTH:
        f_y_in(h).wait_recv()
    rc(xp.at[p2, :, x], xrecv.at[:, x], S_X, E_X, d_x).wait_recv()
    cross(1 - x, 0, pl.ds(0, COLS), L_X).wait_recv()

    def finish(cols, ns):
        cross(1 - x, 1, cols, L_X + 1 + ns[0] // 2).wait_recv()
        width = len(ns) * WIDE
        r2 = lax.dot_general(
            mfull[...].reshape(4 * ROWS, ROWS), tcol[:, :, cols].reshape(4 * ROWS, width),
            (((0,), (0,)), ((), ())), preferred_element_type=F32,
        )
        part = xp[r, :, :, :, cols] + pown[:, :, :, cols] + xrecv[:, :, :, cols]
        obuf[:, cols] = ov[:, cols].astype(F32) + r2 + part.reshape(ROWS, width)
        mine = pl.ds(pl.multiple_of(COLS * c + ns[0] * WIDE, LANE), width)
        for i in range(4):
            for ref, hf, at in ((fbuf, c, mine), (frecv, 1 - c, cols)):
                f8 = jnp.concatenate([ref[b, pl.ds(4 * i, 4), at] for b in BOTH], axis=0)
                rows = pl.ds(pl.multiple_of(16 * i + 8 * hf, 8), 8)
                obuf[rows, cols] += f8
        obuf[:, cols] = obuf[:, cols] / dbuf[:, cols]

    over_columns(finish)

    rc(tcol.at[r], tcol.at[r], S_TX, T_X, d_x).wait_send()
    rc(tcol.at[r], ty, S_TY, T_Y, d_y).wait_send()
    rc(tcol.at[p2], tcol.at[p2], S_FWD, T_FWD, d_p).wait_send()
    t_p(r).wait_send()
    rc(xp.at[p3], prx, S_PAIR, E_D, d_p).wait_send()
    rc(xp.at[p1], pown, S_OUT, O_D, d_p).wait_send()
    rc(xp.at[p2], xrecv, S_X, E_X, d_x).wait_send()
    rc(frecv, frecv, S_F, F_Y, d_y).wait_send()
    x_y().wait_send()
    rc(msend.at[pl.ds(0, 3)], mfull.at[pl.ds(0, 3)], S_M, M_1, d_p).wait_send()

    @pl.when(diag)
    def _():
        g_p().wait_send()
        rc(tr1.at[pl.ds(0, 2)], tr1.at[pl.ds(0, 2)], S_R, R_Y, d_y).wait_send()

    @pl.when(off)
    def _():
        r_p(r).wait_send()
        rc(gbuf, grecv, S_G, G_Y, d_y).wait_send()


def solution(mesh):
    def sweep(t_blk, d_blk, o_blk, v_blk, oooo, wd_blk, wx_blk):
        any_spec = pl.BlockSpec(memory_space=pl.ANY)
        vm = pltpu.VMEM
        return pl.pallas_call(
            kernel,
            out_shape=pltpu.VMEM((ROWS, COLS), F32),
            in_specs=[any_spec] * 7,
            out_specs=pl.BlockSpec(memory_space=pltpu.VMEM),
            scratch_shapes=[
                vm((ROWS, COLS), F32),
                vm((ROWS, COLS), F32),
                vm((ROWS, COLS), BF16),
                vm((KPAD, COLS), BF16),
                vm((ROWS, 256), BF16),
                vm((OCC, LANE, WIDE), BF16),
                vm((OCC, VIRT, WIDE), BF16),
                vm((4, ROWS, COLS), BF16),
                vm((ROWS, COLS), BF16),
                vm((4, ROWS, KPAD), BF16),
                vm((2, VIRT * ZS, LANE), F32),
                vm((2, WIDE, WIDE), BF16),
                vm((4, WIDE, LANE), BF16),
                vm((2 * VIRT, OCC * LANE), BF16),
                vm((2 * VIRT, WIDE), F32),
                vm((VIRT, WIDE), F32),
                vm((WIDE, 512), F32),
                vm((WIDE, 256), F32),
                vm((VIRT * ZS, LANE), F32),
                vm((VIRT * ZS, LANE), F32),
                vm((VIRT, 16, LANE), F32),
                vm((VIRT, 16, LANE), F32),
                vm((2, 16, 2 * COLS), F32),
                vm((32, COLS), F32),
                vm((2, 16, COLS), F32),
                vm((32, COLS), F32),
                vm((4, 4, 2, 8, COLS), F32),
                vm((4, 2, 8, COLS), F32),
                vm((4, 2, 8, COLS), F32),
                vm((4, 2, 8, COLS), F32),
                vm((ROWS, 256), F32),
                vm((ROWS, 256), F32),
                vm((4, ROWS, ROWS), BF16),
                vm((4, ROWS, ROWS), BF16),
                pltpu.SemaphoreType.DMA((10,)),
                pltpu.SemaphoreType.DMA((N_SEND,)),
                pltpu.SemaphoreType.DMA((N_RECV,)),
            ],
            compiler_params=pltpu.CompilerParams(
                collective_id=0, has_side_effects=True, vmem_limit_bytes=54 * 1024 * 1024
            ),
            name="ccd_sweep",
        )(t_blk, d_blk, o_blk, v_blk, oooo, wd_blk.reshape(OCC, VIRT, WIDE), wx_blk.reshape(OCC, VIRT, WIDE))

    amp = P("row", "col")
    wide_spec = P(None, "col")
    return jax.shard_map(
        sweep, mesh=mesh, in_specs=(amp, amp, amp, amp, P(), wide_spec, wide_spec), out_specs=amp, check_vma=False
    )
```

```python
import functools

import jax
import jax.numpy as jnp
from jax import lax
from jax.experimental import pallas as pl
from jax.experimental.pallas import tpu as pltpu
from jax.sharding import PartitionSpec as P

MESH = pl.DeviceIdType.MESH
F32 = jnp.float32
BF16 = jnp.bfloat16

OCC = 16
VIRT = 80
ROWS = 64
COLS = 3200
KPAD = 1664
LANE = 128
HALF_V = VIRT // 2
BOTH = range(2)
WIDE = 640
NCH = COLS // WIDE
ZS = 40

T_X, T_Y, T_P, T_FWD, R_P, G_P, R_X, R_Y, G_Y = 0, 4, 7, 8, 10, 10, 11, 13, 11
E_D, G_D, O_D, E_X, L_X, F_Y, X_Y, M_1, M_2, M_3 = 17, 23, 24, 25, 26, 30, 32, 33, 34, 35
N_RECV = 36
S_TX, S_TY, S_TP, S_FWD, S_R, S_PAIR, S_OUT, S_X, S_F, S_G, S_XY, S_M, S_GD = range(13)
N_SEND = 13
STEPS = (0, 1), (2, 3), (4,)


def split_segments(parts, lane):
    out = []
    for q in range(8):
        m, s = divmod(80 * q, LANE)
        seg = parts[m]
        if s:
            seg = pltpu.roll(seg, LANE - s, axis=1)
            if s + 80 > LANE:
                seg = jnp.where(lane < LANE - s, seg, pltpu.roll(parts[m + 1], LANE - s, axis=1))
        out.append(jnp.where(lane < 80, seg, 0.0))
    return out


def join_segments(segs, lane):
    r = [segs[0]] + [pltpu.roll(segs[q], (80 * q) % LANE, axis=1) for q in range(1, 8)]
    return [
        jnp.where(lane < 80, r[0], r[1]),
        jnp.where(lane < 32, r[1], jnp.where(lane < 112, r[2], r[3])),
        jnp.where(lane < 64, r[3], r[4]),
        jnp.where(lane < 16, r[4], jnp.where(lane < 96, r[5], r[6])),
        jnp.where(lane < 48, r[6], r[7]),
    ]


def kernel(
    t_hbm, d_hbm, o_hbm, v_hbm, oooo_hbm, wd_hbm, wx_hbm, obuf,
    tf, dbuf, ov, vbuf, ob, wdp, wxb,
    tcol, ty, tr1, zt, wxs, tb, l3, r3a, r3b, r5a, r5b, zf, zg, gps, gpz, fbuf, gbuf, gown, frecv, grecv,
    xp, prx, pown, xrecv, xpart, xyrecv, msend, mfull,
    lsem, ss, rs,
):
    r = lax.axis_index("row")
    c = lax.axis_index("col")
    k = lax.rem(r, 2)
    x = r // 2
    p1 = r + 1 - 2 * k
    p2 = lax.rem(r + 2, 4)
    p3 = lax.rem(p1 + 2, 4)
    diag = x == c
    off = x != c
    d_p, d_x, d_d, d_y, d_z = (c, p1), (c, p2), (c, p3), (1 - c, r), (1 - c, p1)
    other = 2 * (1 - x)
    own = 2 * x

    def rc(src, dst, leave, arrive, dev):
        return pltpu.make_async_remote_copy(
            src_ref=src, dst_ref=dst, send_sem=ss.at[leave], recv_sem=rs.at[arrive],
            device_id=dev, device_id_type=MESH,
        )

    def wide(n, base=0):
        return pl.ds(pl.multiple_of(base + n * WIDE, LANE), WIDE)

    def half(h):
        return pl.ds(32 * h, 32)

    def quarter(q):
        return pl.ds(16 * q, 16)

    def ld_t(q):
        return pltpu.make_async_copy(t_hbm.at[quarter(q)], tf.at[quarter(q)], lsem.at[q])

    ld_v = pltpu.make_async_copy(v_hbm, vbuf.at[pl.ds(pl.multiple_of(64 * k, 64), 1600)], lsem.at[4])
    ld_wd = pltpu.make_async_copy(wd_hbm, wdp.at[:, pl.ds(0, VIRT)], lsem.at[5])
    ld_wx = pltpu.make_async_copy(wx_hbm, wxb, lsem.at[6])
    ld_o = pltpu.make_async_copy(o_hbm, ov, lsem.at[7])
    ld_d = pltpu.make_async_copy(d_hbm, dbuf, lsem.at[8])
    ld_oooo = pltpu.make_async_copy(oooo_hbm.at[pl.ds(pl.multiple_of(ROWS * r, ROWS), ROWS)], ob, lsem.at[9])
    for q in range(4):
        ld_t(q).start()

    barrier = pltpu.get_barrier_semaphore()
    for dev in (d_p, d_x, d_d, d_y, d_z):
        pl.semaphore_signal(barrier, inc=1, device_id=dev, device_id_type=MESH)
    for ld in (ld_wx, ld_wd, ld_v, ld_o, ld_oooo, ld_d):
        ld.start()

    def t_x(q, blk):
        return rc(tcol.at[blk, quarter(q)], tcol.at[blk, quarter(q)], S_TX, T_X + q, d_x)

    def t_y(q):
        return rc(tcol.at[r, quarter(q)], ty.at[quarter(q)], S_TY, T_Y + min(q, 2), d_y)

    def t_y_in():
        return rc(tcol.at[r, half(1)], ty.at[half(1)], S_TY, T_Y + 2, d_y)

    def t_fwd(q):
        return rc(tcol.at[p2, quarter(q)], tcol.at[p2, quarter(q)], S_FWD, T_FWD + q // 2, d_p)

    def t_fwd_in(h):
        return rc(tcol.at[p3, half(h)], tcol.at[p3, half(h)], S_FWD, T_FWD + h, d_p)

    def t_p(blk):
        return rc(tcol.at[blk], tcol.at[blk], S_TP, T_P, d_p)

    def my_k(core):
        return pl.ds(pl.multiple_of(1536 * core, LANE), KPAD)

    def r_p(blk):
        return rc(ty.at[:, my_k(1 - k)], tr1.at[blk], S_R, R_P, d_p)

    def r_x(q, core):
        slot = R_Y if q else R_X + lax.rem(k + core, 2)
        return rc(ty.at[quarter(q), my_k(core)], tr1.at[r, quarter(q)], S_R, slot, (c, other + core))

    def r_y(q, core):
        slot = R_Y + 1 if q == 1 else R_Y + 2 + lax.rem(k + core, 2)
        return rc(tcol.at[p2, quarter(q), my_k(core)], tr1.at[p2, quarter(q)], S_R, slot, (1 - c, own + core))

    def r_y_in(core):
        slot = R_Y + 2 + lax.rem(k + core, 2)
        return rc(tr1.at[p2, half(1)], tr1.at[p2, half(1)], S_R, slot, (1 - c, own + core))

    for q in range(4):
        ld_t(q).wait()
        tcol[r, quarter(q)] = tf[quarter(q)].astype(BF16)
        if q == 0:
            pl.semaphore_wait(barrier, 5)
        if q < 2:
            t_x(q, r).start()
        else:
            pl.when(off)(t_x(q, r).start)
        if q < 3:
            t_y(q).start()
        else:
            pl.when(off)(t_y(q).start)
    t_p(r).start()

    lane32 = lax.broadcasted_iota(jnp.int32, (32, LANE), 1)
    lane40 = lax.broadcasted_iota(jnp.int32, (HALF_V, LANE), 1)
    lane16 = lax.broadcasted_iota(jnp.int32, (16, LANE), 1)
    vbuf[pl.ds(pl.multiple_of(1600 * (1 - k), 64), 64)] = jnp.zeros((64, COLS), BF16)
    wdp[:, pl.ds(VIRT, 48)] = jnp.zeros((OCC, 48, WIDE), BF16)

    def slabs(ref, h, col_half):
        @pl.loop(0, NCH)
        def _(g):
            parts = [
                ref[half(h), pl.ds(pl.multiple_of(g * WIDE + LANE * m, LANE), LANE)].astype(F32)
                for m in range(5)
            ]
            for q, seg in enumerate(split_segments(parts, lane32)):
                zt[h, pl.ds(pl.multiple_of((col_half * 40 + g * 8 + q) * ZS, 8), 32)] = seg

    def regroup(h, vh, l3_rows, tb_at):
        def rows(ik):
            return zt[h, pl.ds(HALF_V * ZS * vh + ik, HALF_V, stride=ZS)]

        @pl.loop(0, OCC)
        def _(kk):
            blk = jnp.concatenate([rows(kk), rows(OCC + kk)], axis=0).astype(BF16)
            l3[l3_rows, pl.ds(pl.multiple_of(kk * LANE, LANE), LANE)] = blk

        for i in BOTH:
            @pl.loop(0, OCC // 2)
            def _(k2):
                blk = jnp.concatenate([rows(i * OCC + 2 * k2), rows(i * OCC + 2 * k2 + 1)], axis=0).astype(BF16)
                tb[tb_at + i, pl.ds(pl.multiple_of(k2 * VIRT, 16), VIRT)] = blk

    def r3(rows):
        return jnp.dot(l3[rows], wdp[...].reshape(OCC * LANE, WIDE), preferred_element_type=F32)

    def r5(vh, first, count):
        rhs = jnp.concatenate([tb[first + i] for i in range(count)], axis=1)
        return lax.dot_general(wxs[vh], rhs, (((0,), (0,)), ((), ())), preferred_element_type=F32)

    def s_before():
        for h in BOTH:
            slabs(tf, h, c)
        ld_wx.wait()

        @pl.loop(0, OCC // 2)
        def _(k2):
            w = [wxb[2 * k2 + e].astype(F32) for e in BOTH]
            at = pl.ds(pl.multiple_of(k2 * VIRT, 16), VIRT)
            for vh in BOTH:
                part = [w[e][HALF_V * vh:HALF_V * vh + 40] for e in BOTH]
                wxs[vh, at] = jnp.concatenate(part, axis=0).astype(BF16)

        for h in BOTH:
            regroup(h, c, pl.ds(VIRT * h, VIRT), 2 * h)
        ld_wd.wait()
        r3a[...] = r3(pl.ds(0, 2 * VIRT))
        r5a[...] = r5(c, 0, 4)

    def s_prep(h):
        slabs(ty, h, 1 - c)
        regroup(h, 1 - c, pl.ds(0, VIRT), 0)

    def s_blocks(h):
        r3b[...] = r3(pl.ds(0, VIRT))
        r5b[...] = r5a[:, 256 * h:256 * h + 256] + r5(1 - c, 0, 2)

        @pl.loop(0, 2)
        def _(i):
            rows_a = pl.ds(pl.multiple_of(VIRT * h + HALF_V * i, 8), HALF_V)
            rows_b = pl.ds(pl.multiple_of(HALF_V * i, 8), HALF_V)
            seg_a = split_segments([r3a[rows_a, pl.ds(LANE * m, LANE)] for m in range(5)], lane40)
            seg_b = split_segments([r3b[rows_b, pl.ds(LANE * m, LANE)] for m in range(5)], lane40)
            lanes = pl.ds(pl.multiple_of(i * LANE, LANE), LANE)
            for j in range(8):
                s_a = seg_a[j] - r5b[pl.ds(pl.multiple_of(j * VIRT + HALF_V * c, 8), HALF_V), lanes]
                s_b = seg_b[j] - r5b[pl.ds(pl.multiple_of(j * VIRT + HALF_V * (1 - c), 8), HALF_V), lanes]
                row = (j // 4) * 16 + (2 * h + i) * 4 + j % 4
                zf[pl.ds(HALF_V * ZS * c + row, HALF_V, stride=ZS)] = s_a
                zf[pl.ds(HALF_V * ZS * (1 - c) + row, HALF_V, stride=ZS)] = s_b
                both = [jnp.where(c == 0, s_a, s_b), jnp.where(c == 0, s_b, s_a), jnp.zeros((48, LANE), F32)]
                row = jnp.where(diag, j * 4 + 2 * h + i, h * 16 + j * 2 + i)
                zg[pl.ds(row, VIRT, stride=ZS)] = jnp.transpose(jnp.concatenate(both, axis=0))[:VIRT]

    def tile_at(base, n, m):
        return pl.ds(pl.multiple_of(base + n * WIDE + LANE * m, LANE), LANE)

    def slab(z, g, q, row, size):
        return z[pl.ds(pl.multiple_of((g * 8 + q) * ZS + row, 8), size)]

    def g_y(n, h, b):
        return rc(gbuf.at[b, h, :, wide(n)], grecv.at[k, h, :, wide(n)], S_G, G_Y + k, (1 - c, own + b))

    def g_y_in(core):
        return rc(grecv.at[core], grecv.at[core], S_G, G_Y + core, d_y)

    def g_d(h):
        return rc(gown.at[1 - k, h], grecv.at[k, h], S_GD, G_D, d_p)

    def g_d_in():
        return rc(gown.at[1 - k], grecv.at[1 - k], S_GD, G_D, d_p)

    def f_y_in(h):
        rows = pl.ds(8 * h, 8)
        return rc(frecv.at[:, rows], frecv.at[:, rows], S_F, F_Y + h, d_y)

    def f_y(n, h):
        rows = pl.ds(8 * h, 8)
        return rc(fbuf.at[:, rows, wide(n, COLS * (1 - c))], frecv.at[:, rows, wide(n)], S_F, F_Y + h, d_y)

    def g_off(h):
        lane8 = lax.broadcasted_iota(jnp.int32, (8, LANE), 1)

        def flat(dst, n, hf):
            for b in BOTH:
                segs = [slab(zg, n + NCH * hf, q, 16 * h + 8 * b, 8) for q in range(8)]
                for m, tile in enumerate(join_segments(segs, lane8)):
                    dst[b, h, :, tile_at(0, n, m)] = tile

        @pl.loop(0, NCH)
        def _(n):
            flat(gown, n, c)

        g_d(h).start()

        @pl.loop(0, NCH)
        def _(n):
            flat(gbuf, n, 1 - c)
            for b in BOTH:
                g_y(n, h, b).start()

        grecv[k, h] = gown[k, h]

    def f_off(h, hf, first=0, last=NCH):
        lane8 = lax.broadcasted_iota(jnp.int32, (8, LANE), 1)
        rows = pl.ds(8 * h, 8)

        @pl.loop(first, last)
        def _(n):
            for b in BOTH:
                segs = [slab(zf, n + NCH * hf, q, 16 * b + 8 * h, 8) for q in range(8)]
                for m, tile in enumerate(join_segments(segs, lane8)):
                    fbuf[b, rows, tile_at(COLS * hf, n, m)] = tile
            if hf is not c:
                f_y(n, h).start()

    def g_p():
        return rc(gps, gpz, S_G, G_P, d_p)

    def give_g():
        @pl.loop(0, VIRT, unroll=8)
        def _(v):
            gps[v] = zg[pl.ds(pl.multiple_of(v * ZS + 16 * (1 - k), 8), 16)]

        g_p().start()

    def q_diag():
        g_p().wait_recv()

        def flat(hf, send):
            @pl.loop(0, NCH)
            def _(n):
                for b, mine in ((k, True), (1 - k, False)):
                    row = pl.multiple_of(16 * b, 16)
                    segs = []
                    for q in range(8):
                        g = n + NCH * hf
                        extra = slab(zg, g, q, row, 16) if mine else gpz[g * 8 + q]
                        segs.append(slab(zf, g, q, row, 16) + extra)
                    for m, tile in enumerate(join_segments(segs, lane16)):
                        fbuf[b, :, tile_at(COLS * hf, n, m)] = tile
                if send:
                    for h in BOTH:
                        f_y(n, h).start()

        flat(1 - c, True)
        flat(c, False)

    s_before()

    early, late = 1 - x, x

    def pair(h, cols, step):
        ts = pl.ds(2 * h, 2)
        return rc(xp.at[p3, ts, :, :, cols], prx.at[ts, :, :, cols], S_PAIR, E_D + 3 * h + step, d_p)

    def cross(hf, h, cols, slot):
        ts = pl.ds(2 * h, 2)
        return rc(xp.at[p2, ts, hf, :, cols], xrecv.at[ts, hf, :, cols], S_X, slot, d_x)

    def over_columns(step):
        @pl.loop(0, 2)
        def _(g):
            step(pl.ds(pl.multiple_of(g * 2 * WIDE, LANE), 2 * WIDE), (2 * g, 2 * g + 1))

        step(pl.ds(4 * WIDE, WIDE), (4,))

    def ladder_0():
        def step(cols, ns):
            lhs = tr1[pl.ds(other, 2), half(0)].reshape(64, KPAD)
            prod = jnp.dot(lhs, vbuf[:, cols], preferred_element_type=F32)
            xp[pl.ds(other, 2), pl.ds(0, 2), :, :, cols] = prod.reshape(2, 2, 2, 8, -1)
            pair(0, cols, ns[0] // 2).start()

        over_columns(step)

    def ladder_1():
        def step(cols, ns):
            lhs = jnp.concatenate(
                [tr1[pl.ds(other, 2), half(1)].reshape(64, KPAD), tr1[pl.ds(own, 2)].reshape(LANE, KPAD)], axis=0
            )
            prod = jnp.dot(lhs, vbuf[:, cols], preferred_element_type=F32)
            xp[pl.ds(other, 2), pl.ds(2, 2), :, :, cols] = prod[:64].reshape(2, 2, 2, 8, -1)
            xp[pl.ds(own, 2), :, :, :, cols] = prod[64:].reshape(2, 4, 2, 8, -1)
            pair(1, cols, ns[0] // 2).start()
            rc(xp.at[p1, :, :, :, cols], pown.at[:, :, :, cols], S_OUT, O_D, d_p).start()

        over_columns(step)

    def combine(h, first=0, last=3):
        ts = pl.ds(2 * h, 2)
        for step in range(first, last):
            ns = STEPS[step]
            cols = pl.ds(ns[0] * WIDE, len(ns) * WIDE)
            pair(h, cols, step).wait_recv()
            xp[p2, ts, :, :, cols] += prx[ts, :, :, cols]
            cross(early, h, cols, E_X).start()

    def late_pass(h):
        def step(cols, ns):
            for t in (2 * h, 2 * h + 1):
                g2 = [grecv[core, hh, pl.ds(2 * t, 2), cols] for core in BOTH for hh in BOTH]
                xp[p2, t, late, :, cols] += jnp.concatenate(g2, axis=0)
            cross(late, h, cols, L_X + 1 + ns[0] // 2 if h else L_X).start()

        over_columns(step)

    def x_y():
        return rc(xpart, xyrecv, S_XY, X_Y, d_y)

    def x_part():
        xpart[...] = lax.dot_general(
            ov[...], tcol[...].reshape(4 * ROWS, COLS), (((1,), (1,)), ((), ())), preferred_element_type=F32
        )
        x_y().start()

    def take(h):
        tr1[pl.ds(other, 2), half(h)] = tcol[pl.ds(other, 2), half(h), my_k(k)]

    def send_m():
        x_y().wait_recv()
        m_rows = (ob[...].astype(F32) + 0.5 * (xpart[...] + xyrecv[...])).astype(BF16)
        for q in range(4):
            msend[q] = m_rows[:, q * ROWS:(q + 1) * ROWS]
        mfull[r] = msend[r]
        for cp in m_out():
            cp.start()

    def m_out():
        return (
            rc(msend.at[p1], mfull.at[r], S_M, M_1, d_p),
            rc(msend.at[p2], mfull.at[r], S_M, M_2, d_x),
            rc(msend.at[p3], mfull.at[r], S_M, M_3, d_d),
        )

    def m_in():
        return (
            rc(msend.at[p1], mfull.at[p1], S_M, M_1, d_p),
            rc(msend.at[p2], mfull.at[p2], S_M, M_2, d_x),
            rc(msend.at[p3], mfull.at[p3], S_M, M_3, d_d),
        )

    @pl.when(diag)
    def _():
        t_y(0).wait_recv()
        for cc in (1, 0):
            r_x(0, cc).start()
        t_x(0, p2).wait_recv()
        t_fwd(0).start()
        t_y(1).wait_recv()
        r_x(1, k).start()
        t_x(1, p2).wait_recv()
        t_fwd(1).start()
        r_y(1, 1 - k).start()
        t_y(3).start()
        for q in range(2, 4):
            t_x(q, r).start()
        t_fwd_in(0).wait_recv()
        take(0)
        ld_v.wait()
        ladder_0()
        s_prep(0)
        for q in range(2, 4):
            t_x(q, p2).wait_recv()
            t_fwd(q).start()
            for cc in (1, 0):
                r_y(q, cc).start()
        combine(0)
        s_blocks(0)
        t_p(p1).wait_recv()
        tr1[r] = tcol[r, :, my_k(k)]
        tr1[p1] = tcol[p1, :, my_k(k)]
        t_fwd_in(1).wait_recv()
        take(1)
        ladder_1()
        ld_o.wait()
        x_part()
        combine(1)
        t_y_in().wait_recv()
        s_prep(1)
        s_blocks(1)
        give_g()
        q_diag()
        for core in BOTH:
            g_y_in(core).wait_recv()
        late_pass(0)
        ld_oooo.wait()
        send_m()
        late_pass(1)

    @pl.when(off)
    def _():
        for q in BOTH:
            t_y(q).wait_recv()
        s_prep(0)
        s_blocks(0)
        g_off(0)
        for q in BOTH:
            t_x(q, p2).wait_recv()
            t_fwd(q).start()
        f_off(0, 1 - c, 0, 3)
        ld_v.wait()
        for cc in (1, 0):
            r_x(0, cc).wait_recv()
        r_x(1, k).wait_recv()
        r_y(1, 1 - k).wait_recv()
        ladder_0()
        combine(0, 0, 1)
        t_y_in().wait_recv()
        r_p(r).start()
        tr1[r] = ty[:, my_k(k)]
        s_prep(1)
        combine(0, 1)
        s_blocks(1)
        for q in range(2, 4):
            t_x(q, p2).wait_recv()
            t_fwd(q).start()
        g_off(1)
        g_d_in().wait_recv()
        late_pass(0)
        for cc in (1, 0):
            r_y_in(cc).wait_recv()
        r_p(p1).wait_recv()
        ladder_1()
        t_p(p1).wait_recv()
        for h in BOTH:
            t_fwd_in(h).wait_recv()
        ld_o.wait()
        x_part()
        f_off(0, 1 - c, 3)
        ld_oooo.wait()
        send_m()
        combine(1)
        late_pass(1)
        f_off(1, 1 - c)
        for h in BOTH:
            f_off(h, c)

    for cp in m_in():
        cp.wait_recv()
    ld_d.wait()
    rc(xp.at[p1], pown, S_OUT, O_D, d_p).wait_recv()
    for h in BOTH:
        f_y_in(h).wait_recv()
    rc(xp.at[p2, :, x], xrecv.at[:, x], S_X, E_X, d_x).wait_recv()
    cross(1 - x, 0, pl.ds(0, COLS), L_X).wait_recv()

    def finish(cols, ns):
        cross(1 - x, 1, cols, L_X + 1 + ns[0] // 2).wait_recv()
        width = len(ns) * WIDE
        r2 = lax.dot_general(
            mfull[...].reshape(4 * ROWS, ROWS), tcol[:, :, cols].reshape(4 * ROWS, width),
            (((0,), (0,)), ((), ())), preferred_element_type=F32,
        )
        part = xp[r, :, :, :, cols] + pown[:, :, :, cols] + xrecv[:, :, :, cols]
        obuf[:, cols] = ov[:, cols].astype(F32) + r2 + part.reshape(ROWS, width)
        mine = pl.ds(pl.multiple_of(COLS * c + ns[0] * WIDE, LANE), width)
        for i in range(4):
            for ref, hf, at in ((fbuf, c, mine), (frecv, 1 - c, cols)):
                f8 = jnp.concatenate([ref[b, pl.ds(4 * i, 4), at] for b in BOTH], axis=0)
                rows = pl.ds(pl.multiple_of(16 * i + 8 * hf, 8), 8)
                obuf[rows, cols] += f8
        obuf[:, cols] = obuf[:, cols] / dbuf[:, cols]

    over_columns(finish)

    rc(tcol.at[r], tcol.at[r], S_TX, T_X, d_x).wait_send()
    rc(tcol.at[r], ty, S_TY, T_Y, d_y).wait_send()
    rc(tcol.at[p2], tcol.at[p2], S_FWD, T_FWD, d_p).wait_send()
    t_p(r).wait_send()
    rc(xp.at[p3], prx, S_PAIR, E_D, d_p).wait_send()
    rc(xp.at[p1], pown, S_OUT, O_D, d_p).wait_send()
    rc(xp.at[p2], xrecv, S_X, E_X, d_x).wait_send()
    rc(frecv, frecv, S_F, F_Y, d_y).wait_send()
    x_y().wait_send()
    rc(msend.at[pl.ds(0, 3)], mfull.at[pl.ds(0, 3)], S_M, M_1, d_p).wait_send()

    @pl.when(diag)
    def _():
        g_p().wait_send()
        rc(tr1.at[pl.ds(0, 2)], tr1.at[pl.ds(0, 2)], S_R, R_Y, d_y).wait_send()

    @pl.when(off)
    def _():
        r_p(r).wait_send()
        rc(gbuf, grecv, S_G, G_Y, d_y).wait_send()
        g_d_in().wait_send()


def solution(mesh):
    def sweep(t_blk, d_blk, o_blk, v_blk, oooo, wd_blk, wx_blk):
        any_spec = pl.BlockSpec(memory_space=pl.ANY)
        vm = pltpu.VMEM
        return pl.pallas_call(
            kernel,
            out_shape=pltpu.VMEM((ROWS, COLS), F32),
            in_specs=[any_spec] * 7,
            out_specs=pl.BlockSpec(memory_space=pltpu.VMEM),
            scratch_shapes=[
                vm((ROWS, COLS), F32),
                vm((ROWS, COLS), F32),
                vm((ROWS, COLS), BF16),
                vm((KPAD, COLS), BF16),
                vm((ROWS, 256), BF16),
                vm((OCC, LANE, WIDE), BF16),
                vm((OCC, VIRT, WIDE), BF16),
                vm((4, ROWS, COLS), BF16),
                vm((ROWS, COLS), BF16),
                vm((4, ROWS, KPAD), BF16),
                vm((2, VIRT * ZS, LANE), F32),
                vm((2, WIDE, WIDE), BF16),
                vm((4, WIDE, LANE), BF16),
                vm((2 * VIRT, OCC * LANE), BF16),
                vm((2 * VIRT, WIDE), F32),
                vm((VIRT, WIDE), F32),
                vm((WIDE, 512), F32),
                vm((WIDE, 256), F32),
                vm((VIRT * ZS, LANE), F32),
                vm((VIRT * ZS, LANE), F32),
                vm((VIRT, 16, LANE), F32),
                vm((VIRT, 16, LANE), F32),
                vm((2, 16, 2 * COLS), F32),
                vm((2, 2, 8, COLS), F32),
                vm((2, 2, 8, COLS), F32),
                vm((2, 16, COLS), F32),
                vm((2, 2, 8, COLS), F32),
                vm((4, 4, 2, 8, COLS), F32),
                vm((4, 2, 8, COLS), F32),
                vm((4, 2, 8, COLS), F32),
                vm((4, 2, 8, COLS), F32),
                vm((ROWS, 256), F32),
                vm((ROWS, 256), F32),
                vm((4, ROWS, ROWS), BF16),
                vm((4, ROWS, ROWS), BF16),
                pltpu.SemaphoreType.DMA((10,)),
                pltpu.SemaphoreType.DMA((N_SEND,)),
                pltpu.SemaphoreType.DMA((N_RECV,)),
            ],
            compiler_params=pltpu.CompilerParams(
                collective_id=0, has_side_effects=True, vmem_limit_bytes=54 * 1024 * 1024
            ),
            name="ccd_sweep",
        )(t_blk, d_blk, o_blk, v_blk, oooo, wd_blk.reshape(OCC, VIRT, WIDE), wx_blk.reshape(OCC, VIRT, WIDE))

    amp = P("row", "col")
    wide_spec = P(None, "col")
    return jax.shard_map(
        sweep, mesh=mesh, in_specs=(amp, amp, amp, amp, P(), wide_spec, wide_spec), out_specs=amp, check_vma=False
    )
```

```python
import functools

import jax
import jax.numpy as jnp
from jax import lax
from jax.experimental import pallas as pl
from jax.experimental.pallas import tpu as pltpu
from jax.sharding import PartitionSpec as P

MESH = pl.DeviceIdType.MESH
F32 = jnp.float32
BF16 = jnp.bfloat16

OCC = 16
VIRT = 80
ROWS = 64
COLS = 3200
KPAD = 1664
LANE = 128
HALF_V = VIRT // 2
BOTH = range(2)
WIDE = 640
NCH = COLS // WIDE
ZS = 40

T_X, T_Y, T_P, T_FWD, R_P, G_P, R_X, R_Y, G_Y = 0, 4, 7, 8, 10, 10, 11, 13, 11
E_D, G_D, O_D, E_X, L_X, F_Y, X_Y, M_1, M_2, M_3 = 17, 23, 24, 25, 26, 30, 32, 33, 34, 35
N_RECV = 36
S_TX, S_TY, S_TP, S_FWD, S_R, S_PAIR, S_OUT, S_X, S_F, S_G, S_XY, S_M, S_GD = range(13)
N_SEND = 13
STEPS = (0, 1), (2, 3), (4,)


def split_segments(parts, lane):
    out = []
    for q in range(8):
        m, s = divmod(80 * q, LANE)
        seg = parts[m]
        if s:
            seg = pltpu.roll(seg, LANE - s, axis=1)
            if s + 80 > LANE:
                seg = jnp.where(lane < LANE - s, seg, pltpu.roll(parts[m + 1], LANE - s, axis=1))
        out.append(jnp.where(lane < 80, seg, 0.0))
    return out


def join_segments(segs, lane):
    r = [segs[0]] + [pltpu.roll(segs[q], (80 * q) % LANE, axis=1) for q in range(1, 8)]
    return [
        jnp.where(lane < 80, r[0], r[1]),
        jnp.where(lane < 32, r[1], jnp.where(lane < 112, r[2], r[3])),
        jnp.where(lane < 64, r[3], r[4]),
        jnp.where(lane < 16, r[4], jnp.where(lane < 96, r[5], r[6])),
        jnp.where(lane < 48, r[6], r[7]),
    ]


def kernel(
    t_hbm, d_hbm, o_hbm, v_hbm, oooo_hbm, wd_hbm, wx_hbm, obuf,
    tf, dbuf, ov, vbuf, ob, wdp, wxb,
    tcol, ty, tr1, zt, wxs, tb, l3, r3a, r3b, r5a, r5b, zf, zg, gps, gpz, fbuf, gbuf, gown, frecv, grecv,
    xp, prx, pown, xrecv, xpart, xyrecv, msend, mfull,
    lsem, ss, rs,
):
    r = lax.axis_index("row")
    c = lax.axis_index("col")
    k = lax.rem(r, 2)
    x = r // 2
    p1 = r + 1 - 2 * k
    p2 = lax.rem(r + 2, 4)
    p3 = lax.rem(p1 + 2, 4)
    diag = x == c
    off = x != c
    d_p, d_x, d_d, d_y, d_z = (c, p1), (c, p2), (c, p3), (1 - c, r), (1 - c, p1)
    other = 2 * (1 - x)
    own = 2 * x

    def rc(src, dst, leave, arrive, dev):
        return pltpu.make_async_remote_copy(
            src_ref=src, dst_ref=dst, send_sem=ss.at[leave], recv_sem=rs.at[arrive],
            device_id=dev, device_id_type=MESH,
        )

    def wide(n, base=0):
        return pl.ds(pl.multiple_of(base + n * WIDE, LANE), WIDE)

    def half(h):
        return pl.ds(32 * h, 32)

    def quarter(q):
        return pl.ds(16 * q, 16)

    def ld_t(q):
        return pltpu.make_async_copy(t_hbm.at[quarter(q)], tf.at[quarter(q)], lsem.at[q])

    ld_v = pltpu.make_async_copy(v_hbm, vbuf.at[pl.ds(pl.multiple_of(64 * k, 64), 1600)], lsem.at[4])
    ld_wd = pltpu.make_async_copy(wd_hbm, wdp.at[:, pl.ds(0, VIRT)], lsem.at[5])
    ld_wx = pltpu.make_async_copy(wx_hbm, wxb, lsem.at[6])
    ld_o = pltpu.make_async_copy(o_hbm, ov, lsem.at[7])
    ld_d = pltpu.make_async_copy(d_hbm, dbuf, lsem.at[8])
    ld_oooo = pltpu.make_async_copy(oooo_hbm.at[pl.ds(pl.multiple_of(ROWS * r, ROWS), ROWS)], ob, lsem.at[9])
    for q in range(4):
        ld_t(q).start()

    barrier = pltpu.get_barrier_semaphore()
    for dev in (d_p, d_x, d_d, d_y, d_z):
        pl.semaphore_signal(barrier, inc=1, device_id=dev, device_id_type=MESH)
    for ld in (ld_wx, ld_wd, ld_v, ld_o, ld_oooo, ld_d):
        ld.start()

    def t_x(q, blk):
        return rc(tcol.at[blk, quarter(q)], tcol.at[blk, quarter(q)], S_TX, T_X + q, d_x)

    def t_y(q):
        return rc(tcol.at[r, quarter(q)], ty.at[quarter(q)], S_TY, T_Y + min(q, 2), d_y)

    def t_y_in():
        return rc(tcol.at[r, half(1)], ty.at[half(1)], S_TY, T_Y + 2, d_y)

    def t_fwd(q):
        return rc(tcol.at[p2, quarter(q)], tcol.at[p2, quarter(q)], S_FWD, T_FWD + q // 2, d_p)

    def t_fwd_in(h):
        return rc(tcol.at[p3, half(h)], tcol.at[p3, half(h)], S_FWD, T_FWD + h, d_p)

    def t_p(blk):
        return rc(tcol.at[blk], tcol.at[blk], S_TP, T_P, d_p)

    def my_k(core):
        return pl.ds(pl.multiple_of(1536 * core, LANE), KPAD)

    def r_p(blk):
        return rc(ty.at[:, my_k(1 - k)], tr1.at[blk], S_R, R_P, d_p)

    def r_x(q, core):
        slot = R_Y if q else R_X + lax.rem(k + core, 2)
        return rc(ty.at[quarter(q), my_k(core)], tr1.at[r, quarter(q)], S_R, slot, (c, other + core))

    def r_y(q, core):
        slot = R_Y + 1 if q == 1 else R_Y + 2 + lax.rem(k + core, 2)
        return rc(tcol.at[p2, quarter(q), my_k(core)], tr1.at[p2, quarter(q)], S_R, slot, (1 - c, own + core))

    def r_y_in(core):
        slot = R_Y + 2 + lax.rem(k + core, 2)
        return rc(tr1.at[p2, half(1)], tr1.at[p2, half(1)], S_R, slot, (1 - c, own + core))

    def send_t(q):
        if q < 2:
            t_x(q, r).start()
        else:
            pl.when(off)(t_x(q, r).start)
        if q < 3:
            t_y(q).start()
        else:
            pl.when(off)(t_y(q).start)

    for q in range(4):
        ld_t(q).wait()
        tcol[r, quarter(q)] = tf[quarter(q)].astype(BF16)
        if q == 0:
            pl.semaphore_wait(barrier, 5)
            send_t(q)
        elif q == 1:
            @pl.when(k == 0)
            def _():
                send_t(q)

    t_p(r).start()

    lane32 = lax.broadcasted_iota(jnp.int32, (32, LANE), 1)
    lane40 = lax.broadcasted_iota(jnp.int32, (HALF_V, LANE), 1)
    lane16 = lax.broadcasted_iota(jnp.int32, (16, LANE), 1)
    vbuf[pl.ds(pl.multiple_of(1600 * (1 - k), 64), 64)] = jnp.zeros((64, COLS), BF16)
    wdp[:, pl.ds(VIRT, 48)] = jnp.zeros((OCC, 48, WIDE), BF16)

    def slabs(ref, h, col_half):
        @pl.loop(0, NCH)
        def _(g):
            parts = [
                ref[half(h), pl.ds(pl.multiple_of(g * WIDE + LANE * m, LANE), LANE)].astype(F32)
                for m in range(5)
            ]
            for q, seg in enumerate(split_segments(parts, lane32)):
                zt[h, pl.ds(pl.multiple_of((col_half * 40 + g * 8 + q) * ZS, 8), 32)] = seg

    def regroup(h, vh, l3_rows, tb_at):
        def rows(ik):
            return zt[h, pl.ds(HALF_V * ZS * vh + ik, HALF_V, stride=ZS)]

        @pl.loop(0, OCC)
        def _(kk):
            blk = jnp.concatenate([rows(kk), rows(OCC + kk)], axis=0).astype(BF16)
            l3[l3_rows, pl.ds(pl.multiple_of(kk * LANE, LANE), LANE)] = blk

        for i in BOTH:
            @pl.loop(0, OCC // 2)
            def _(k2):
                blk = jnp.concatenate([rows(i * OCC + 2 * k2), rows(i * OCC + 2 * k2 + 1)], axis=0).astype(BF16)
                tb[tb_at + i, pl.ds(pl.multiple_of(k2 * VIRT, 16), VIRT)] = blk

    def r3(rows):
        return jnp.dot(l3[rows], wdp[...].reshape(OCC * LANE, WIDE), preferred_element_type=F32)

    def r5(vh, first, count):
        rhs = jnp.concatenate([tb[first + i] for i in range(count)], axis=1)
        return lax.dot_general(wxs[vh], rhs, (((0,), (0,)), ((), ())), preferred_element_type=F32)

    def s_before():
        for h in BOTH:
            slabs(tf, h, c)
        ld_wx.wait()

        @pl.loop(0, OCC // 2)
        def _(k2):
            w = [wxb[2 * k2 + e].astype(F32) for e in BOTH]
            at = pl.ds(pl.multiple_of(k2 * VIRT, 16), VIRT)
            for vh in BOTH:
                part = [w[e][HALF_V * vh:HALF_V * vh + 40] for e in BOTH]
                wxs[vh, at] = jnp.concatenate(part, axis=0).astype(BF16)

        for h in BOTH:
            regroup(h, c, pl.ds(VIRT * h, VIRT), 2 * h)

        @pl.when(k == 1)
        def _():
            for q in range(1, 4):
                send_t(q)

        ld_wd.wait()
        r3a[...] = r3(pl.ds(0, 2 * VIRT))
        r5a[...] = r5(c, 0, 4)

        @pl.when(k == 0)
        def _():
            for q in range(2, 4):
                send_t(q)

    def s_prep(h):
        slabs(ty, h, 1 - c)
        regroup(h, 1 - c, pl.ds(0, VIRT), 0)

    def s_blocks(h):
        r3b[...] = r3(pl.ds(0, VIRT))
        r5b[...] = r5a[:, 256 * h:256 * h + 256] + r5(1 - c, 0, 2)

        @pl.loop(0, 2)
        def _(i):
            rows_a = pl.ds(pl.multiple_of(VIRT * h + HALF_V * i, 8), HALF_V)
            rows_b = pl.ds(pl.multiple_of(HALF_V * i, 8), HALF_V)
            seg_a = split_segments([r3a[rows_a, pl.ds(LANE * m, LANE)] for m in range(5)], lane40)
            seg_b = split_segments([r3b[rows_b, pl.ds(LANE * m, LANE)] for m in range(5)], lane40)
            lanes = pl.ds(pl.multiple_of(i * LANE, LANE), LANE)
            for j in range(8):
                s_a = seg_a[j] - r5b[pl.ds(pl.multiple_of(j * VIRT + HALF_V * c, 8), HALF_V), lanes]
                s_b = seg_b[j] - r5b[pl.ds(pl.multiple_of(j * VIRT + HALF_V * (1 - c), 8), HALF_V), lanes]
                row = (j // 4) * 16 + (2 * h + i) * 4 + j % 4
                zf[pl.ds(HALF_V * ZS * c + row, HALF_V, stride=ZS)] = s_a
                zf[pl.ds(HALF_V * ZS * (1 - c) + row, HALF_V, stride=ZS)] = s_b
                both = [jnp.where(c == 0, s_a, s_b), jnp.where(c == 0, s_b, s_a), jnp.zeros((48, LANE), F32)]
                row = jnp.where(diag, j * 4 + 2 * h + i, h * 16 + j * 2 + i)
                zg[pl.ds(row, VIRT, stride=ZS)] = jnp.transpose(jnp.concatenate(both, axis=0))[:VIRT]

    def tile_at(base, n, m):
        return pl.ds(pl.multiple_of(base + n * WIDE + LANE * m, LANE), LANE)

    def slab(z, g, q, row, size):
        return z[pl.ds(pl.multiple_of((g * 8 + q) * ZS + row, 8), size)]

    def g_y(n, h, b):
        return rc(gbuf.at[b, h, :, wide(n)], grecv.at[k, h, :, wide(n)], S_G, G_Y + k, (1 - c, own + b))

    def g_y_in(core):
        return rc(grecv.at[core], grecv.at[core], S_G, G_Y + core, d_y)

    def g_d(h):
        return rc(gown.at[1 - k, h], grecv.at[k, h], S_GD, G_D, d_p)

    def g_d_in():
        return rc(gown.at[1 - k], grecv.at[1 - k], S_GD, G_D, d_p)

    def f_y_in(h):
        rows = pl.ds(8 * h, 8)
        return rc(frecv.at[:, rows], frecv.at[:, rows], S_F, F_Y + h, d_y)

    def f_y(n, h):
        rows = pl.ds(8 * h, 8)
        return rc(fbuf.at[:, rows, wide(n, COLS * (1 - c))], frecv.at[:, rows, wide(n)], S_F, F_Y + h, d_y)

    def g_off(h):
        lane8 = lax.broadcasted_iota(jnp.int32, (8, LANE), 1)

        def flat(dst, n, hf):
            for b in BOTH:
                segs = [slab(zg, n + NCH * hf, q, 16 * h + 8 * b, 8) for q in range(8)]
                for m, tile in enumerate(join_segments(segs, lane8)):
                    dst[b, h, :, tile_at(0, n, m)] = tile

        @pl.loop(0, NCH)
        def _(n):
            flat(gown, n, c)

        g_d(h).start()

        @pl.loop(0, NCH)
        def _(n):
            flat(gbuf, n, 1 - c)
            for b in BOTH:
                g_y(n, h, b).start()

        grecv[k, h] = gown[k, h]

    def f_off(h, hf, first=0, last=NCH):
        lane8 = lax.broadcasted_iota(jnp.int32, (8, LANE), 1)
        rows = pl.ds(8 * h, 8)

        @pl.loop(first, last)
        def _(n):
            for b in BOTH:
                segs = [slab(zf, n + NCH * hf, q, 16 * b + 8 * h, 8) for q in range(8)]
                for m, tile in enumerate(join_segments(segs, lane8)):
                    fbuf[b, rows, tile_at(COLS * hf, n, m)] = tile
            if hf is not c:
                f_y(n, h).start()

    def g_p():
        return rc(gps, gpz, S_G, G_P, d_p)

    def give_g():
        @pl.loop(0, VIRT, unroll=8)
        def _(v):
            gps[v] = zg[pl.ds(pl.multiple_of(v * ZS + 16 * (1 - k), 8), 16)]

        g_p().start()

    def q_diag():
        g_p().wait_recv()

        def flat(hf, send):
            @pl.loop(0, NCH)
            def _(n):
                for b, mine in ((k, True), (1 - k, False)):
                    row = pl.multiple_of(16 * b, 16)
                    segs = []
                    for q in range(8):
                        g = n + NCH * hf
                        extra = slab(zg, g, q, row, 16) if mine else gpz[g * 8 + q]
                        segs.append(slab(zf, g, q, row, 16) + extra)
                    for m, tile in enumerate(join_segments(segs, lane16)):
                        fbuf[b, :, tile_at(COLS * hf, n, m)] = tile
                if send:
                    for h in BOTH:
                        f_y(n, h).start()

        flat(1 - c, True)
        flat(c, False)

    s_before()

    early, late = 1 - x, x

    def pair(h, cols, step):
        ts = pl.ds(2 * h, 2)
        return rc(xp.at[p3, ts, :, :, cols], prx.at[ts, :, :, cols], S_PAIR, E_D + 3 * h + step, d_p)

    def cross(hf, h, cols, slot):
        ts = pl.ds(2 * h, 2)
        return rc(xp.at[p2, ts, hf, :, cols], xrecv.at[ts, hf, :, cols], S_X, slot, d_x)

    def over_columns(step):
        @pl.loop(0, 2)
        def _(g):
            step(pl.ds(pl.multiple_of(g * 2 * WIDE, LANE), 2 * WIDE), (2 * g, 2 * g + 1))

        step(pl.ds(4 * WIDE, WIDE), (4,))

    def ladder_0():
        def step(cols, ns):
            lhs = tr1[pl.ds(other, 2), half(0)].reshape(64, KPAD)
            prod = jnp.dot(lhs, vbuf[:, cols], preferred_element_type=F32)
            xp[pl.ds(other, 2), pl.ds(0, 2), :, :, cols] = prod.reshape(2, 2, 2, 8, -1)
            pair(0, cols, ns[0] // 2).start()

        over_columns(step)

    def ladder_1():
        def step(cols, ns):
            lhs = jnp.concatenate(
                [tr1[pl.ds(other, 2), half(1)].reshape(64, KPAD), tr1[pl.ds(own, 2)].reshape(LANE, KPAD)], axis=0
            )
            prod = jnp.dot(lhs, vbuf[:, cols], preferred_element_type=F32)
            xp[pl.ds(other, 2), pl.ds(2, 2), :, :, cols] = prod[:64].reshape(2, 2, 2, 8, -1)
            xp[pl.ds(own, 2), :, :, :, cols] = prod[64:].reshape(2, 4, 2, 8, -1)
            pair(1, cols, ns[0] // 2).start()
            rc(xp.at[p1, :, :, :, cols], pown.at[:, :, :, cols], S_OUT, O_D, d_p).start()

        over_columns(step)

    def combine(h, first=0, last=3):
        ts = pl.ds(2 * h, 2)
        for step in range(first, last):
            ns = STEPS[step]
            cols = pl.ds(ns[0] * WIDE, len(ns) * WIDE)
            pair(h, cols, step).wait_recv()
            xp[p2, ts, :, :, cols] += prx[ts, :, :, cols]
            cross(early, h, cols, E_X).start()

    def late_pass(h):
        def step(cols, ns):
            for t in (2 * h, 2 * h + 1):
                g2 = [grecv[core, hh, pl.ds(2 * t, 2), cols] for core in BOTH for hh in BOTH]
                xp[p2, t, late, :, cols] += jnp.concatenate(g2, axis=0)
            cross(late, h, cols, L_X + 1 + ns[0] // 2 if h else L_X).start()

        over_columns(step)

    def x_y():
        return rc(xpart, xyrecv, S_XY, X_Y, d_y)

    def x_part():
        xpart[...] = lax.dot_general(
            ov[...], tcol[...].reshape(4 * ROWS, COLS), (((1,), (1,)), ((), ())), preferred_element_type=F32
        )
        x_y().start()

    def take(h):
        tr1[pl.ds(other, 2), half(h)] = tcol[pl.ds(other, 2), half(h), my_k(k)]

    def send_m():
        x_y().wait_recv()
        m_rows = (ob[...].astype(F32) + 0.5 * (xpart[...] + xyrecv[...])).astype(BF16)
        for q in range(4):
            msend[q] = m_rows[:, q * ROWS:(q + 1) * ROWS]
        mfull[r] = msend[r]
        for cp in m_out():
            cp.start()

    def m_out():
        return (
            rc(msend.at[p1], mfull.at[r], S_M, M_1, d_p),
            rc(msend.at[p2], mfull.at[r], S_M, M_2, d_x),
            rc(msend.at[p3], mfull.at[r], S_M, M_3, d_d),
        )

    def m_in():
        return (
            rc(msend.at[p1], mfull.at[p1], S_M, M_1, d_p),
            rc(msend.at[p2], mfull.at[p2], S_M, M_2, d_x),
            rc(msend.at[p3], mfull.at[p3], S_M, M_3, d_d),
        )

    @pl.when(diag)
    def _():
        t_y(0).wait_recv()
        for cc in (1, 0):
            r_x(0, cc).start()
        t_x(0, p2).wait_recv()
        t_fwd(0).start()
        t_y(1).wait_recv()
        r_x(1, k).start()
        t_x(1, p2).wait_recv()
        t_fwd(1).start()
        r_y(1, 1 - k).start()
        t_y(3).start()
        for q in range(2, 4):
            t_x(q, r).start()
        t_fwd_in(0).wait_recv()
        take(0)
        ld_v.wait()
        ladder_0()
        s_prep(0)
        for q in range(2, 4):
            t_x(q, p2).wait_recv()
            t_fwd(q).start()
            for cc in (1, 0):
                r_y(q, cc).start()
        combine(0)
        s_blocks(0)
        t_p(p1).wait_recv()
        tr1[r] = tcol[r, :, my_k(k)]
        tr1[p1] = tcol[p1, :, my_k(k)]
        t_fwd_in(1).wait_recv()
        take(1)
        ladder_1()
        ld_o.wait()
        x_part()
        combine(1)
        t_y_in().wait_recv()
        s_prep(1)
        s_blocks(1)
        give_g()
        q_diag()
        for core in BOTH:
            g_y_in(core).wait_recv()
        late_pass(0)
        ld_oooo.wait()
        send_m()
        late_pass(1)

    @pl.when(off)
    def _():
        for q in BOTH:
            t_y(q).wait_recv()
        s_prep(0)
        s_blocks(0)
        g_off(0)
        for q in BOTH:
            t_x(q, p2).wait_recv()
            t_fwd(q).start()
        f_off(0, 1 - c, 0, 2)
        ld_v.wait()
        for cc in (1, 0):
            r_x(0, cc).wait_recv()
        r_x(1, k).wait_recv()
        r_y(1, 1 - k).wait_recv()
        ladder_0()
        combine(0, 0, 1)
        t_y_in().wait_recv()
        r_p(r).start()
        tr1[r] = ty[:, my_k(k)]
        s_prep(1)
        combine(0, 1)
        s_blocks(1)
        for q in range(2, 4):
            t_x(q, p2).wait_recv()
            t_fwd(q).start()
        g_off(1)
        g_d_in().wait_recv()
        late_pass(0)
        for cc in (1, 0):
            r_y_in(cc).wait_recv()
        r_p(p1).wait_recv()
        ladder_1()
        t_p(p1).wait_recv()
        for h in BOTH:
            t_fwd_in(h).wait_recv()
        ld_o.wait()
        x_part()
        f_off(0, 1 - c, 2)
        ld_oooo.wait()
        send_m()
        combine(1)
        late_pass(1)
        f_off(1, 1 - c)
        for h in BOTH:
            f_off(h, c)

    for cp in m_in():
        cp.wait_recv()
    ld_d.wait()
    rc(xp.at[p1], pown, S_OUT, O_D, d_p).wait_recv()
    for h in BOTH:
        f_y_in(h).wait_recv()
    rc(xp.at[p2, :, x], xrecv.at[:, x], S_X, E_X, d_x).wait_recv()
    cross(1 - x, 0, pl.ds(0, COLS), L_X).wait_recv()

    def finish(cols, ns):
        cross(1 - x, 1, cols, L_X + 1 + ns[0] // 2).wait_recv()
        width = len(ns) * WIDE
        r2 = lax.dot_general(
            mfull[...].reshape(4 * ROWS, ROWS), tcol[:, :, cols].reshape(4 * ROWS, width),
            (((0,), (0,)), ((), ())), preferred_element_type=F32,
        )
        part = xp[r, :, :, :, cols] + pown[:, :, :, cols] + xrecv[:, :, :, cols]
        obuf[:, cols] = ov[:, cols].astype(F32) + r2 + part.reshape(ROWS, width)
        mine = pl.ds(pl.multiple_of(COLS * c + ns[0] * WIDE, LANE), width)
        for i in range(4):
            for ref, hf, at in ((fbuf, c, mine), (frecv, 1 - c, cols)):
                f8 = jnp.concatenate([ref[b, pl.ds(4 * i, 4), at] for b in BOTH], axis=0)
                rows = pl.ds(pl.multiple_of(16 * i + 8 * hf, 8), 8)
                obuf[rows, cols] += f8
        obuf[:, cols] = obuf[:, cols] / dbuf[:, cols]

    over_columns(finish)

    rc(tcol.at[r], tcol.at[r], S_TX, T_X, d_x).wait_send()
    rc(tcol.at[r], ty, S_TY, T_Y, d_y).wait_send()
    rc(tcol.at[p2], tcol.at[p2], S_FWD, T_FWD, d_p).wait_send()
    t_p(r).wait_send()
    rc(xp.at[p3], prx, S_PAIR, E_D, d_p).wait_send()
    rc(xp.at[p1], pown, S_OUT, O_D, d_p).wait_send()
    rc(xp.at[p2], xrecv, S_X, E_X, d_x).wait_send()
    rc(frecv, frecv, S_F, F_Y, d_y).wait_send()
    x_y().wait_send()
    rc(msend.at[pl.ds(0, 3)], mfull.at[pl.ds(0, 3)], S_M, M_1, d_p).wait_send()

    @pl.when(diag)
    def _():
        g_p().wait_send()
        rc(tr1.at[pl.ds(0, 2)], tr1.at[pl.ds(0, 2)], S_R, R_Y, d_y).wait_send()

    @pl.when(off)
    def _():
        r_p(r).wait_send()
        rc(gbuf, grecv, S_G, G_Y, d_y).wait_send()
        g_d_in().wait_send()


def solution(mesh):
    def sweep(t_blk, d_blk, o_blk, v_blk, oooo, wd_blk, wx_blk):
        any_spec = pl.BlockSpec(memory_space=pl.ANY)
        vm = pltpu.VMEM
        return pl.pallas_call(
            kernel,
            out_shape=pltpu.VMEM((ROWS, COLS), F32),
            in_specs=[any_spec] * 7,
            out_specs=pl.BlockSpec(memory_space=pltpu.VMEM),
            scratch_shapes=[
                vm((ROWS, COLS), F32),
                vm((ROWS, COLS), F32),
                vm((ROWS, COLS), BF16),
                vm((KPAD, COLS), BF16),
                vm((ROWS, 256), BF16),
                vm((OCC, LANE, WIDE), BF16),
                vm((OCC, VIRT, WIDE), BF16),
                vm((4, ROWS, COLS), BF16),
                vm((ROWS, COLS), BF16),
                vm((4, ROWS, KPAD), BF16),
                vm((2, VIRT * ZS, LANE), F32),
                vm((2, WIDE, WIDE), BF16),
                vm((4, WIDE, LANE), BF16),
                vm((2 * VIRT, OCC * LANE), BF16),
                vm((2 * VIRT, WIDE), F32),
                vm((VIRT, WIDE), F32),
                vm((WIDE, 512), F32),
                vm((WIDE, 256), F32),
                vm((VIRT * ZS, LANE), F32),
                vm((VIRT * ZS, LANE), F32),
                vm((VIRT, 16, LANE), F32),
                vm((VIRT, 16, LANE), F32),
                vm((2, 16, 2 * COLS), F32),
                vm((2, 2, 8, COLS), F32),
                vm((2, 2, 8, COLS), F32),
                vm((2, 16, COLS), F32),
                vm((2, 2, 8, COLS), F32),
                vm((4, 4, 2, 8, COLS), F32),
                vm((4, 2, 8, COLS), F32),
                vm((4, 2, 8, COLS), F32),
                vm((4, 2, 8, COLS), F32),
                vm((ROWS, 256), F32),
                vm((ROWS, 256), F32),
                vm((4, ROWS, ROWS), BF16),
                vm((4, ROWS, ROWS), BF16),
                pltpu.SemaphoreType.DMA((10,)),
                pltpu.SemaphoreType.DMA((N_SEND,)),
                pltpu.SemaphoreType.DMA((N_RECV,)),
            ],
            compiler_params=pltpu.CompilerParams(
                collective_id=0, has_side_effects=True, vmem_limit_bytes=54 * 1024 * 1024
            ),
            name="ccd_sweep",
        )(t_blk, d_blk, o_blk, v_blk, oooo, wd_blk.reshape(OCC, VIRT, WIDE), wx_blk.reshape(OCC, VIRT, WIDE))

    amp = P("row", "col")
    wide_spec = P(None, "col")
    return jax.shard_map(
        sweep, mesh=mesh, in_specs=(amp, amp, amp, amp, P(), wide_spec, wide_spec), out_specs=amp, check_vma=False
    )
```

```python
import functools

import jax
import jax.numpy as jnp
from jax import lax
from jax.experimental import pallas as pl
from jax.experimental.pallas import tpu as pltpu
from jax.sharding import PartitionSpec as P

MESH = pl.DeviceIdType.MESH
F32 = jnp.float32
BF16 = jnp.bfloat16

OCC = 16
VIRT = 80
ROWS = 64
COLS = 3200
KPAD = 1664
LANE = 128
HALF_V = VIRT // 2
BOTH = range(2)
WIDE = 640
NCH = COLS // WIDE
ZS = 40

T_X, T_Y, T_P, T_FWD, R_P, G_P, R_0, R_1, G_Y = 0, 4, 7, 8, 10, 10, 11, 12, 11
E_D, G_D, O_D, L_X, F_Y, X_Y, M_I = 13, 19, 20, 21, 25, 26, 27
N_RECV = 28
S_T, S_R, S_XP, S_F, S_G, S_XY, S_M, S_GD = range(8)
N_SEND = 8
STEPS = (0, 1), (2, 3), (4,)


def split_segments(parts, lane):
    out = []
    for q in range(8):
        m, s = divmod(80 * q, LANE)
        seg = parts[m]
        if s:
            seg = pltpu.roll(seg, LANE - s, axis=1)
            if s + 80 > LANE:
                seg = jnp.where(lane < LANE - s, seg, pltpu.roll(parts[m + 1], LANE - s, axis=1))
        out.append(jnp.where(lane < 80, seg, 0.0))
    return out


def join_segments(segs, lane):
    r = [segs[0]] + [pltpu.roll(segs[q], (80 * q) % LANE, axis=1) for q in range(1, 8)]
    return [
        jnp.where(lane < 80, r[0], r[1]),
        jnp.where(lane < 32, r[1], jnp.where(lane < 112, r[2], r[3])),
        jnp.where(lane < 64, r[3], r[4]),
        jnp.where(lane < 16, r[4], jnp.where(lane < 96, r[5], r[6])),
        jnp.where(lane < 48, r[6], r[7]),
    ]


def kernel(
    t_hbm, d_hbm, o_hbm, v_hbm, oooo_hbm, wd_hbm, wx_hbm, obuf,
    tf, dbuf, ov, vbuf, ob, wdp, wxb,
    tcol, ty, tr1, zt, wxs, tb, l3, r3a, r3b, r5a, r5b, zf, zg, gps, gpz, fbuf, gbuf, gown, frecv, grecv,
    xp, prx, pown, xrecv, xpart, xyrecv, msend, mfull,
    lsem, ss, rs,
):
    r = lax.axis_index("row")
    c = lax.axis_index("col")
    k = lax.rem(r, 2)
    x = r // 2
    p1 = r + 1 - 2 * k
    p2 = lax.rem(r + 2, 4)
    p3 = lax.rem(p1 + 2, 4)
    diag = x == c
    off = x != c
    d_p, d_x, d_d, d_y, d_z = (c, p1), (c, p2), (c, p3), (1 - c, r), (1 - c, p1)
    other = 2 * (1 - x)
    own = 2 * x

    def rc(src, dst, leave, arrive, dev):
        return pltpu.make_async_remote_copy(
            src_ref=src, dst_ref=dst, send_sem=ss.at[leave], recv_sem=rs.at[arrive],
            device_id=dev, device_id_type=MESH,
        )

    def wide(n, base=0):
        return pl.ds(pl.multiple_of(base + n * WIDE, LANE), WIDE)

    def half(h):
        return pl.ds(32 * h, 32)

    def quarter(q):
        return pl.ds(16 * q, 16)

    def ld_t(q):
        return pltpu.make_async_copy(t_hbm.at[quarter(q)], tf.at[quarter(q)], lsem.at[q])

    ld_v = pltpu.make_async_copy(v_hbm, vbuf.at[pl.ds(pl.multiple_of(64 * k, 64), 1600)], lsem.at[4])
    ld_wd = pltpu.make_async_copy(wd_hbm, wdp.at[:, pl.ds(0, VIRT)], lsem.at[5])
    ld_wx = pltpu.make_async_copy(wx_hbm, wxb, lsem.at[6])
    ld_o = pltpu.make_async_copy(o_hbm, ov, lsem.at[7])
    ld_d = pltpu.make_async_copy(d_hbm, dbuf, lsem.at[8])
    ld_oooo = pltpu.make_async_copy(oooo_hbm.at[pl.ds(pl.multiple_of(ROWS * r, ROWS), ROWS)], ob, lsem.at[9])
    for q in range(4):
        ld_t(q).start()

    barrier = pltpu.get_barrier_semaphore()
    for dev in (d_p, d_x, d_d, d_y, d_z):
        pl.semaphore_signal(barrier, inc=1, device_id=dev, device_id_type=MESH)
    for ld in (ld_wx, ld_wd, ld_v, ld_o, ld_oooo, ld_d):
        ld.start()

    def t_x(q, blk):
        return rc(tcol.at[blk, quarter(q)], tcol.at[blk, quarter(q)], S_T, T_X + q, d_x)

    def t_y(q):
        return rc(tcol.at[r, quarter(q)], ty.at[quarter(q)], S_T, T_Y + min(q, 2), d_y)

    def t_y_in():
        return rc(tcol.at[r, half(1)], ty.at[half(1)], S_T, T_Y + 2, d_y)

    def t_fwd(q):
        return rc(tcol.at[p2, quarter(q)], tcol.at[p2, quarter(q)], S_T, T_FWD + q // 2, d_p)

    def t_fwd_in(h):
        return rc(tcol.at[p3, half(h)], tcol.at[p3, half(h)], S_T, T_FWD + h, d_p)

    def t_p(blk):
        return rc(tcol.at[blk], tcol.at[blk], S_T, T_P, d_p)

    def my_k(core):
        return pl.ds(pl.multiple_of(1536 * core, LANE), KPAD)

    def r_p(blk):
        return rc(ty.at[:, my_k(1 - k)], tr1.at[blk], S_R, R_P, d_p)

    def r_x(q, core):
        return rc(ty.at[quarter(q), my_k(core)], tr1.at[r, quarter(q)], S_R, R_0, (c, other + core))

    def r_y(q, core):
        slot = R_0 if q == 1 else R_1
        return rc(tcol.at[p2, quarter(q), my_k(core)], tr1.at[p2, quarter(q)], S_R, slot, (1 - c, own + core))

    def r_in(h, slot):
        return rc(tr1.at[pl.ds(other, 2), half(h)], tr1.at[pl.ds(other, 2), half(h)], S_R, slot, d_y)

    def send_t(q):
        if q < 2:
            t_x(q, r).start()
        else:
            pl.when(off)(t_x(q, r).start)
        if q < 3:
            t_y(q).start()
        else:
            pl.when(off)(t_y(q).start)

    for q in range(4):
        ld_t(q).wait()
        tcol[r, quarter(q)] = tf[quarter(q)].astype(BF16)
        if q == 0:
            pl.semaphore_wait(barrier, 5)
            send_t(q)
        elif q == 1:
            @pl.when(k == 0)
            def _():
                send_t(q)

    t_p(r).start()

    lane32 = lax.broadcasted_iota(jnp.int32, (32, LANE), 1)
    lane40 = lax.broadcasted_iota(jnp.int32, (HALF_V, LANE), 1)
    lane16 = lax.broadcasted_iota(jnp.int32, (16, LANE), 1)
    vbuf[pl.ds(pl.multiple_of(1600 * (1 - k), 64), 64)] = jnp.zeros((64, COLS), BF16)
    wdp[:, pl.ds(VIRT, 48)] = jnp.zeros((OCC, 48, WIDE), BF16)

    def slabs(ref, h, col_half):
        @pl.loop(0, NCH)
        def _(g):
            parts = [
                ref[half(h), pl.ds(pl.multiple_of(g * WIDE + LANE * m, LANE), LANE)].astype(F32)
                for m in range(5)
            ]
            for q, seg in enumerate(split_segments(parts, lane32)):
                zt[h, pl.ds(pl.multiple_of((col_half * 40 + g * 8 + q) * ZS, 8), 32)] = seg

    def regroup(h, vh, l3_rows, tb_at):
        def rows(ik):
            return zt[h, pl.ds(HALF_V * ZS * vh + ik, HALF_V, stride=ZS)]

        @pl.loop(0, OCC)
        def _(kk):
            blk = jnp.concatenate([rows(kk), rows(OCC + kk)], axis=0).astype(BF16)
            l3[l3_rows, pl.ds(pl.multiple_of(kk * LANE, LANE), LANE)] = blk

        for i in BOTH:
            @pl.loop(0, OCC // 2)
            def _(k2):
                blk = jnp.concatenate([rows(i * OCC + 2 * k2), rows(i * OCC + 2 * k2 + 1)], axis=0).astype(BF16)
                tb[tb_at + i, pl.ds(pl.multiple_of(k2 * VIRT, 16), VIRT)] = blk

    def r3(rows):
        return jnp.dot(l3[rows], wdp[...].reshape(OCC * LANE, WIDE), preferred_element_type=F32)

    def r5(vh, first, count):
        rhs = jnp.concatenate([tb[first + i] for i in range(count)], axis=1)
        return lax.dot_general(wxs[vh], rhs, (((0,), (0,)), ((), ())), preferred_element_type=F32)

    def s_before():
        for h in BOTH:
            slabs(tf, h, c)
        ld_wx.wait()

        @pl.loop(0, OCC // 2)
        def _(k2):
            w = [wxb[2 * k2 + e].astype(F32) for e in BOTH]
            at = pl.ds(pl.multiple_of(k2 * VIRT, 16), VIRT)
            for vh in BOTH:
                part = [w[e][HALF_V * vh:HALF_V * vh + 40] for e in BOTH]
                wxs[vh, at] = jnp.concatenate(part, axis=0).astype(BF16)

        for h in BOTH:
            regroup(h, c, pl.ds(VIRT * h, VIRT), 2 * h)

        @pl.when(k == 1)
        def _():
            for q in range(1, 4):
                send_t(q)

        ld_wd.wait()
        r3a[...] = r3(pl.ds(0, 2 * VIRT))
        r5a[...] = r5(c, 0, 4)

        @pl.when(k == 0)
        def _():
            for q in range(2, 4):
                send_t(q)

    def s_prep(h):
        slabs(ty, h, 1 - c)
        regroup(h, 1 - c, pl.ds(0, VIRT), 0)

    def s_blocks(h):
        r3b[...] = r3(pl.ds(0, VIRT))
        r5b[...] = r5a[:, 256 * h:256 * h + 256] + r5(1 - c, 0, 2)

        @pl.loop(0, 2)
        def _(i):
            rows_a = pl.ds(pl.multiple_of(VIRT * h + HALF_V * i, 8), HALF_V)
            rows_b = pl.ds(pl.multiple_of(HALF_V * i, 8), HALF_V)
            seg_a = split_segments([r3a[rows_a, pl.ds(LANE * m, LANE)] for m in range(5)], lane40)
            seg_b = split_segments([r3b[rows_b, pl.ds(LANE * m, LANE)] for m in range(5)], lane40)
            lanes = pl.ds(pl.multiple_of(i * LANE, LANE), LANE)
            for j in range(8):
                s_a = seg_a[j] - r5b[pl.ds(pl.multiple_of(j * VIRT + HALF_V * c, 8), HALF_V), lanes]
                s_b = seg_b[j] - r5b[pl.ds(pl.multiple_of(j * VIRT + HALF_V * (1 - c), 8), HALF_V), lanes]
                row = (j // 4) * 16 + (2 * h + i) * 4 + j % 4
                zf[pl.ds(HALF_V * ZS * c + row, HALF_V, stride=ZS)] = s_a
                zf[pl.ds(HALF_V * ZS * (1 - c) + row, HALF_V, stride=ZS)] = s_b
                both = [jnp.where(c == 0, s_a, s_b), jnp.where(c == 0, s_b, s_a), jnp.zeros((48, LANE), F32)]
                row = jnp.where(diag, j * 4 + 2 * h + i, h * 16 + j * 2 + i)
                zg[pl.ds(row, VIRT, stride=ZS)] = jnp.transpose(jnp.concatenate(both, axis=0))[:VIRT]

    def tile_at(base, n, m):
        return pl.ds(pl.multiple_of(base + n * WIDE + LANE * m, LANE), LANE)

    def slab(z, g, q, row, size):
        return z[pl.ds(pl.multiple_of((g * 8 + q) * ZS + row, 8), size)]

    def g_y(n, h, b):
        return rc(gbuf.at[b, h, :, wide(n)], grecv.at[k, h, :, wide(n)], S_G, G_Y, (1 - c, own + b))

    def g_y_in():
        return rc(grecv, grecv, S_G, G_Y, d_y)

    def g_d(h):
        return rc(gown.at[1 - k, h], grecv.at[k, h], S_GD, G_D, d_p)

    def g_d_in():
        return rc(gown.at[1 - k], grecv.at[1 - k], S_GD, G_D, d_p)

    def f_y_in():
        return rc(frecv, frecv, S_F, F_Y, d_y)

    def f_y(n, h):
        rows = pl.ds(8 * h, 8)
        return rc(fbuf.at[:, rows, wide(n, COLS * (1 - c))], frecv.at[:, rows, wide(n)], S_F, F_Y, d_y)

    def g_off(h):
        lane8 = lax.broadcasted_iota(jnp.int32, (8, LANE), 1)

        def flat(dst, n, hf):
            for b in BOTH:
                segs = [slab(zg, n + NCH * hf, q, 16 * h + 8 * b, 8) for q in range(8)]
                for m, tile in enumerate(join_segments(segs, lane8)):
                    dst[b, h, :, tile_at(0, n, m)] = tile

        @pl.loop(0, NCH)
        def _(n):
            flat(gown, n, c)

        g_d(h).start()

        @pl.loop(0, NCH)
        def _(n):
            flat(gbuf, n, 1 - c)
            for b in BOTH:
                g_y(n, h, b).start()

        grecv[k, h] = gown[k, h]

    def f_off(h, hf, first=0, last=NCH):
        lane8 = lax.broadcasted_iota(jnp.int32, (8, LANE), 1)
        rows = pl.ds(8 * h, 8)

        @pl.loop(first, last)
        def _(n):
            for b in BOTH:
                segs = [slab(zf, n + NCH * hf, q, 16 * b + 8 * h, 8) for q in range(8)]
                for m, tile in enumerate(join_segments(segs, lane8)):
                    fbuf[b, rows, tile_at(COLS * hf, n, m)] = tile
            if hf is not c:
                f_y(n, h).start()

    def g_p():
        return rc(gps, gpz, S_G, G_P, d_p)

    def give_g():
        @pl.loop(0, VIRT, unroll=8)
        def _(v):
            gps[v] = zg[pl.ds(pl.multiple_of(v * ZS + 16 * (1 - k), 8), 16)]

        g_p().start()

    def q_diag():
        g_p().wait_recv()

        def flat(hf, send):
            @pl.loop(0, NCH)
            def _(n):
                for b, mine in ((k, True), (1 - k, False)):
                    row = pl.multiple_of(16 * b, 16)
                    segs = []
                    for q in range(8):
                        g = n + NCH * hf
                        extra = slab(zg, g, q, row, 16) if mine else gpz[g * 8 + q]
                        segs.append(slab(zf, g, q, row, 16) + extra)
                    for m, tile in enumerate(join_segments(segs, lane16)):
                        fbuf[b, :, tile_at(COLS * hf, n, m)] = tile
                if send:
                    for h in BOTH:
                        f_y(n, h).start()

        flat(1 - c, True)
        flat(c, False)

    s_before()

    early, late = 1 - x, x

    def pair(h, cols, step):
        ts = pl.ds(2 * h, 2)
        return rc(xp.at[p3, ts, :, :, cols], prx.at[ts, :, :, cols], S_XP, E_D + 3 * h + step, d_p)

    def cross(hf, h, cols, slot):
        ts = pl.ds(2 * h, 2)
        return rc(xp.at[p2, ts, hf, :, cols], xrecv.at[ts, hf, :, cols], S_XP, slot, d_x)

    def over_columns(step):
        @pl.loop(0, 2)
        def _(g):
            step(pl.ds(pl.multiple_of(g * 2 * WIDE, LANE), 2 * WIDE), (2 * g, 2 * g + 1))

        step(pl.ds(4 * WIDE, WIDE), (4,))

    def ladder_0():
        def step(cols, ns):
            lhs = tr1[pl.ds(other, 2), half(0)].reshape(64, KPAD)
            prod = jnp.dot(lhs, vbuf[:, cols], preferred_element_type=F32)
            xp[pl.ds(other, 2), pl.ds(0, 2), :, :, cols] = prod.reshape(2, 2, 2, 8, -1)
            pair(0, cols, ns[0] // 2).start()

        over_columns(step)

    def ladder_1():
        def step(cols, ns):
            lhs = jnp.concatenate(
                [tr1[pl.ds(other, 2), half(1)].reshape(64, KPAD), tr1[pl.ds(own, 2)].reshape(LANE, KPAD)], axis=0
            )
            prod = jnp.dot(lhs, vbuf[:, cols], preferred_element_type=F32)
            xp[pl.ds(other, 2), pl.ds(2, 2), :, :, cols] = prod[:64].reshape(2, 2, 2, 8, -1)
            xp[pl.ds(own, 2), :, :, :, cols] = prod[64:].reshape(2, 4, 2, 8, -1)
            pair(1, cols, ns[0] // 2).start()
            rc(xp.at[p1, :, :, :, cols], pown.at[:, :, :, cols], S_XP, O_D, d_p).start()

        over_columns(step)

    def combine(h, first=0, last=3):
        ts = pl.ds(2 * h, 2)
        for step in range(first, last):
            ns = STEPS[step]
            cols = pl.ds(ns[0] * WIDE, len(ns) * WIDE)
            pair(h, cols, step).wait_recv()
            xp[p2, ts, :, :, cols] += prx[ts, :, :, cols]
            cross(early, h, cols, L_X).start()

    def late_pass(h):
        def step(cols, ns):
            for t in (2 * h, 2 * h + 1):
                g2 = [grecv[core, hh, pl.ds(2 * t, 2), cols] for core in BOTH for hh in BOTH]
                xp[p2, t, late, :, cols] += jnp.concatenate(g2, axis=0)
            cross(late, h, cols, L_X + 1 + ns[0] // 2 if h else L_X).start()

        over_columns(step)

    def x_y():
        return rc(xpart, xyrecv, S_XY, X_Y, d_y)

    def x_part():
        xpart[...] = lax.dot_general(
            ov[...], tcol[...].reshape(4 * ROWS, COLS), (((1,), (1,)), ((), ())), preferred_element_type=F32
        )
        x_y().start()

    def take(h):
        tr1[pl.ds(other, 2), half(h)] = tcol[pl.ds(other, 2), half(h), my_k(k)]

    def send_m():
        x_y().wait_recv()
        m_rows = (ob[...].astype(F32) + 0.5 * (xpart[...] + xyrecv[...])).astype(BF16)
        for q in range(4):
            msend[q] = m_rows[:, q * ROWS:(q + 1) * ROWS]
        mfull[r] = msend[r]
        for cp in m_out():
            cp.start()

    def m_out():
        return (
            rc(msend.at[p1], mfull.at[r], S_M, M_I, d_p),
            rc(msend.at[p2], mfull.at[r], S_M, M_I, d_x),
            rc(msend.at[p3], mfull.at[r], S_M, M_I, d_d),
        )

    def m_in():
        return rc(mfull.at[pl.ds(0, 3)], mfull.at[pl.ds(0, 3)], S_M, M_I, d_p)

    @pl.when(diag)
    def _():
        t_y(0).wait_recv()
        for cc in (1, 0):
            r_x(0, cc).start()
        t_x(0, p2).wait_recv()
        t_fwd(0).start()
        t_y(1).wait_recv()
        r_x(1, k).start()
        t_x(1, p2).wait_recv()
        t_fwd(1).start()
        r_y(1, 1 - k).start()
        t_y(3).start()
        for q in range(2, 4):
            t_x(q, r).start()
        t_fwd_in(0).wait_recv()
        take(0)
        ld_v.wait()
        ladder_0()
        s_prep(0)
        for q in range(2, 4):
            t_x(q, p2).wait_recv()
            t_fwd(q).start()
            for cc in (1, 0):
                r_y(q, cc).start()
        combine(0)
        s_blocks(0)
        t_p(p1).wait_recv()
        tr1[r] = tcol[r, :, my_k(k)]
        tr1[p1] = tcol[p1, :, my_k(k)]
        t_fwd_in(1).wait_recv()
        take(1)
        ladder_1()
        ld_o.wait()
        x_part()
        combine(1)
        t_y_in().wait_recv()
        s_prep(1)
        s_blocks(1)
        give_g()
        q_diag()
        g_y_in().wait_recv()
        late_pass(0)
        ld_oooo.wait()
        send_m()
        late_pass(1)

    @pl.when(off)
    def _():
        for q in BOTH:
            t_y(q).wait_recv()
        s_prep(0)
        s_blocks(0)
        g_off(0)
        for q in BOTH:
            t_x(q, p2).wait_recv()
            t_fwd(q).start()
        f_off(0, 1 - c, 0, 2)
        ld_v.wait()
        r_in(0, R_0).wait_recv()
        ladder_0()
        combine(0, 0, 1)
        t_y_in().wait_recv()
        r_p(r).start()
        tr1[r] = ty[:, my_k(k)]
        s_prep(1)
        combine(0, 1)
        s_blocks(1)
        for q in range(2, 4):
            t_x(q, p2).wait_recv()
            t_fwd(q).start()
        g_off(1)
        g_d_in().wait_recv()
        late_pass(0)
        r_in(1, R_1).wait_recv()
        r_p(p1).wait_recv()
        ladder_1()
        t_p(p1).wait_recv()
        for h in BOTH:
            t_fwd_in(h).wait_recv()
        ld_o.wait()
        x_part()
        f_off(0, 1 - c, 2)
        ld_oooo.wait()
        send_m()
        combine(1)
        late_pass(1)
        f_off(1, 1 - c)
        for h in BOTH:
            f_off(h, c)

    m_in().wait_recv()
    ld_d.wait()
    rc(xp.at[p1], pown, S_XP, O_D, d_p).wait_recv()
    f_y_in().wait_recv()
    rc(xp.at[p2, pl.ds(0, 3)], xrecv.at[pl.ds(0, 3)], S_XP, L_X, d_x).wait_recv()

    def settle(t, hf, cols):
        rows = pl.ds(pl.multiple_of(16 * t + 8 * hf, 8), 8)
        obuf[rows, cols] = (obuf[rows, cols] + xrecv[t, hf, :, cols]) / dbuf[rows, cols]

    def gather(cols, ns):
        width = len(ns) * WIDE
        r2 = lax.dot_general(
            mfull[...].reshape(4 * ROWS, ROWS), tcol[:, :, cols].reshape(4 * ROWS, width),
            (((0,), (0,)), ((), ())), preferred_element_type=F32,
        )
        part = xp[r, :, :, :, cols] + pown[:, :, :, cols]
        obuf[:, cols] = ov[:, cols].astype(F32) + r2 + part.reshape(ROWS, width)
        mine = pl.ds(pl.multiple_of(COLS * c + ns[0] * WIDE, LANE), width)
        for i in range(4):
            for ref, hf, at in ((fbuf, c, mine), (frecv, 1 - c, cols)):
                f8 = jnp.concatenate([ref[b, pl.ds(4 * i, 4), at] for b in BOTH], axis=0)
                rows = pl.ds(pl.multiple_of(16 * i + 8 * hf, 8), 8)
                obuf[rows, cols] += f8
            settle(i, x, cols)
            if i < 2:
                settle(i, 1 - x, cols)

    def finish(cols, ns):
        cross(1 - x, 1, cols, L_X + 1 + ns[0] // 2).wait_recv()
        for t in (2, 3):
            settle(t, 1 - x, cols)

    over_columns(gather)
    over_columns(finish)

    rc(tcol, tcol, S_T, T_X, d_x).wait_send()
    rc(xp.at[pl.ds(0, 3)], xp.at[pl.ds(0, 3)], S_XP, L_X, d_x).wait_send()
    rc(frecv, frecv, S_F, F_Y, d_y).wait_send()
    x_y().wait_send()
    rc(msend.at[pl.ds(0, 3)], mfull.at[pl.ds(0, 3)], S_M, M_I, d_p).wait_send()

    @pl.when(diag)
    def _():
        g_p().wait_send()
        rc(tr1.at[pl.ds(0, 2)], tr1.at[pl.ds(0, 2)], S_R, R_1, d_y).wait_send()

    @pl.when(off)
    def _():
        r_p(r).wait_send()
        rc(gbuf, grecv, S_G, G_Y, d_y).wait_send()
        g_d_in().wait_send()


def solution(mesh):
    def sweep(t_blk, d_blk, o_blk, v_blk, oooo, wd_blk, wx_blk):
        any_spec = pl.BlockSpec(memory_space=pl.ANY)
        vm = pltpu.VMEM
        return pl.pallas_call(
            kernel,
            out_shape=pltpu.VMEM((ROWS, COLS), F32),
            in_specs=[any_spec] * 7,
            out_specs=pl.BlockSpec(memory_space=pltpu.VMEM),
            scratch_shapes=[
                vm((ROWS, COLS), F32),
                vm((ROWS, COLS), F32),
                vm((ROWS, COLS), BF16),
                vm((KPAD, COLS), BF16),
                vm((ROWS, 256), BF16),
                vm((OCC, LANE, WIDE), BF16),
                vm((OCC, VIRT, WIDE), BF16),
                vm((4, ROWS, COLS), BF16),
                vm((ROWS, COLS), BF16),
                vm((4, ROWS, KPAD), BF16),
                vm((2, VIRT * ZS, LANE), F32),
                vm((2, WIDE, WIDE), BF16),
                vm((4, WIDE, LANE), BF16),
                vm((2 * VIRT, OCC * LANE), BF16),
                vm((2 * VIRT, WIDE), F32),
                vm((VIRT, WIDE), F32),
                vm((WIDE, 512), F32),
                vm((WIDE, 256), F32),
                vm((VIRT * ZS, LANE), F32),
                vm((VIRT * ZS, LANE), F32),
                vm((VIRT, 16, LANE), F32),
                vm((VIRT, 16, LANE), F32),
                vm((2, 16, 2 * COLS), F32),
                vm((2, 2, 8, COLS), F32),
                vm((2, 2, 8, COLS), F32),
                vm((2, 16, COLS), F32),
                vm((2, 2, 8, COLS), F32),
                vm((4, 4, 2, 8, COLS), F32),
                vm((4, 2, 8, COLS), F32),
                vm((4, 2, 8, COLS), F32),
                vm((4, 2, 8, COLS), F32),
                vm((ROWS, 256), F32),
                vm((ROWS, 256), F32),
                vm((4, ROWS, ROWS), BF16),
                vm((4, ROWS, ROWS), BF16),
                pltpu.SemaphoreType.DMA((10,)),
                pltpu.SemaphoreType.DMA((N_SEND,)),
                pltpu.SemaphoreType.DMA((N_RECV,)),
            ],
            compiler_params=pltpu.CompilerParams(
                collective_id=0, has_side_effects=True, vmem_limit_bytes=54 * 1024 * 1024
            ),
            name="ccd_sweep",
        )(t_blk, d_blk, o_blk, v_blk, oooo, wd_blk.reshape(OCC, VIRT, WIDE), wx_blk.reshape(OCC, VIRT, WIDE))

    amp = P("row", "col")
    wide_spec = P(None, "col")
    return jax.shard_map(
        sweep, mesh=mesh, in_specs=(amp, amp, amp, amp, P(), wide_spec, wide_spec), out_specs=amp, check_vma=False
    )
```
